128 devices in a mesh: gx: 4 (over y), gy: 4 (over z), gz: 8 (over x, core).
Axes of the slice: x: 4, y: 4, z: 4, core: 2. Of those that a mesh axis runs over, the one named last changes fastest.
Arguments:
- start: float32 [4, 4, 8, 1, 32, 1024], P('gx', 'gy', 'gz'), may hold values from -6 to 6
- stencils: float32 [6, 4, 4, 8, 32, 32], P(None, 'gx', 'gy', 'gz'), as said below
Outputs:
- basis: float32 [4, 4, 8, 1, 5, 32, 1024], P('gx', 'gy', 'gz')
- coefficients: float32 [1, 2, 5], replicated
The draws below stay inside these ranges and needn't reach their ends.
Inputs may be any that keep to these rules, and one draw needn't show every extreme that they name: `stencils`: each of a patch's six matrices is symmetric positive definite.
All inputs are finite; a program needn't handle non-finite values.
Results may differ from the reference program's by a relative error of at most 0.0003.
Values sent between devices are 32-bit elements; how exact they have to be, the bound alone decides.
A program may use at most 128 MiB of HBM per device.

```python
import jax
import jax.numpy as jnp
from jax import lax

C = 32
PROBES = 1
ITERS = 5
PATCH_X = 4
PATCH_Y = 4
PATCH_Z = 8
N_GX = 4
N_GY = 4
N_GZ = 8


def draw_stencils(key, part):
    key_entries = jax.random.fold_in(key, 11)
    key_scale = jax.random.fold_in(key, 12)
    shape = (6, PATCH_X, PATCH_Y, PATCH_Z, C, C)
    entries = jax.random.normal(key_entries, shape, jnp.float32)
    rows = jnp.arange(C)
    band = (jnp.abs(rows[:, None] - rows[None, :]) <= 4).astype(jnp.float32)
    factor = entries * band
    square = jnp.einsum('...ij,...kj->...ik', factor, factor) / 9.0
    square = square + 0.5 * jnp.eye(C, dtype=jnp.float32)
    scales = jnp.exp(jax.random.uniform(key_scale, (6, PATCH_X, PATCH_Y, PATCH_Z, 1, 1), jnp.float32, -0.7, 0.7))
    return (square * scales).astype(jnp.float32)


def level_of(stream_key, shape, cuts, smallest, high):
    loudness = 1.0
    for axis_at, blocks in cuts:
        steps = jax.random.uniform(jax.random.fold_in(jax.random.fold_in(stream_key, 6), axis_at), (blocks,), jnp.float32, smallest / len(cuts), high / len(cuts))
        loudness = loudness * jnp.repeat(jnp.exp(steps), shape[axis_at] // blocks).reshape((-1,) + (1,) * (len(shape) - 1 - axis_at))
    return loudness


def bell_draw(rng, extent, spread, bound, pieces=(), held_as=jnp.bfloat16):
    result = jax.random.normal(rng, extent, jnp.float32) * spread
    if len(pieces) > 0:
        result = level_of(rng, extent, pieces, -0.22, 0.18) * result
    return jnp.clip(result, min=-bound, max=bound).astype(held_as)


def setup_inputs(seed: int = 0) -> dict:
    splits = jax.random.split(jax.random.key(seed), 3)
    return {
        "start": bell_draw(splits[0], (PATCH_X, PATCH_Y, PATCH_Z, PROBES, C, C * C), 1.0, 6.0, ((0, 4), (1, 4), (2, 8)), jnp.float32),
        "stencils": draw_stencils(jax.random.fold_in(splits[2], 71), 0),
    }


def along(field, stencils, which, dim):
    grid = field.reshape(N_GX, C, N_GY, C, N_GZ, C)
    matrix = stencils[which]
    forms = ['xaybzc,xyzea->xeybzc', 'xaybzc,xyzeb->xayezc', 'xaybzc,xyzec->xaybze']
    out = jnp.einsum(forms[dim], grid, matrix, precision=lax.Precision.HIGHEST)
    return out.reshape(N_GX * C, N_GY * C, N_GZ * C)

def fold(field, dim, groups):
    moved = jnp.moveaxis(field, dim, 0)
    rest = moved.shape[1:]
    blocks = moved.reshape((groups, C) + rest)
    zero_row = jnp.zeros((1,) + rest, jnp.float32)
    first = blocks[:, 0] + jnp.concatenate([zero_row, blocks[:-1, C - 1]], axis=0)
    last = blocks[:, C - 1] + jnp.concatenate([blocks[1:, 0], zero_row], axis=0)
    blocks = blocks.at[:, 0].set(first).at[:, C - 1].set(last)
    return jnp.moveaxis(blocks.reshape((groups * C,) + rest), 0, dim)

def assemble(field):
    field = fold(field, 0, N_GX)
    field = fold(field, 1, N_GY)
    return fold(field, 2, N_GZ)

def weight_vector(groups):
    index = jnp.arange(groups * C)
    plane = index % C
    block = index // C
    shared = (plane == 0) & (block > 0) | (plane == C - 1) & (block < groups - 1)
    return jnp.where(shared, 0.5, 1.0).astype(jnp.float32)

def operate(field, stencils):
    first = along(field, stencils, 5, 2)
    second = along(first, stencils, 4, 1)
    term_one = along(second, stencils, 0, 0)
    third = along(first, stencils, 1, 1)
    fourth = along(field, stencils, 2, 2)
    fifth = along(fourth, stencils, 4, 1)
    term_two = along(third + fifth, stencils, 3, 0)
    return assemble(term_one + term_two)

def single(start_one, stencils, weights):
    first = assemble(weights * start_one)
    vector = first / jnp.sqrt(jnp.sum(weights * first * first))
    vectors = [vector]
    alphas = []
    betas = []
    for j in range(ITERS):
        image = operate(vectors[j], stencils)
        alpha = jnp.sum(weights * image * vectors[j])
        image = image - alpha * vectors[j]
        if j > 0:
            image = image - betas[j - 1] * vectors[j - 1]
        heights = [jnp.sum(weights * basis_vec * image) for basis_vec in vectors]
        for i in range(j + 1):
            image = image - heights[i] * vectors[i]
        beta = jnp.sqrt(jnp.sum(weights * image * image))
        vectors.append(image / beta)
        alphas.append(alpha)
        betas.append(beta)
    coeffs = jnp.stack([jnp.stack(alphas), jnp.stack(betas)])
    return (jnp.stack(vectors[1:]), coeffs)

def reference(start, stencils):
    weights = weight_vector(N_GX)[:, None, None] * weight_vector(N_GY)[None, :, None] * weight_vector(N_GZ)[None, None, :]
    seven = start.reshape(N_GX, N_GY, N_GZ, PROBES, C, C, C)
    whole = jnp.transpose(seven, (3, 0, 4, 1, 5, 2, 6)).reshape(PROBES, N_GX * C, N_GY * C, N_GZ * C)
    basis_whole, coefficients = lax.map(lambda one: single(one, stencils, weights), whole)
    split = basis_whole.reshape(PROBES, ITERS, N_GX, C, N_GY, C, N_GZ, C)
    basis = jnp.transpose(split, (2, 4, 6, 0, 1, 3, 5, 7)).reshape(N_GX, N_GY, N_GZ, PROBES, ITERS, C, C * C)
    return (basis, coefficients)
```

```python
import functools

import jax
import jax.numpy as jnp
from jax import lax
from jax.experimental import pallas as pl
from jax.experimental.pallas import tpu as pltpu
from jax.sharding import PartitionSpec as P

ITERS = 5
C = 32
MESH = pl.DeviceIdType.MESH
F32 = jnp.float32
AXES = ("gx", "gy", "gz")
DIRS = [
    (dx, dy, dz)
    for dx in (-1, 0, 1)
    for dy in (-1, 0, 1)
    for dz in (-1, 0, 1)
    if (dx, dy, dz) != (0, 0, 0)
]
SLOT = {d: i for i, d in enumerate(DIRS)}
SHRINK = 2.0**-17


def iota(shape, dim):
    return lax.broadcasted_iota(jnp.int32, shape, dim)


def roll(x, shift, axis):
    size = x.shape[axis]
    shift = shift % size
    return x if shift == 0 else pltpu.roll(x, shift, axis)


def swap(field):
    x = field.reshape(32, 8, 128)
    s, l = iota((1, 8, 128), 1), iota((1, 8, 128), 2)
    s1, l1 = (s // 2) % 2, l // 64
    r = roll(x, 64, 2)
    x = jnp.where(s1 == l1, x, jnp.where(s1 == 0, roll(r, -2, 1), roll(r, 2, 1)))
    s0, l0 = s % 2, (l // 32) % 2
    up, down = roll(roll(x, 32, 2), -1, 1), roll(roll(x, -32, 2), 1, 1)
    x = jnp.where(s0 == l0, x, jnp.where(s0 == 0, up, down))
    even = jnp.concatenate([x[t * 4 : t * 4 + 4] for t in range(0, 8, 2)], axis=0)
    odd = jnp.concatenate([x[t * 4 : t * 4 + 4] for t in range(1, 8, 2)], axis=0)
    half = s < 4
    top = jnp.where(half, even, roll(odd, 4, 1))
    bottom = jnp.where(half, roll(even, 4, 1), odd)
    parts = []
    for ai in range(4):
        for part in (top, bottom):
            for k in range(4):
                parts.append(part[k * 4 + ai : k * 4 + ai + 1])
    return jnp.concatenate(parts, axis=0).reshape(256, 128)


def wide(field):
    return jnp.concatenate([field[t * 32 : t * 32 + 32] for t in range(8)], axis=1)


def tall(field):
    return jnp.concatenate([field[:, t * 128 : t * 128 + 128] for t in range(8)], axis=0)


def dot(left, right):
    return lax.dot_general(
        left,
        right,
        (((1,), (0,)), ((), ())),
        precision=lax.Precision.HIGHEST,
        preferred_element_type=F32,
    )


def matvec(field, xmat_ref, ymat_ref, zmat_ref):
    first = dot(xmat_ref[...], wide(field))
    mass, stiff = swap(tall(first[:C])), swap(tall(first[C:]))
    second = dot(ymat_ref[...], jnp.concatenate([wide(stiff), wide(mass)], axis=0))
    third = jnp.concatenate([tall(second[:C]), tall(second[C:])], axis=1)
    return swap(dot(third, zmat_ref[...]))


def block_diagonal(matrix):
    zero = jnp.zeros((C, C), F32)
    rows = []
    for i in range(4):
        rows.append(jnp.concatenate([matrix if k == i else zero for k in range(4)], axis=1))
    return jnp.concatenate(rows, axis=0)


def weight_field(sizes, here):
    row, lane = iota((256, 128), 0), iota((256, 128), 1)
    places = (row % C, (row // C) * 4 + lane // C, lane % C)
    weight = jnp.ones((256, 128), F32)
    for place, size, at in zip(places, sizes, here):
        low = jnp.where(at > 0, 0.5, 1.0).astype(F32)
        high = jnp.where(at < size - 1, 0.5, 1.0).astype(F32)
        weight = weight * jnp.where(place == 0, low, jnp.where(place == C - 1, high, 1.0))
    return weight


def neighbour(sizes, here, step):
    fine = None
    for size, at, d in zip(sizes, here, step):
        if d != 0:
            inside = at > 0 if d < 0 else at < size - 1
            fine = inside if fine is None else jnp.logical_and(fine, inside)
    return fine, tuple(at + d for at, d in zip(here, step))


def pack(out_ref, send_ref):
    s, l = iota((8, 128), 0), iota((8, 128), 1)
    lower = lambda t, ai: out_ref[pl.ds(t * 32 + ai * 8, 8), :]
    zero = jnp.zeros((8, 128), F32)
    low, high = zero, zero
    for t in range(8):
        for ai in range(4):
            r = ai * 8 + t
            moved = roll(lower(t, ai), r, 1)
            low = jnp.where(l % C == r, moved, low)
            high = jnp.where(l % C == (r + C - 1) % C, moved, high)
    for dz, plane, base in ((-1, low, 0), (1, high, -31)):
        for dx in (-1, 0, 1):
            for dy in (-1, 0, 1):
                lanes = base - dx * 24 - dy * 103
                part = roll(roll(plane, lanes, 1), dx, 0)
                keep = None
                if dx != 0:
                    keep = (s == (7 if dx < 0 else 0)) & ((l % C) // 8 == (3 if dx < 0 else 0))
                if dy != 0:
                    mine = (l // C == (3 if dy < 0 else 0)) & (l % 8 == (7 if dy < 0 else 0))
                    keep = mine if keep is None else keep & mine
                send_ref[SLOT[(dx, dy, dz)]] = part if keep is None else jnp.where(keep, part, 0.0)
    for dx in (-1, 1):
        plane = out_ref[pl.ds(0 if dx < 0 else C - 1, 8, stride=C), :]
        send_ref[SLOT[(dx, 0, 0)]] = plane
        for dy in (-1, 1):
            part = roll(roll(plane, 96 if dy < 0 else 32, 1), dy, 0)
            keep = (s == (7 if dy < 0 else 0)) & (l // C == (3 if dy < 0 else 0))
            send_ref[SLOT[(dx, dy, 0)]] = jnp.where(keep, part, 0.0)
    for dy in (-1, 1):
        plane = zero
        for ai in range(4):
            piece = roll(lower(0 if dy < 0 else 7, ai), C * (ai + (0 if dy < 0 else 1)), 1)
            plane = jnp.where(l // C == ai, piece, plane)
        send_ref[SLOT[(0, dy, 0)]] = plane


def unpack(out_ref, got_ref):
    l = iota((8, 128), 1)
    near = (-1, 0, 1)
    for dx in (-1, 1):
        plane = sum(got_ref[SLOT[(dx, dy, 0)]] for dy in near)
        rows = pl.ds(C - 1 if dx < 0 else 0, 8, stride=C)
        out_ref[rows, :] = out_ref[rows, :] + plane
    low, high = (
        sum(got_ref[SLOT[(dx, dy, dz)]] for dx in near for dy in near) for dz in (1, -1)
    )
    first, last = got_ref[SLOT[(0, 1, 0)]], got_ref[SLOT[(0, -1, 0)]]
    for t in range(8):
        for ai in range(4):
            r = ai * 8 + t
            rows = pl.ds(t * 32 + ai * 8, 8)
            add = jnp.where(l % C == 0, roll(low, -r, 1), 0.0)
            add = add + jnp.where(l % C == C - 1, roll(high, 31 - r, 1), 0.0)
            if t == 0:
                add = add + jnp.where(l < C, roll(first, -C * ai, 1), 0.0)
            if t == 7:
                add = add + jnp.where(l >= 96, roll(last, 96 - C * ai, 1), 0.0)
            out_ref[rows, :] = out_ref[rows, :] + add


def kernel(
    sizes,
    start_ref,
    stencils_ref,
    basis_ref,
    coefficients_ref,
    out,
    vecs,
    images,
    weights,
    xmat,
    ymat,
    zmat,
    sends,
    gots,
    line,
    plane,
    coef,
    send_sem,
    got_sem,
    line_send,
    line_got,
    plane_send,
    plane_got,
):
    here = tuple(lax.axis_index(a) for a in AXES)
    nx, ny, nz = sizes
    gx, gy, gz = here
    line_peers = [(gx, gy, lax.rem(gz + k, nz)) for k in range(1, nz)]
    plane_peers = [
        (lax.rem(gx + k, nx), lax.rem(gy + m, ny), gz)
        for k in range(nx)
        for m in range(ny)
        if (k, m) != (0, 0)
    ]
    spans = [
        1 + jnp.where(at > 0, 1, 0) + jnp.where(at < size - 1, 1, 0)
        for at, size in zip(here, sizes)
    ]
    degree = spans[0] * spans[1] * spans[2] - 1
    degrees = sorted(
        {
            i * j * k - 1
            for i in span_set(nx)
            for j in span_set(ny)
            for k in span_set(nz)
        }
    )

    gots[...] = jnp.zeros_like(gots)

    barrier = pltpu.get_barrier_semaphore()
    for d in DIRS:
        fine, there = neighbour(sizes, here, d)

        @pl.when(fine)
        def _():
            pl.semaphore_signal(barrier, inc=1, device_id=there, device_id_type=MESH)

    for there in line_peers + plane_peers:
        pl.semaphore_signal(barrier, inc=1, device_id=there, device_id_type=MESH)

    vecs[...] = jnp.zeros_like(vecs)
    images[...] = jnp.zeros_like(images)
    coef[...] = jnp.zeros_like(coef)
    weights[...] = weight_field(sizes, here)
    kx, ky, kz, mx, my, mz = (stencils_ref[i] for i in range(6))
    xmat[...] = jnp.concatenate([mx, kx], axis=0)
    top = jnp.concatenate([my, ky], axis=1)
    ymat[...] = jnp.concatenate([top, jnp.concatenate([jnp.zeros((C, C), F32), my], axis=1)], axis=0)
    zmat[...] = jnp.concatenate([block_diagonal(mz.T), block_diagonal(kz.T)], axis=0)

    def exchange_start(par):
        pack(out, sends.at[par])
        if True:
            for d in sorted(DIRS, key=lambda d: -sum(abs(i) for i in d)):
                fine, there = neighbour(sizes, here, d)

                @pl.when(fine)
                def _():
                    pltpu.make_async_remote_copy(
                        src_ref=sends.at[par, SLOT[d]],
                        dst_ref=gots.at[par, SLOT[d]],
                        send_sem=send_sem.at[par],
                        recv_sem=got_sem.at[par],
                        device_id=there,
                        device_id_type=MESH,
                    ).start()

    def exchange_end(par):
        for n in degrees:

            @pl.when(degree == n)
            def _():
                both = pltpu.make_async_remote_copy(
                    src_ref=sends.at[par, pl.ds(0, n)],
                    dst_ref=gots.at[par, pl.ds(0, n)],
                    send_sem=send_sem.at[par],
                    recv_sem=got_sem.at[par],
                    device_id=line_peers[0],
                    device_id_type=MESH,
                )
                both.wait_recv()
                both.wait_send()

        unpack(out, gots.at[par])

    def reduce_start(buffer, at, peers, par, s_sem, g_sem, tile):
        buffer[par, at] = tile
        for there in peers:
            pltpu.make_async_remote_copy(
                src_ref=buffer.at[par, at],
                dst_ref=buffer.at[par, at],
                send_sem=s_sem.at[par],
                recv_sem=g_sem.at[par],
                device_id=there,
                device_id_type=MESH,
            ).start()

    def reduce_end(buffer, peers, par, s_sem, g_sem):
        both = pltpu.make_async_remote_copy(
            src_ref=buffer.at[par, pl.ds(0, len(peers))],
            dst_ref=buffer.at[par, pl.ds(0, len(peers))],
            send_sem=s_sem.at[par],
            recv_sem=g_sem.at[par],
            device_id=peers[0],
            device_id_type=MESH,
        )
        both.wait_recv()
        both.wait_send()
        return sum(buffer[par, k] for k in range(len(peers) + 1))

    def products(image):
        weighted = weights[...] * image
        pairs = [(vecs[i], weighted) for i in range(ITERS)]
        pairs += [(image, weighted), (vecs[0], weights[...] * vecs[0])]
        tile = jnp.zeros((8, 128), F32)
        for k, (left, right) in enumerate(pairs):
            lanes = jnp.sum(jnp.sum((left * right).reshape(32, 8, 128), axis=0), axis=0, keepdims=True)
            tile = jnp.where(iota((8, 128), 0) == k, lanes, tile)
        return tile

    def products_start(par, image):
        reduce_start(line, gz, line_peers, par, line_send, line_got, products(image))

    def products_middle(par):
        tile = reduce_end(line, line_peers, par, line_send, line_got)
        reduce_start(plane, gx * ny + gy, plane_peers, par, plane_send, plane_got, tile)

    def products_end(par):
        tile = reduce_end(plane, plane_peers, par, plane_send, plane_got)
        return jnp.sum(tile, axis=1, keepdims=True)

    def advance(j, totals, following):
        first = j == 0
        inverse = jnp.where(first, lax.rsqrt(totals[6:7]), 1.0)
        square = jnp.where(first, 1.0 / totals[6:7], 1.0)

        @pl.when(first)
        def _():
            vecs[0] = vecs[0] * inverse
            images[0] = images[0] * inverse

        heights = [totals[i : i + 1] * square for i in range(ITERS)]
        length = totals[5:6] * square
        beta = jnp.sqrt(length - sum(h * h for h in heights))
        alpha = sum(jnp.where(j == i, heights[i], 0.0) for i in range(ITERS))
        over = 1.0 / beta
        new = images[j]
        for i in range(ITERS):
            new = new - heights[i] * vecs[i]
        vecs[j + 1] = new * over
        s, l = iota((8, 128), 0), iota((8, 128), 1)
        entry = jnp.where(s == 0, alpha, jnp.where(s == 1, beta, 0.0))
        coef[...] = coef[...] + jnp.where(l == j, entry, 0.0)
        if following:
            image = out[...] * inverse
            for i in range(ITERS):
                image = image - heights[i] * images[i]
            images[j + 1] = image * over

    out[...] = tall(start_ref[...]) * weights[...] * SHRINK
    pl.semaphore_wait(barrier, degree + len(line_peers) + len(plane_peers))
    exchange_start(0)
    exchange_end(0)
    vecs[0] = out[...]
    out[...] = matvec(out[...], xmat, ymat, zmat)
    exchange_start(1)
    exchange_end(1)
    images[0] = out[...]

    def body(j, carry):
        par = lax.rem(j, 2)
        image = images[j]
        products_start(par, image)
        out[...] = matvec(image, xmat, ymat, zmat)
        exchange_start(par)
        products_middle(par)
        exchange_end(par)
        advance(j, products_end(par), True)
        return carry

    lax.fori_loop(0, ITERS - 1, body, 0)
    par = (ITERS - 1) % 2
    products_start(par, images[ITERS - 1])
    products_middle(par)
    advance(ITERS - 1, products_end(par), False)
    for i in range(ITERS):
        basis_ref[i] = wide(vecs[i + 1])
    coefficients_ref[...] = coef[0:2, 0:ITERS]


def span_set(size):
    return {1} if size == 1 else {2} if size == 2 else {2, 3}


def shards(sizes, start, stencils):
    nx, ny, nz = sizes
    vmem = pl.BlockSpec(memory_space=pltpu.VMEM)
    basis, coefficients = pl.pallas_call(
        functools.partial(kernel, sizes),
        out_shape=(
            jax.ShapeDtypeStruct((ITERS, C, C * C), F32),
            jax.ShapeDtypeStruct((2, ITERS), F32),
        ),
        in_specs=[vmem, vmem],
        out_specs=(vmem, vmem),
        scratch_shapes=[
            pltpu.VMEM((256, 128), F32),
            pltpu.VMEM((ITERS + 1, 256, 128), F32),
            pltpu.VMEM((ITERS, 256, 128), F32),
            pltpu.VMEM((256, 128), F32),
            pltpu.VMEM((2 * C, C), F32),
            pltpu.VMEM((2 * C, 2 * C), F32),
            pltpu.VMEM((256, 128), F32),
            pltpu.VMEM((2, len(DIRS), 8, 128), F32),
            pltpu.VMEM((2, len(DIRS), 8, 128), F32),
            pltpu.VMEM((2, nz, 8, 128), F32),
            pltpu.VMEM((2, nx * ny, 8, 128), F32),
            pltpu.VMEM((8, 128), F32),
        ]
        + [pltpu.SemaphoreType.DMA((2,))] * 6,
        compiler_params=pltpu.CompilerParams(collective_id=0, has_side_effects=True),
    )(start.reshape(C, C * C), stencils.reshape(6, C, C))
    return (
        basis.reshape(1, 1, 1, 1, ITERS, C, C * C),
        coefficients.reshape(1, 2, ITERS),
    )


def solution(mesh):
    sizes = tuple(mesh.shape[a] for a in AXES)
    return jax.shard_map(
        functools.partial(shards, sizes),
        mesh=mesh,
        in_specs=(P("gx", "gy", "gz", None, None, None), P(None, "gx", "gy", "gz", None, None)),
        out_specs=(P("gx", "gy", "gz", None, None, None, None), P()),
        check_vma=False,
    )
```

```python
import functools

import jax
import jax.numpy as jnp
from jax import lax
from jax.experimental import pallas as pl
from jax.experimental.pallas import tpu as pltpu
from jax.sharding import PartitionSpec as P

ITERS = 5
C = 32
MESH = pl.DeviceIdType.MESH
F32 = jnp.float32
AXES = ("gx", "gy", "gz")
DIRS = [
    (dx, dy, dz)
    for dx in (-1, 0, 1)
    for dy in (-1, 0, 1)
    for dz in (-1, 0, 1)
    if (dx, dy, dz) != (0, 0, 0)
]
SLOT = {d: i for i, d in enumerate(DIRS)}
SHRINK = 2.0**-17


def iota(shape, dim):
    return lax.broadcasted_iota(jnp.int32, shape, dim)


def roll(x, shift, axis):
    size = x.shape[axis]
    shift = shift % size
    return x if shift == 0 else pltpu.roll(x, shift, axis)


def swap(field):
    x = field.reshape(32, 8, 128)
    s, l = iota((1, 8, 128), 1), iota((1, 8, 128), 2)
    s1, l1 = (s // 2) % 2, l // 64
    r = roll(x, 64, 2)
    x = jnp.where(s1 == l1, x, jnp.where(s1 == 0, roll(r, -2, 1), roll(r, 2, 1)))
    s0, l0 = s % 2, (l // 32) % 2
    up, down = roll(roll(x, 32, 2), -1, 1), roll(roll(x, -32, 2), 1, 1)
    x = jnp.where(s0 == l0, x, jnp.where(s0 == 0, up, down))
    even = jnp.concatenate([x[t * 4 : t * 4 + 4] for t in range(0, 8, 2)], axis=0)
    odd = jnp.concatenate([x[t * 4 : t * 4 + 4] for t in range(1, 8, 2)], axis=0)
    half = s < 4
    top = jnp.where(half, even, roll(odd, 4, 1))
    bottom = jnp.where(half, roll(even, 4, 1), odd)
    parts = []
    for ai in range(4):
        for part in (top, bottom):
            for k in range(4):
                parts.append(part[k * 4 + ai : k * 4 + ai + 1])
    return jnp.concatenate(parts, axis=0).reshape(256, 128)


def wide(field):
    return jnp.concatenate([field[t * 32 : t * 32 + 32] for t in range(8)], axis=1)


def tall(field):
    return jnp.concatenate([field[:, t * 128 : t * 128 + 128] for t in range(8)], axis=0)


def dot(left, right):
    return lax.dot_general(
        left,
        right,
        (((1,), (0,)), ((), ())),
        precision=lax.Precision.HIGHEST,
        preferred_element_type=F32,
    )


def matvec(field, xmat_ref, ymat_ref, zmat_ref):
    first = dot(xmat_ref[...], wide(field))
    mass, stiff = swap(tall(first[:C])), swap(tall(first[C:]))
    second = dot(ymat_ref[...], jnp.concatenate([wide(stiff), wide(mass)], axis=0))
    third = jnp.concatenate([tall(second[:C]), tall(second[C:])], axis=1)
    return swap(dot(third, zmat_ref[...]))


def block_diagonal(matrix):
    zero = jnp.zeros((C, C), F32)
    rows = []
    for i in range(4):
        rows.append(jnp.concatenate([matrix if k == i else zero for k in range(4)], axis=1))
    return jnp.concatenate(rows, axis=0)


def weight_field(sizes, here):
    row, lane = iota((256, 128), 0), iota((256, 128), 1)
    places = (row % C, (row // C) * 4 + lane // C, lane % C)
    weight = jnp.ones((256, 128), F32)
    for place, size, at in zip(places, sizes, here):
        low = jnp.where(at > 0, 0.5, 1.0).astype(F32)
        high = jnp.where(at < size - 1, 0.5, 1.0).astype(F32)
        weight = weight * jnp.where(place == 0, low, jnp.where(place == C - 1, high, 1.0))
    return weight


def neighbour(sizes, here, step):
    fine = None
    for size, at, d in zip(sizes, here, step):
        if d != 0:
            inside = at > 0 if d < 0 else at < size - 1
            fine = inside if fine is None else jnp.logical_and(fine, inside)
    return fine, tuple(at + d for at, d in zip(here, step))


def pack(out_ref, send_ref):
    s, l = iota((8, 128), 0), iota((8, 128), 1)
    lower = lambda t, ai: out_ref[pl.ds(t * 32 + ai * 8, 8), :]
    zero = jnp.zeros((8, 128), F32)
    low, high = zero, zero
    for t in range(8):
        for ai in range(4):
            r = ai * 8 + t
            moved = roll(lower(t, ai), r, 1)
            low = jnp.where(l % C == r, moved, low)
            high = jnp.where(l % C == (r + C - 1) % C, moved, high)
    for dz, plane, base in ((-1, low, 0), (1, high, -31)):
        for dx in (-1, 0, 1):
            for dy in (-1, 0, 1):
                lanes = base - dx * 24 - dy * 103
                part = roll(roll(plane, lanes, 1), dx, 0)
                keep = None
                if dx != 0:
                    keep = (s == (7 if dx < 0 else 0)) & ((l % C) // 8 == (3 if dx < 0 else 0))
                if dy != 0:
                    mine = (l // C == (3 if dy < 0 else 0)) & (l % 8 == (7 if dy < 0 else 0))
                    keep = mine if keep is None else keep & mine
                send_ref[SLOT[(dx, dy, dz)]] = part if keep is None else jnp.where(keep, part, 0.0)
    for dx in (-1, 1):
        plane = out_ref[pl.ds(0 if dx < 0 else C - 1, 8, stride=C), :]
        send_ref[SLOT[(dx, 0, 0)]] = plane
        for dy in (-1, 1):
            part = roll(roll(plane, 96 if dy < 0 else 32, 1), dy, 0)
            keep = (s == (7 if dy < 0 else 0)) & (l // C == (3 if dy < 0 else 0))
            send_ref[SLOT[(dx, dy, 0)]] = jnp.where(keep, part, 0.0)
    for dy in (-1, 1):
        plane = zero
        for ai in range(4):
            piece = roll(lower(0 if dy < 0 else 7, ai), C * (ai + (0 if dy < 0 else 1)), 1)
            plane = jnp.where(l // C == ai, piece, plane)
        send_ref[SLOT[(0, dy, 0)]] = plane


def unpack(out_ref, got_ref):
    l = iota((8, 128), 1)
    near = (-1, 0, 1)
    for dx in (-1, 1):
        plane = sum(got_ref[SLOT[(dx, dy, 0)]] for dy in near)
        rows = pl.ds(C - 1 if dx < 0 else 0, 8, stride=C)
        out_ref[rows, :] = out_ref[rows, :] + plane
    low, high = (
        sum(got_ref[SLOT[(dx, dy, dz)]] for dx in near for dy in near) for dz in (1, -1)
    )
    first, last = got_ref[SLOT[(0, 1, 0)]], got_ref[SLOT[(0, -1, 0)]]
    for t in range(8):
        for ai in range(4):
            r = ai * 8 + t
            rows = pl.ds(t * 32 + ai * 8, 8)
            add = jnp.where(l % C == 0, roll(low, -r, 1), 0.0)
            add = add + jnp.where(l % C == C - 1, roll(high, 31 - r, 1), 0.0)
            if t == 0:
                add = add + jnp.where(l < C, roll(first, -C * ai, 1), 0.0)
            if t == 7:
                add = add + jnp.where(l >= 96, roll(last, 96 - C * ai, 1), 0.0)
            out_ref[rows, :] = out_ref[rows, :] + add


def kernel(
    sizes,
    start_ref,
    stencils_ref,
    basis_ref,
    coefficients_ref,
    out,
    vecs,
    images,
    weights,
    xmat,
    ymat,
    zmat,
    sends,
    gots,
    terms,
    coef,
    send_sem,
    got_sem,
    term_send,
    term_got,
):
    here = tuple(lax.axis_index(a) for a in AXES)
    nx, ny, nz = sizes
    gx, gy, gz = here
    me = (gx * ny + gy) * nz + gz
    hops = lambda k, size: min(k, size - k)
    steps = sorted(
        ((i, j, k) for i in range(nx) for j in range(ny) for k in range(nz)),
        key=lambda d: -(hops(d[0], nx) + hops(d[1], ny) + hops(d[2], nz) / 2),
    )
    along = [[lax.rem(at + k, size) for k in range(size)] for at, size in zip(here, sizes)]
    everyone = [tuple(along[a][d[a]] for a in range(3)) for d in steps if any(d)]
    spans = [
        1 + jnp.where(at > 0, 1, 0) + jnp.where(at < size - 1, 1, 0)
        for at, size in zip(here, sizes)
    ]
    degree = spans[0] * spans[1] * spans[2] - 1
    degrees = sorted(
        {
            i * j * k - 1
            for i in span_set(nx)
            for j in span_set(ny)
            for k in span_set(nz)
        }
    )

    gots[...] = jnp.zeros_like(gots)

    barrier = pltpu.get_barrier_semaphore()
    for d in DIRS:
        fine, there = neighbour(sizes, here, d)

        @pl.when(fine)
        def _():
            pl.semaphore_signal(barrier, inc=1, device_id=there, device_id_type=MESH)

    for there in everyone:
        pl.semaphore_signal(barrier, inc=1, device_id=there, device_id_type=MESH)

    vecs[...] = jnp.zeros_like(vecs)
    images[...] = jnp.zeros_like(images)
    coef[...] = jnp.zeros_like(coef)
    weights[...] = weight_field(sizes, here)
    kx, ky, kz, mx, my, mz = (stencils_ref[i] for i in range(6))
    xmat[...] = jnp.concatenate([mx, kx], axis=0)
    top = jnp.concatenate([my, ky], axis=1)
    ymat[...] = jnp.concatenate([top, jnp.concatenate([jnp.zeros((C, C), F32), my], axis=1)], axis=0)
    zmat[...] = jnp.concatenate([block_diagonal(mz.T), block_diagonal(kz.T)], axis=0)

    def exchange_start(par):
        pack(out, sends.at[par])
        if True:
            for d in sorted(DIRS, key=lambda d: -sum(abs(i) for i in d)):
                fine, there = neighbour(sizes, here, d)

                @pl.when(fine)
                def _():
                    pltpu.make_async_remote_copy(
                        src_ref=sends.at[par, SLOT[d]],
                        dst_ref=gots.at[par, SLOT[d]],
                        send_sem=send_sem.at[par],
                        recv_sem=got_sem.at[par],
                        device_id=there,
                        device_id_type=MESH,
                    ).start()

    def exchange_end(par):
        for n in degrees:

            @pl.when(degree == n)
            def _():
                both = pltpu.make_async_remote_copy(
                    src_ref=sends.at[par, pl.ds(0, n)],
                    dst_ref=gots.at[par, pl.ds(0, n)],
                    send_sem=send_sem.at[par],
                    recv_sem=got_sem.at[par],
                    device_id=everyone[0],
                    device_id_type=MESH,
                )
                both.wait_recv()
                both.wait_send()

        unpack(out, gots.at[par])

    def products(image):
        weighted = weights[...] * image
        pairs = [(vecs[i], weighted) for i in range(ITERS)]
        pairs += [(image, weighted), (vecs[0], weights[...] * vecs[0])]
        s, l = iota((8, 128), 0), iota((8, 128), 1)
        tile = jnp.zeros((8, 128), F32)
        for k, (left, right) in enumerate(pairs):
            lanes = jnp.sum(jnp.sum((left * right).reshape(32, 8, 128), axis=0), axis=0, keepdims=True)
            tile = jnp.where(s == k, lanes, tile)
        column = jnp.sum(tile, axis=1, keepdims=True)
        return jnp.sum(jnp.where(s == l, column, 0.0), axis=0, keepdims=True)

    def products_start(par, image):
        mine = pl.ds(me, 1)
        terms[par, mine] = products(image)
        for there in everyone:
            pltpu.make_async_remote_copy(
                src_ref=terms.at[par, mine],
                dst_ref=terms.at[par, mine],
                send_sem=term_send.at[par],
                recv_sem=term_got.at[par],
                device_id=there,
                device_id_type=MESH,
            ).start()

    def products_end(par):
        others = pl.ds(0, len(everyone))
        both = pltpu.make_async_remote_copy(
            src_ref=terms.at[par, others],
            dst_ref=terms.at[par, others],
            send_sem=term_send.at[par],
            recv_sem=term_got.at[par],
            device_id=everyone[0],
            device_id_type=MESH,
        )
        both.wait_recv()
        both.wait_send()
        row = jnp.sum(terms[par], axis=0, keepdims=True)
        s, l = iota((8, 128), 0), iota((8, 128), 1)
        return jnp.sum(jnp.where(s == l, row, 0.0), axis=1, keepdims=True)

    def advance(j, totals, following):
        first = j == 0
        inverse = jnp.where(first, lax.rsqrt(totals[6:7]), 1.0)
        square = jnp.where(first, 1.0 / totals[6:7], 1.0)

        @pl.when(first)
        def _():
            vecs[0] = vecs[0] * inverse
            images[0] = images[0] * inverse

        heights = [totals[i : i + 1] * square for i in range(ITERS)]
        length = totals[5:6] * square
        beta = jnp.sqrt(length - sum(h * h for h in heights))
        alpha = sum(jnp.where(j == i, heights[i], 0.0) for i in range(ITERS))
        over = 1.0 / beta
        new = images[j]
        for i in range(ITERS):
            new = new - heights[i] * vecs[i]
        vecs[j + 1] = new * over
        s, l = iota((8, 128), 0), iota((8, 128), 1)
        entry = jnp.where(s == 0, alpha, jnp.where(s == 1, beta, 0.0))
        coef[...] = coef[...] + jnp.where(l == j, entry, 0.0)
        if following:
            image = out[...] * inverse
            for i in range(ITERS):
                image = image - heights[i] * images[i]
            images[j + 1] = image * over

    out[...] = tall(start_ref[...]) * weights[...] * SHRINK
    pl.semaphore_wait(barrier, degree + len(everyone))
    exchange_start(0)
    exchange_end(0)
    vecs[0] = out[...]
    out[...] = matvec(out[...], xmat, ymat, zmat)
    exchange_start(1)
    exchange_end(1)
    images[0] = out[...]

    def body(j, carry):
        par = lax.rem(j, 2)
        image = images[j]
        products_start(par, image)
        out[...] = matvec(image, xmat, ymat, zmat)
        exchange_start(par)
        exchange_end(par)
        advance(j, products_end(par), True)
        return carry

    lax.fori_loop(0, ITERS - 1, body, 0)
    par = (ITERS - 1) % 2
    products_start(par, images[ITERS - 1])
    advance(ITERS - 1, products_end(par), False)
    for i in range(ITERS):
        basis_ref[i] = wide(vecs[i + 1])
    coefficients_ref[...] = coef[0:2, 0:ITERS]


def span_set(size):
    return {1} if size == 1 else {2} if size == 2 else {2, 3}


def shards(sizes, start, stencils):
    nx, ny, nz = sizes
    vmem = pl.BlockSpec(memory_space=pltpu.VMEM)
    basis, coefficients = pl.pallas_call(
        functools.partial(kernel, sizes),
        out_shape=(
            jax.ShapeDtypeStruct((ITERS, C, C * C), F32),
            jax.ShapeDtypeStruct((2, ITERS), F32),
        ),
        in_specs=[vmem, vmem],
        out_specs=(vmem, vmem),
        scratch_shapes=[
            pltpu.VMEM((256, 128), F32),
            pltpu.VMEM((ITERS + 1, 256, 128), F32),
            pltpu.VMEM((ITERS, 256, 128), F32),
            pltpu.VMEM((256, 128), F32),
            pltpu.VMEM((2 * C, C), F32),
            pltpu.VMEM((2 * C, 2 * C), F32),
            pltpu.VMEM((256, 128), F32),
            pltpu.VMEM((2, len(DIRS), 8, 128), F32),
            pltpu.VMEM((2, len(DIRS), 8, 128), F32),
            pltpu.VMEM((2, nx * ny * nz, 128), F32),
            pltpu.VMEM((8, 128), F32),
        ]
        + [pltpu.SemaphoreType.DMA((2,))] * 4,
        compiler_params=pltpu.CompilerParams(collective_id=0, has_side_effects=True),
    )(start.reshape(C, C * C), stencils.reshape(6, C, C))
    return (
        basis.reshape(1, 1, 1, 1, ITERS, C, C * C),
        coefficients.reshape(1, 2, ITERS),
    )


def solution(mesh):
    sizes = tuple(mesh.shape[a] for a in AXES)
    return jax.shard_map(
        functools.partial(shards, sizes),
        mesh=mesh,
        in_specs=(P("gx", "gy", "gz", None, None, None), P(None, "gx", "gy", "gz", None, None)),
        out_specs=(P("gx", "gy", "gz", None, None, None, None), P()),
        check_vma=False,
    )
```

```python
import functools

import jax
import jax.numpy as jnp
from jax import lax
from jax.experimental import pallas as pl
from jax.experimental.pallas import tpu as pltpu
from jax.sharding import PartitionSpec as P

ITERS = 5
C = 32
MESH = pl.DeviceIdType.MESH
F32 = jnp.float32
AXES = ("gx", "gy", "gz")
DIRS = [
    (dx, dy, dz)
    for dx in (-1, 0, 1)
    for dy in (-1, 0, 1)
    for dz in (-1, 0, 1)
    if (dx, dy, dz) != (0, 0, 0)
]
SLOT = {d: i for i, d in enumerate(DIRS)}
SHRINK = 2.0**-17


def iota(shape, dim):
    return lax.broadcasted_iota(jnp.int32, shape, dim)


def roll(x, shift, axis):
    size = x.shape[axis]
    shift = shift % size
    return x if shift == 0 else pltpu.roll(x, shift, axis)


def swap(field):
    x = field.reshape(32, 8, 128)
    s, l = iota((1, 8, 128), 1), iota((1, 8, 128), 2)
    s1, l1 = (s // 2) % 2, l // 64
    r = roll(x, 64, 2)
    x = jnp.where(s1 == l1, x, jnp.where(s1 == 0, roll(r, -2, 1), roll(r, 2, 1)))
    s0, l0 = s % 2, (l // 32) % 2
    up, down = roll(roll(x, 32, 2), -1, 1), roll(roll(x, -32, 2), 1, 1)
    x = jnp.where(s0 == l0, x, jnp.where(s0 == 0, up, down))
    even = jnp.concatenate([x[t * 4 : t * 4 + 4] for t in range(0, 8, 2)], axis=0)
    odd = jnp.concatenate([x[t * 4 : t * 4 + 4] for t in range(1, 8, 2)], axis=0)
    half = s < 4
    top = jnp.where(half, even, roll(odd, 4, 1))
    bottom = jnp.where(half, roll(even, 4, 1), odd)
    parts = []
    for ai in range(4):
        for part in (top, bottom):
            for k in range(4):
                parts.append(part[k * 4 + ai : k * 4 + ai + 1])
    return jnp.concatenate(parts, axis=0).reshape(256, 128)


def wide(field):
    return jnp.concatenate([field[t * 32 : t * 32 + 32] for t in range(8)], axis=1)


def tall(field):
    return jnp.concatenate([field[:, t * 128 : t * 128 + 128] for t in range(8)], axis=0)


def dot(left, right):
    return lax.dot_general(
        left,
        right,
        (((1,), (0,)), ((), ())),
        precision=lax.Precision.HIGHEST,
        preferred_element_type=F32,
    )


def matvec(field, xmat_ref, ymat_ref, zmat_ref):
    first = dot(xmat_ref[...], wide(field))
    mass, stiff = swap(tall(first[:C])), swap(tall(first[C:]))
    second = dot(ymat_ref[...], jnp.concatenate([wide(stiff), wide(mass)], axis=0))
    third = jnp.concatenate([tall(second[:C]), tall(second[C:])], axis=1)
    return swap(dot(third, zmat_ref[...]))


def block_diagonal(matrix):
    zero = jnp.zeros((C, C), F32)
    rows = []
    for i in range(4):
        rows.append(jnp.concatenate([matrix if k == i else zero for k in range(4)], axis=1))
    return jnp.concatenate(rows, axis=0)


def weight_field(sizes, here):
    row, lane = iota((256, 128), 0), iota((256, 128), 1)
    places = (row % C, (row // C) * 4 + lane // C, lane % C)
    weight = jnp.ones((256, 128), F32)
    for place, size, at in zip(places, sizes, here):
        low = jnp.where(at > 0, 0.5, 1.0).astype(F32)
        high = jnp.where(at < size - 1, 0.5, 1.0).astype(F32)
        weight = weight * jnp.where(place == 0, low, jnp.where(place == C - 1, high, 1.0))
    return weight


def neighbour(sizes, here, step):
    fine = None
    for size, at, d in zip(sizes, here, step):
        if d != 0:
            inside = at > 0 if d < 0 else at < size - 1
            fine = inside if fine is None else jnp.logical_and(fine, inside)
    return fine, tuple(at + d for at, d in zip(here, step))


def axis_leaps(size, at, step):
    if size <= step + 1:
        return []
    if size == 2 * step:
        return [(True, lax.rem(at + step, size))]
    return [(at >= step, at - step), (at < size - step, at + step)]


def leaps(sizes, here, step):
    choices = [[(True, at)] + axis_leaps(size, at, step) for size, at in zip(sizes, here)]
    found = []
    for i, x in enumerate(choices[0]):
        for j, y in enumerate(choices[1]):
            for k, z in enumerate(choices[2]):
                if i + j + k > 0:
                    tests = [c[0] for c in (x, y, z) if c[0] is not True]
                    fine = functools.reduce(jnp.logical_and, tests) if tests else True
                    found.append((fine, (x[1], y[1], z[1])))
    return found


def leap_count(sizes, here, step):
    total = 1
    for size, at in zip(sizes, here):
        count = 1
        for fine, _ in axis_leaps(size, at, step):
            count = count + (1 if fine is True else jnp.where(fine, 1, 0))
        total = total * count
    return total - 1


def pack(out_ref, send_ref):
    s, l = iota((8, 128), 0), iota((8, 128), 1)
    lower = lambda t, ai: out_ref[pl.ds(t * 32 + ai * 8, 8), :]
    zero = jnp.zeros((8, 128), F32)
    low, high = zero, zero
    for t in range(8):
        for ai in range(4):
            r = ai * 8 + t
            moved = roll(lower(t, ai), r, 1)
            low = jnp.where(l % C == r, moved, low)
            high = jnp.where(l % C == (r + C - 1) % C, moved, high)
    for dz, plane, base in ((-1, low, 0), (1, high, -31)):
        for dx in (-1, 0, 1):
            for dy in (-1, 0, 1):
                lanes = base - dx * 24 - dy * 103
                part = roll(roll(plane, lanes, 1), dx, 0)
                keep = None
                if dx != 0:
                    keep = (s == (7 if dx < 0 else 0)) & ((l % C) // 8 == (3 if dx < 0 else 0))
                if dy != 0:
                    mine = (l // C == (3 if dy < 0 else 0)) & (l % 8 == (7 if dy < 0 else 0))
                    keep = mine if keep is None else keep & mine
                send_ref[SLOT[(dx, dy, dz)]] = part if keep is None else jnp.where(keep, part, 0.0)
    for dx in (-1, 1):
        plane = out_ref[pl.ds(0 if dx < 0 else C - 1, 8, stride=C), :]
        send_ref[SLOT[(dx, 0, 0)]] = plane
        for dy in (-1, 1):
            part = roll(roll(plane, 96 if dy < 0 else 32, 1), dy, 0)
            keep = (s == (7 if dy < 0 else 0)) & (l // C == (3 if dy < 0 else 0))
            send_ref[SLOT[(dx, dy, 0)]] = jnp.where(keep, part, 0.0)
    for dy in (-1, 1):
        plane = zero
        for ai in range(4):
            piece = roll(lower(0 if dy < 0 else 7, ai), C * (ai + (0 if dy < 0 else 1)), 1)
            plane = jnp.where(l // C == ai, piece, plane)
        send_ref[SLOT[(0, dy, 0)]] = plane


def unpack(out_ref, got_ref):
    l = iota((8, 128), 1)
    near = (-1, 0, 1)
    for dx in (-1, 1):
        plane = sum(got_ref[SLOT[(dx, dy, 0)]] for dy in near)
        rows = pl.ds(C - 1 if dx < 0 else 0, 8, stride=C)
        out_ref[rows, :] = out_ref[rows, :] + plane
    low, high = (
        sum(got_ref[SLOT[(dx, dy, dz)]] for dx in near for dy in near) for dz in (1, -1)
    )
    first, last = got_ref[SLOT[(0, 1, 0)]], got_ref[SLOT[(0, -1, 0)]]
    for t in range(8):
        for ai in range(4):
            r = ai * 8 + t
            rows = pl.ds(t * 32 + ai * 8, 8)
            add = jnp.where(l % C == 0, roll(low, -r, 1), 0.0)
            add = add + jnp.where(l % C == C - 1, roll(high, 31 - r, 1), 0.0)
            if t == 0:
                add = add + jnp.where(l < C, roll(first, -C * ai, 1), 0.0)
            if t == 7:
                add = add + jnp.where(l >= 96, roll(last, 96 - C * ai, 1), 0.0)
            out_ref[rows, :] = out_ref[rows, :] + add


def kernel(
    sizes,
    start_hbm,
    stencils_hbm,
    basis_ref,
    coefficients_ref,
    start_ref,
    stencils_ref,
    wides,
    small,
    out,
    vecs,
    images,
    weights,
    xmat,
    ymat,
    zmat,
    sends,
    gots,
    terms,
    coef,
    send_sem,
    got_sem,
    term_send,
    term_got,
    in_sem,
    out_sem,
    near,
    far,
):
    here = tuple(lax.axis_index(a) for a in AXES)
    nx, ny, nz = sizes
    gx, gy, gz = here
    me = (gx * ny + gy) * nz + gz
    hops = lambda k, size: min(k, size - k)
    steps = sorted(
        ((i, j, k) for i in range(nx) for j in range(ny) for k in range(nz)),
        key=lambda d: -(hops(d[0], nx) + hops(d[1], ny) + hops(d[2], nz) / 2),
    )
    along = [[lax.rem(at + k, size) for k in range(size)] for at, size in zip(here, sizes)]
    everyone = [tuple(along[a][d[a]] for a in range(3)) for d in steps if any(d)]
    spans = [
        1 + jnp.where(at > 0, 1, 0) + jnp.where(at < size - 1, 1, 0)
        for at, size in zip(here, sizes)
    ]
    degree = spans[0] * spans[1] * spans[2] - 1
    degrees = sorted(
        {
            i * j * k - 1
            for i in span_set(nx)
            for j in span_set(ny)
            for k in span_set(nz)
        }
    )

    inputs = [
        pltpu.make_async_copy(start_hbm, start_ref, in_sem.at[0]),
        pltpu.make_async_copy(stencils_hbm, stencils_ref, in_sem.at[1]),
    ]
    for copy in inputs:
        copy.start()
    gots[...] = jnp.zeros_like(gots)
    barrier = pltpu.get_barrier_semaphore()
    for d in DIRS:
        fine, there = neighbour(sizes, here, d)

        @pl.when(fine)
        def _():
            pl.semaphore_signal(barrier, inc=1, device_id=there, device_id_type=MESH)

    vecs[...] = jnp.zeros_like(vecs)
    images[...] = jnp.zeros_like(images)
    coef[...] = jnp.zeros_like(coef)
    weights[...] = weight_field(sizes, here)
    for copy in inputs:
        copy.wait()
    kx, ky, kz, mx, my, mz = (stencils_ref[i] for i in range(6))
    xmat[...] = jnp.concatenate([mx, kx], axis=0)
    top = jnp.concatenate([my, ky], axis=1)
    ymat[...] = jnp.concatenate([top, jnp.concatenate([jnp.zeros((C, C), F32), my], axis=1)], axis=0)
    zmat[...] = jnp.concatenate([block_diagonal(mz.T), block_diagonal(kz.T)], axis=0)

    def greet(fine, there, semaphore):
        def signal():
            pl.semaphore_signal(semaphore, inc=1, device_id=there, device_id_type=MESH)

        if fine is True:
            signal()
        else:
            pl.when(fine)(signal)

    def exchange_start(par):
        pack(out, sends.at[par])
        if True:
            for d in sorted(DIRS, key=lambda d: -sum(abs(i) for i in d)):
                fine, there = neighbour(sizes, here, d)

                @pl.when(fine)
                def _():
                    pltpu.make_async_remote_copy(
                        src_ref=sends.at[par, SLOT[d]],
                        dst_ref=gots.at[par, SLOT[d]],
                        send_sem=send_sem.at[par],
                        recv_sem=got_sem.at[par],
                        device_id=there,
                        device_id_type=MESH,
                    ).start()

    def exchange_end(par):
        for n in degrees:

            @pl.when(degree == n)
            def _():
                both = pltpu.make_async_remote_copy(
                    src_ref=sends.at[par, pl.ds(0, n)],
                    dst_ref=gots.at[par, pl.ds(0, n)],
                    send_sem=send_sem.at[par],
                    recv_sem=got_sem.at[par],
                    device_id=everyone[0],
                    device_id_type=MESH,
                )
                both.wait_recv()
                both.wait_send()

        unpack(out, gots.at[par])

    def products(image):
        weighted = weights[...] * image
        pairs = [(vecs[i], weighted) for i in range(ITERS)]
        pairs += [(image, weighted), (vecs[0], weights[...] * vecs[0])]
        s, l = iota((8, 128), 0), iota((8, 128), 1)
        tile = jnp.zeros((8, 128), F32)
        for k, (left, right) in enumerate(pairs):
            lanes = jnp.sum(jnp.sum((left * right).reshape(32, 8, 128), axis=0), axis=0, keepdims=True)
            tile = jnp.where(s == k, lanes, tile)
        column = jnp.sum(tile, axis=1, keepdims=True)
        return jnp.sum(jnp.where(s == l, column, 0.0), axis=0, keepdims=True)

    def products_start(par, image):
        mine = pl.ds(me, 1)
        terms[par, mine] = products(image)
        for there in everyone:
            pltpu.make_async_remote_copy(
                src_ref=terms.at[par, mine],
                dst_ref=terms.at[par, mine],
                send_sem=term_send.at[par],
                recv_sem=term_got.at[par],
                device_id=there,
                device_id_type=MESH,
            ).start()

    def products_end(par):
        others = pl.ds(0, len(everyone))
        both = pltpu.make_async_remote_copy(
            src_ref=terms.at[par, others],
            dst_ref=terms.at[par, others],
            send_sem=term_send.at[par],
            recv_sem=term_got.at[par],
            device_id=everyone[0],
            device_id_type=MESH,
        )
        both.wait_recv()
        both.wait_send()
        row = jnp.sum(terms[par], axis=0, keepdims=True)
        s, l = iota((8, 128), 0), iota((8, 128), 1)
        return jnp.sum(jnp.where(s == l, row, 0.0), axis=1, keepdims=True)

    def advance(j, totals, following):
        first = j == 0
        inverse = jnp.where(first, lax.rsqrt(totals[6:7]), 1.0)
        square = jnp.where(first, 1.0 / totals[6:7], 1.0)

        @pl.when(first)
        def _():
            vecs[0] = vecs[0] * inverse
            images[0] = images[0] * inverse

        heights = [totals[i : i + 1] * square for i in range(ITERS)]
        length = totals[5:6] * square
        beta = jnp.sqrt(length - sum(h * h for h in heights))
        alpha = sum(jnp.where(j == i, heights[i], 0.0) for i in range(ITERS))
        over = 1.0 / beta
        new = images[j]
        for i in range(ITERS):
            new = new - heights[i] * vecs[i]
        vecs[j + 1] = new * over
        s, l = iota((8, 128), 0), iota((8, 128), 1)
        entry = jnp.where(s == 0, alpha, jnp.where(s == 1, beta, 0.0))
        coef[...] = coef[...] + jnp.where(l == j, entry, 0.0)
        if following:
            image = out[...] * inverse
            for i in range(ITERS):
                image = image - heights[i] * images[i]
            images[j + 1] = image * over

    def leaving(i):
        return pltpu.make_async_copy(wides.at[i - 1], basis_ref.at[i - 1], out_sem.at[i - 1])

    def leave(i):
        wides[i - 1] = wide(vecs[i])
        return leaving(i)

    out[...] = tall(start_ref[...]) * weights[...] * SHRINK
    pl.semaphore_wait(barrier, degree)
    exchange_start(0)
    exchange_end(0)
    for fine, there in leaps(sizes, here, 2):
        greet(fine, there, near)
    vecs[0] = out[...]
    out[...] = matvec(out[...], xmat, ymat, zmat)
    pl.semaphore_wait(near, leap_count(sizes, here, 2))
    for fine, there in leaps(sizes, here, 4):
        greet(fine, there, far)
    exchange_start(1)
    pl.semaphore_wait(far, leap_count(sizes, here, 4))
    exchange_end(1)
    images[0] = out[...]

    def body(j, carry):
        par = lax.rem(j, 2)
        image = images[j]
        products_start(par, image)
        out[...] = matvec(image, xmat, ymat, zmat)
        exchange_start(par)

        @pl.when(j > 0)
        def _():
            leave(j).start()

        exchange_end(par)
        advance(j, products_end(par), True)
        return carry

    lax.fori_loop(0, ITERS - 1, body, 0)
    par = (ITERS - 1) % 2
    products_start(par, images[ITERS - 1])
    leave(ITERS - 1).start()
    advance(ITERS - 1, products_end(par), False)
    leave(ITERS).start()
    small[...] = coef[0:2, 0:ITERS]
    last = pltpu.make_async_copy(small, coefficients_ref, out_sem.at[ITERS])
    last.start()
    for i in range(1, ITERS + 1):
        leaving(i).wait()
    last.wait()


def span_set(size):
    return {1} if size == 1 else {2} if size == 2 else {2, 3}


def shards(sizes, start, stencils):
    nx, ny, nz = sizes
    hbm = pl.BlockSpec(memory_space=pltpu.HBM)
    anyw = pl.BlockSpec(memory_space=pl.ANY)
    basis, coefficients = pl.pallas_call(
        functools.partial(kernel, sizes),
        out_shape=(
            jax.ShapeDtypeStruct((ITERS, C, C * C), F32),
            jax.ShapeDtypeStruct((2, ITERS), F32),
        ),
        in_specs=[hbm, hbm],
        out_specs=(anyw, anyw),
        scratch_shapes=[
            pltpu.VMEM((C, C * C), F32),
            pltpu.VMEM((6, C, C), F32),
            pltpu.VMEM((ITERS, C, C * C), F32),
            pltpu.VMEM((2, ITERS), F32),
            pltpu.VMEM((256, 128), F32),
            pltpu.VMEM((ITERS + 1, 256, 128), F32),
            pltpu.VMEM((ITERS, 256, 128), F32),
            pltpu.VMEM((256, 128), F32),
            pltpu.VMEM((2 * C, C), F32),
            pltpu.VMEM((2 * C, 2 * C), F32),
            pltpu.VMEM((256, 128), F32),
            pltpu.VMEM((2, len(DIRS), 8, 128), F32),
            pltpu.VMEM((2, len(DIRS), 8, 128), F32),
            pltpu.VMEM((2, nx * ny * nz, 128), F32),
            pltpu.VMEM((8, 128), F32),
        ]
        + [pltpu.SemaphoreType.DMA((2,))] * 5
        + [pltpu.SemaphoreType.DMA((ITERS + 1,)), pltpu.SemaphoreType.REGULAR, pltpu.SemaphoreType.REGULAR],
        compiler_params=pltpu.CompilerParams(collective_id=0, has_side_effects=True),
    )(start.reshape(C, C * C), stencils.reshape(6, C, C))
    return (
        basis.reshape(1, 1, 1, 1, ITERS, C, C * C),
        coefficients.reshape(1, 2, ITERS),
    )


def solution(mesh):
    sizes = tuple(mesh.shape[a] for a in AXES)
    return jax.shard_map(
        functools.partial(shards, sizes),
        mesh=mesh,
        in_specs=(P("gx", "gy", "gz", None, None, None), P(None, "gx", "gy", "gz", None, None)),
        out_specs=(P("gx", "gy", "gz", None, None, None, None), P()),
        check_vma=False,
    )
```

```python
import functools

import jax
import jax.numpy as jnp
from jax import lax
from jax.experimental import pallas as pl
from jax.experimental.pallas import tpu as pltpu
from jax.sharding import PartitionSpec as P

ITERS = 5
C = 32
MESH = pl.DeviceIdType.MESH
F32 = jnp.float32
AXES = ("gx", "gy", "gz")
DIRS = [
    (dx, dy, dz)
    for dx in (-1, 0, 1)
    for dy in (-1, 0, 1)
    for dz in (-1, 0, 1)
    if (dx, dy, dz) != (0, 0, 0)
]
SLOT = {d: i for i, d in enumerate(DIRS)}
SHRINK = 2.0**-17


def iota(shape, dim):
    return lax.broadcasted_iota(jnp.int32, shape, dim)


def roll(x, shift, axis):
    size = x.shape[axis]
    shift = shift % size
    return x if shift == 0 else pltpu.roll(x, shift, axis)


def swap(field):
    x = field.reshape(32, 8, 128)
    s, l = iota((1, 8, 128), 1), iota((1, 8, 128), 2)
    s1, l1 = (s // 2) % 2, l // 64
    r = roll(x, 64, 2)
    x = jnp.where(s1 == l1, x, jnp.where(s1 == 0, roll(r, -2, 1), roll(r, 2, 1)))
    s0, l0 = s % 2, (l // 32) % 2
    up, down = roll(roll(x, 32, 2), -1, 1), roll(roll(x, -32, 2), 1, 1)
    x = jnp.where(s0 == l0, x, jnp.where(s0 == 0, up, down))
    even = jnp.concatenate([x[t * 4 : t * 4 + 4] for t in range(0, 8, 2)], axis=0)
    odd = jnp.concatenate([x[t * 4 : t * 4 + 4] for t in range(1, 8, 2)], axis=0)
    half = s < 4
    top = jnp.where(half, even, roll(odd, 4, 1))
    bottom = jnp.where(half, roll(even, 4, 1), odd)
    parts = []
    for ai in range(4):
        for part in (top, bottom):
            for k in range(4):
                parts.append(part[k * 4 + ai : k * 4 + ai + 1])
    return jnp.concatenate(parts, axis=0).reshape(256, 128)


def wide(field):
    return jnp.concatenate([field[t * 32 : t * 32 + 32] for t in range(8)], axis=1)


def tall(field):
    return jnp.concatenate([field[:, t * 128 : t * 128 + 128] for t in range(8)], axis=0)


def dot(left, right):
    return lax.dot_general(
        left,
        right,
        (((1,), (0,)), ((), ())),
        precision=lax.Precision.HIGHEST,
        preferred_element_type=F32,
    )


def matvec(field, xmat_ref, ymat_ref, zmat_ref):
    first = dot(xmat_ref[...], wide(field))
    mass, stiff = swap(tall(first[:C])), swap(tall(first[C:]))
    second = dot(ymat_ref[...], jnp.concatenate([wide(stiff), wide(mass)], axis=0))
    third = jnp.concatenate([tall(second[:C]), tall(second[C:])], axis=1)
    return swap(dot(third, zmat_ref[...]))


def block_diagonal(matrix):
    zero = jnp.zeros((C, C), F32)
    rows = []
    for i in range(4):
        rows.append(jnp.concatenate([matrix if k == i else zero for k in range(4)], axis=1))
    return jnp.concatenate(rows, axis=0)


def weight_field(sizes, here):
    row, lane = iota((256, 128), 0), iota((256, 128), 1)
    places = (row % C, (row // C) * 4 + lane // C, lane % C)
    weight = jnp.ones((256, 128), F32)
    for place, size, at in zip(places, sizes, here):
        low = jnp.where(at > 0, 0.5, 1.0).astype(F32)
        high = jnp.where(at < size - 1, 0.5, 1.0).astype(F32)
        weight = weight * jnp.where(place == 0, low, jnp.where(place == C - 1, high, 1.0))
    return weight


def neighbour(sizes, here, step):
    fine = None
    for size, at, d in zip(sizes, here, step):
        if d != 0:
            inside = at > 0 if d < 0 else at < size - 1
            fine = inside if fine is None else jnp.logical_and(fine, inside)
    return fine, tuple(at + d for at, d in zip(here, step))


def pack(out_ref, send_ref):
    s, l = iota((8, 128), 0), iota((8, 128), 1)
    lower = lambda t, ai: out_ref[pl.ds(t * 32 + ai * 8, 8), :]
    zero = jnp.zeros((8, 128), F32)
    low, high = zero, zero
    for t in range(8):
        for ai in range(4):
            r = ai * 8 + t
            moved = roll(lower(t, ai), r, 1)
            low = jnp.where(l % C == r, moved, low)
            high = jnp.where(l % C == (r + C - 1) % C, moved, high)
    for dz, plane, base in ((-1, low, 0), (1, high, -31)):
        for dx in (-1, 0, 1):
            for dy in (-1, 0, 1):
                lanes = base - dx * 24 - dy * 103
                part = roll(roll(plane, lanes, 1), dx, 0)
                keep = None
                if dx != 0:
                    keep = (s == (7 if dx < 0 else 0)) & ((l % C) // 8 == (3 if dx < 0 else 0))
                if dy != 0:
                    mine = (l // C == (3 if dy < 0 else 0)) & (l % 8 == (7 if dy < 0 else 0))
                    keep = mine if keep is None else keep & mine
                send_ref[SLOT[(dx, dy, dz)]] = part if keep is None else jnp.where(keep, part, 0.0)
    for dx in (-1, 1):
        plane = out_ref[pl.ds(0 if dx < 0 else C - 1, 8, stride=C), :]
        send_ref[SLOT[(dx, 0, 0)]] = plane
        for dy in (-1, 1):
            part = roll(roll(plane, 96 if dy < 0 else 32, 1), dy, 0)
            keep = (s == (7 if dy < 0 else 0)) & (l // C == (3 if dy < 0 else 0))
            send_ref[SLOT[(dx, dy, 0)]] = jnp.where(keep, part, 0.0)
    for dy in (-1, 1):
        plane = zero
        for ai in range(4):
            piece = roll(lower(0 if dy < 0 else 7, ai), C * (ai + (0 if dy < 0 else 1)), 1)
            plane = jnp.where(l // C == ai, piece, plane)
        send_ref[SLOT[(0, dy, 0)]] = plane


def unpack(out_ref, got_ref):
    l = iota((8, 128), 1)
    near = (-1, 0, 1)
    for dx in (-1, 1):
        plane = sum(got_ref[SLOT[(dx, dy, 0)]] for dy in near)
        rows = pl.ds(C - 1 if dx < 0 else 0, 8, stride=C)
        out_ref[rows, :] = out_ref[rows, :] + plane
    low, high = (
        sum(got_ref[SLOT[(dx, dy, dz)]] for dx in near for dy in near) for dz in (1, -1)
    )
    first, last = got_ref[SLOT[(0, 1, 0)]], got_ref[SLOT[(0, -1, 0)]]
    for t in range(8):
        for ai in range(4):
            r = ai * 8 + t
            rows = pl.ds(t * 32 + ai * 8, 8)
            add = jnp.where(l % C == 0, roll(low, -r, 1), 0.0)
            add = add + jnp.where(l % C == C - 1, roll(high, 31 - r, 1), 0.0)
            if t == 0:
                add = add + jnp.where(l < C, roll(first, -C * ai, 1), 0.0)
            if t == 7:
                add = add + jnp.where(l >= 96, roll(last, 96 - C * ai, 1), 0.0)
            out_ref[rows, :] = out_ref[rows, :] + add


def kernel(
    sizes,
    start_hbm,
    stencils_hbm,
    basis_ref,
    coefficients_ref,
    start_ref,
    stencils_ref,
    wides,
    small,
    out,
    powers,
    vecs,
    weights,
    xmat,
    ymat,
    zmat,
    sends,
    gots,
    terms,
    send_sem,
    got_sem,
    term_send,
    term_got,
    in_sem,
    out_sem,
):
    here = tuple(lax.axis_index(a) for a in AXES)
    nx, ny, nz = sizes
    gx, gy, gz = here
    me = (gx * ny + gy) * nz + gz
    hops = lambda k, size: min(k, size - k)
    steps = sorted(
        ((i, j, k) for i in range(nx) for j in range(ny) for k in range(nz)),
        key=lambda d: -(hops(d[0], nx) + hops(d[1], ny) + hops(d[2], nz) / 2),
    )
    along = [[lax.rem(at + k, size) for k in range(size)] for at, size in zip(here, sizes)]
    everyone = [tuple(along[a][d[a]] for a in range(3)) for d in steps if any(d)]
    spans = [
        1 + jnp.where(at > 0, 1, 0) + jnp.where(at < size - 1, 1, 0)
        for at, size in zip(here, sizes)
    ]
    degree = spans[0] * spans[1] * spans[2] - 1
    degrees = sorted(
        {
            i * j * k - 1
            for i in span_set(nx)
            for j in span_set(ny)
            for k in span_set(nz)
        }
    )

    inputs = [
        pltpu.make_async_copy(start_hbm, start_ref, in_sem.at[0]),
        pltpu.make_async_copy(stencils_hbm, stencils_ref, in_sem.at[1]),
    ]
    for copy in inputs:
        copy.start()
    gots[...] = jnp.zeros_like(gots)
    barrier = pltpu.get_barrier_semaphore()
    for there in everyone:
        pl.semaphore_signal(barrier, inc=1, device_id=there, device_id_type=MESH)

    weights[...] = weight_field(sizes, here)
    for copy in inputs:
        copy.wait()
    kx, ky, kz, mx, my, mz = (stencils_ref[i] for i in range(6))
    xmat[...] = jnp.concatenate([mx, kx], axis=0)
    top = jnp.concatenate([my, ky], axis=1)
    ymat[...] = jnp.concatenate([top, jnp.concatenate([jnp.zeros((C, C), F32), my], axis=1)], axis=0)
    zmat[...] = jnp.concatenate([block_diagonal(mz.T), block_diagonal(kz.T)], axis=0)

    def exchange_start(par):
        pack(out, sends.at[par])
        if True:
            for d in sorted(DIRS, key=lambda d: -sum(abs(i) for i in d)):
                fine, there = neighbour(sizes, here, d)

                @pl.when(fine)
                def _():
                    pltpu.make_async_remote_copy(
                        src_ref=sends.at[par, SLOT[d]],
                        dst_ref=gots.at[par, SLOT[d]],
                        send_sem=send_sem.at[par],
                        recv_sem=got_sem.at[par],
                        device_id=there,
                        device_id_type=MESH,
                    ).start()

    def exchange_end(par):
        for n in degrees:

            @pl.when(degree == n)
            def _():
                both = pltpu.make_async_remote_copy(
                    src_ref=sends.at[par, pl.ds(0, n)],
                    dst_ref=gots.at[par, pl.ds(0, n)],
                    send_sem=send_sem.at[par],
                    recv_sem=got_sem.at[par],
                    device_id=everyone[0],
                    device_id_type=MESH,
                )
                both.wait_recv()
                both.wait_send()

        unpack(out, gots.at[par])

    def gather_start(k, pairs):
        s, l = iota((8, 128), 0), iota((8, 128), 1)
        tile = jnp.zeros((8, 128), F32)
        for i, (left, right) in enumerate(pairs):
            lanes = jnp.sum(jnp.sum((left * right).reshape(32, 8, 128), axis=0), axis=0, keepdims=True)
            tile = jnp.where(s == i, lanes, tile)
        column = jnp.sum(tile, axis=1, keepdims=True)
        gather_row(k, jnp.sum(jnp.where(s == l, column, 0.0), axis=0, keepdims=True))

    def gather_row(k, row):
        mine = pl.ds(me, 1)
        terms[k, mine] = row
        for there in everyone:
            pltpu.make_async_remote_copy(
                src_ref=terms.at[k, mine],
                dst_ref=terms.at[k, mine],
                send_sem=term_send.at[k],
                recv_sem=term_got.at[k],
                device_id=there,
                device_id_type=MESH,
            ).start()

    def gather_end(k, count):
        others = pl.ds(0, len(everyone))
        both = pltpu.make_async_remote_copy(
            src_ref=terms.at[k, others],
            dst_ref=terms.at[k, others],
            send_sem=term_send.at[k],
            recv_sem=term_got.at[k],
            device_id=everyone[0],
            device_id_type=MESH,
        )
        both.wait_recv()
        both.wait_send()
        row = jnp.sum(terms[k], axis=0, keepdims=True)
        s, l = iota((8, 128), 0), iota((8, 128), 1)
        column = jnp.sum(jnp.where(s == l, row, 0.0), axis=1, keepdims=True)
        return [column[i : i + 1] for i in range(count)]

    def leaving(i):
        return pltpu.make_async_copy(wides.at[i - 1], basis_ref.at[i - 1], out_sem.at[i - 1])

    def settle(i, image, height):
        new = image
        for k in range(i):
            new = new - height[k] * vecs[k]
        new = new * (1.0 / height[i])
        if i < ITERS:
            vecs[i] = new
        if i > 0:
            wides[i - 1] = wide(new)
            leaving(i).start()

    def heights(products, known):
        *with_known, with_last, square = products
        i = len(known)
        found = list(with_known)
        last = with_last
        for k in range(i - 1):
            last = last - known[i - 1][k] * found[k]
        found.append(last / known[i - 1][i - 1])
        for value in found:
            square = square - value * value
        found.append(jnp.sqrt(square))
        return found

    out[...] = tall(start_ref[...]) * weights[...] * SHRINK
    pl.semaphore_wait(barrier, len(everyone))
    exchange_start(0)
    trace = [jnp.sum(jnp.where(iota((C, C), 0) == iota((C, C), 1), m, 0.0), keepdims=True) / C for m in (kx, ky, kz, mx, my, mz)]
    mean = trace[0] * trace[4] * trace[5] + trace[3] * trace[1] * trace[5] + trace[3] * trace[4] * trace[2]
    gather_row(0, jnp.broadcast_to(mean / (nx * ny * nz), (1, 128)))
    exchange_end(0)
    powers[0] = out[...]

    out[...] = matvec(powers[0], xmat, ymat, zmat)
    exchange_start(1)
    exchange_end(1)
    powers[1] = out[...]

    out[...] = matvec(powers[1], xmat, ymat, zmat)
    exchange_start(0)
    weighted = weights[...] * powers[1]
    gather_start(1, [(powers[0], weights[...] * powers[0]), (powers[0], weighted), (powers[1], weighted)])
    (size,) = gather_end(0, 1)
    exchange_end(0)
    powers[2] = out[...] * (1.0 / size)

    triangle, alphas, betas = [], [], []
    for j in range(2, ITERS + 1):
        if j < ITERS:
            out[...] = matvec(powers[j], xmat, ymat, zmat)
            exchange_start((j + 1) % 2)
        weighted = weights[...] * powers[j]
        earlier = [vecs[k] if j > 2 else powers[0] for k in range(j - 1)]
        gather_start(j, [(v, weighted) for v in earlier + [powers[j - 1], powers[j]]])
        rounds = [j - 1] if j < ITERS else [j - 1, j]
        for k in rounds:
            if k == 1:
                square, *rest = gather_end(1, 3)
                triangle.append([jnp.sqrt(square)])
                settle(0, powers[0], triangle[0])
                triangle.append(heights(rest, triangle))
                hess = {(1, 0): 1.0, (1, 1): 0.0, (2, 1): size}
            else:
                products = gather_end(k, k + 1)
                if k == 2:
                    products[0] = products[0] / triangle[0][0]
                triangle.append(heights(products, triangle))
            settle(k, powers[k], triangle[k])
            i = k - 1
            diagonal = triangle[k][i] * hess[(k, i)] / triangle[i][i]
            if i > 0:
                diagonal = diagonal + hess[(i, i)] - triangle[i][i - 1] * hess[(i, i - 1)] / triangle[i - 1][i - 1]
            alphas.append(diagonal)
            betas.append(triangle[k][k] * hess[(k, i)] / triangle[i][i])
        if j < ITERS:
            exchange_end((j + 1) % 2)
            new = out[...] - alphas[j - 2] * powers[j]
            lead = betas[j - 2]
            if j == 2:
                lead = lead * triangle[0][0]
            else:
                behind = betas[j - 3]
                if j == 3:
                    behind = behind / triangle[0][0]
                new = new - behind * powers[j - 1]
            powers[j + 1] = new * (1.0 / lead)
            hess[(j, j)], hess[(j + 1, j)] = alphas[j - 2], lead

    s, l = iota((8, 128), 0), iota((8, 128), 1)
    tile = jnp.zeros((8, 128), F32)
    for j in range(ITERS):
        tile = jnp.where((s == 0) & (l == j), alphas[j], jnp.where((s == 1) & (l == j), betas[j], tile))
    small[...] = tile[0:2, 0:ITERS]
    last = pltpu.make_async_copy(small, coefficients_ref, out_sem.at[ITERS])
    last.start()
    for i in range(1, ITERS + 1):
        leaving(i).wait()
    last.wait()


def span_set(size):
    return {1} if size == 1 else {2} if size == 2 else {2, 3}


def shards(sizes, start, stencils):
    nx, ny, nz = sizes
    hbm = pl.BlockSpec(memory_space=pltpu.HBM)
    anyw = pl.BlockSpec(memory_space=pl.ANY)
    basis, coefficients = pl.pallas_call(
        functools.partial(kernel, sizes),
        out_shape=(
            jax.ShapeDtypeStruct((ITERS, C, C * C), F32),
            jax.ShapeDtypeStruct((2, ITERS), F32),
        ),
        in_specs=[hbm, hbm],
        out_specs=(anyw, anyw),
        scratch_shapes=[
            pltpu.VMEM((C, C * C), F32),
            pltpu.VMEM((6, C, C), F32),
            pltpu.VMEM((ITERS, C, C * C), F32),
            pltpu.VMEM((2, ITERS), F32),
            pltpu.VMEM((256, 128), F32),
            pltpu.VMEM((ITERS + 1, 256, 128), F32),
            pltpu.VMEM((ITERS, 256, 128), F32),
            pltpu.VMEM((256, 128), F32),
            pltpu.VMEM((2 * C, C), F32),
            pltpu.VMEM((2 * C, 2 * C), F32),
            pltpu.VMEM((256, 128), F32),
            pltpu.VMEM((2, len(DIRS), 8, 128), F32),
            pltpu.VMEM((2, len(DIRS), 8, 128), F32),
            pltpu.VMEM((ITERS + 1, nx * ny * nz, 128), F32),
        ]
        + [pltpu.SemaphoreType.DMA((2,))] * 2
        + [pltpu.SemaphoreType.DMA((ITERS + 1,))] * 2
        + [pltpu.SemaphoreType.DMA((2,)), pltpu.SemaphoreType.DMA((ITERS + 1,))],
        compiler_params=pltpu.CompilerParams(collective_id=0, has_side_effects=True),
    )(start.reshape(C, C * C), stencils.reshape(6, C, C))
    return (
        basis.reshape(1, 1, 1, 1, ITERS, C, C * C),
        coefficients.reshape(1, 2, ITERS),
    )


def solution(mesh):
    sizes = tuple(mesh.shape[a] for a in AXES)
    return jax.shard_map(
        functools.partial(shards, sizes),
        mesh=mesh,
        in_specs=(P("gx", "gy", "gz", None, None, None), P(None, "gx", "gy", "gz", None, None)),
        out_specs=(P("gx", "gy", "gz", None, None, None, None), P()),
        check_vma=False,
    )
```

```python
import functools

import jax
import jax.numpy as jnp
from jax import lax
from jax.experimental import pallas as pl
from jax.experimental.pallas import tpu as pltpu
from jax.sharding import PartitionSpec as P

ITERS = 5
C = 32
MESH = pl.DeviceIdType.MESH
F32 = jnp.float32
BF16 = jnp.bfloat16
AXES = ("gx", "gy", "gz")
DIRS = [
    (dx, dy, dz)
    for dx in (-1, 0, 1)
    for dy in (-1, 0, 1)
    for dz in (-1, 0, 1)
    if (dx, dy, dz) != (0, 0, 0)
]
SLOT = {d: i for i, d in enumerate(DIRS)}
SHRINK = 2.0**-17


def iota(shape, dim):
    return lax.broadcasted_iota(jnp.int32, shape, dim)


def roll(x, shift, axis):
    size = x.shape[axis]
    shift = shift % size
    return x if shift == 0 else pltpu.roll(x, shift, axis)


def swap(field):
    x = field.reshape(32, 8, 128)
    s, l = iota((1, 8, 128), 1), iota((1, 8, 128), 2)
    s1, l1 = (s // 2) % 2, l // 64
    r = roll(x, 64, 2)
    x = jnp.where(s1 == l1, x, jnp.where(s1 == 0, roll(r, -2, 1), roll(r, 2, 1)))
    s0, l0 = s % 2, (l // 32) % 2
    up, down = roll(roll(x, 32, 2), -1, 1), roll(roll(x, -32, 2), 1, 1)
    x = jnp.where(s0 == l0, x, jnp.where(s0 == 0, up, down))
    even = jnp.concatenate([x[t * 4 : t * 4 + 4] for t in range(0, 8, 2)], axis=0)
    odd = jnp.concatenate([x[t * 4 : t * 4 + 4] for t in range(1, 8, 2)], axis=0)
    half = s < 4
    top = jnp.where(half, even, roll(odd, 4, 1))
    bottom = jnp.where(half, roll(even, 4, 1), odd)
    parts = []
    for ai in range(4):
        for part in (top, bottom):
            for k in range(4):
                parts.append(part[k * 4 + ai : k * 4 + ai + 1])
    return jnp.concatenate(parts, axis=0).reshape(256, 128)


def wide(field):
    return jnp.concatenate([field[t * 32 : t * 32 + 32] for t in range(8)], axis=1)


def tall(field):
    return jnp.concatenate([field[:, t * 128 : t * 128 + 128] for t in range(8)], axis=0)


def split(x):
    high = x.astype(BF16)
    rest = x - high.astype(F32)
    middle = rest.astype(BF16)
    return high, middle, (rest - middle.astype(F32)).astype(BF16)


PAIRS = ((0, 0), (0, 1), (1, 0), (1, 1), (0, 2), (2, 0))


def dot(left, right):
    return jnp.dot(left, right, preferred_element_type=F32)


def spread(matrix):
    parts = split(matrix)
    return jnp.concatenate([parts[i] for i, _ in PAIRS], axis=1)


def stack(field):
    parts = split(field)
    return jnp.concatenate([parts[i] for _, i in PAIRS], axis=0)


def matvec(field, xmat_ref, ymat_ref, zmat_ref):
    first = dot(xmat_ref[...], stack(wide(field)))
    mass, stiff = swap(tall(first[:C])), swap(tall(first[C:]))
    second = dot(ymat_ref[...], stack(jnp.concatenate([wide(stiff), wide(mass)], axis=0)))
    third = jnp.concatenate([tall(second[:C]), tall(second[C:])], axis=1)
    high, middle, low = split(third)
    pair = zmat_ref[:, 0:256]
    both = dot(high, pair) + dot(middle, pair)
    rest = dot(low, zmat_ref[:, 0:128]) + dot(high, zmat_ref[:, 256:384])
    return swap(both[:, :128] + (both[:, 128:] + rest))


def block_diagonal(matrix):
    zero = jnp.zeros((C, C), F32)
    rows = []
    for i in range(4):
        rows.append(jnp.concatenate([matrix if k == i else zero for k in range(4)], axis=1))
    return jnp.concatenate(rows, axis=0)


def weight_field(sizes, here):
    row, lane = iota((256, 128), 0), iota((256, 128), 1)
    places = (row % C, (row // C) * 4 + lane // C, lane % C)
    weight = jnp.ones((256, 128), F32)
    for place, size, at in zip(places, sizes, here):
        low = jnp.where(at > 0, 0.5, 1.0).astype(F32)
        high = jnp.where(at < size - 1, 0.5, 1.0).astype(F32)
        weight = weight * jnp.where(place == 0, low, jnp.where(place == C - 1, high, 1.0))
    return weight


def neighbour(sizes, here, step):
    fine = None
    for size, at, d in zip(sizes, here, step):
        if d != 0:
            inside = at > 0 if d < 0 else at < size - 1
            fine = inside if fine is None else jnp.logical_and(fine, inside)
    return fine, tuple(at + d for at, d in zip(here, step))


def pack(out_ref, send_ref):
    s, l = iota((8, 128), 0), iota((8, 128), 1)
    lower = lambda t, ai: out_ref[pl.ds(t * 32 + ai * 8, 8), :]
    zero = jnp.zeros((8, 128), F32)
    low, high = zero, zero
    for t in range(8):
        for ai in range(4):
            r = ai * 8 + t
            moved = roll(lower(t, ai), r, 1)
            low = jnp.where(l % C == r, moved, low)
            high = jnp.where(l % C == (r + C - 1) % C, moved, high)
    for dz, plane, base in ((-1, low, 0), (1, high, -31)):
        for dx in (-1, 0, 1):
            for dy in (-1, 0, 1):
                lanes = base - dx * 24 - dy * 103
                part = roll(roll(plane, lanes, 1), dx, 0)
                keep = None
                if dx != 0:
                    keep = (s == (7 if dx < 0 else 0)) & ((l % C) // 8 == (3 if dx < 0 else 0))
                if dy != 0:
                    mine = (l // C == (3 if dy < 0 else 0)) & (l % 8 == (7 if dy < 0 else 0))
                    keep = mine if keep is None else keep & mine
                send_ref[SLOT[(dx, dy, dz)]] = part if keep is None else jnp.where(keep, part, 0.0)
    for dx in (-1, 1):
        plane = out_ref[pl.ds(0 if dx < 0 else C - 1, 8, stride=C), :]
        send_ref[SLOT[(dx, 0, 0)]] = plane
        for dy in (-1, 1):
            part = roll(roll(plane, 96 if dy < 0 else 32, 1), dy, 0)
            keep = (s == (7 if dy < 0 else 0)) & (l // C == (3 if dy < 0 else 0))
            send_ref[SLOT[(dx, dy, 0)]] = jnp.where(keep, part, 0.0)
    for dy in (-1, 1):
        plane = zero
        for ai in range(4):
            piece = roll(lower(0 if dy < 0 else 7, ai), C * (ai + (0 if dy < 0 else 1)), 1)
            plane = jnp.where(l // C == ai, piece, plane)
        send_ref[SLOT[(0, dy, 0)]] = plane


def unpack(out_ref, got_ref):
    l = iota((8, 128), 1)
    near = (-1, 0, 1)
    for dx in (-1, 1):
        plane = sum(got_ref[SLOT[(dx, dy, 0)]] for dy in near)
        rows = pl.ds(C - 1 if dx < 0 else 0, 8, stride=C)
        out_ref[rows, :] = out_ref[rows, :] + plane
    low, high = (
        sum(got_ref[SLOT[(dx, dy, dz)]] for dx in near for dy in near) for dz in (1, -1)
    )
    first, last = got_ref[SLOT[(0, 1, 0)]], got_ref[SLOT[(0, -1, 0)]]
    for t in range(8):
        for ai in range(4):
            r = ai * 8 + t
            rows = pl.ds(t * 32 + ai * 8, 8)
            add = jnp.where(l % C == 0, roll(low, -r, 1), 0.0)
            add = add + jnp.where(l % C == C - 1, roll(high, 31 - r, 1), 0.0)
            if t == 0:
                add = add + jnp.where(l < C, roll(first, -C * ai, 1), 0.0)
            if t == 7:
                add = add + jnp.where(l >= 96, roll(last, 96 - C * ai, 1), 0.0)
            out_ref[rows, :] = out_ref[rows, :] + add


def kernel(
    sizes,
    start_hbm,
    stencils_hbm,
    basis_ref,
    coefficients_ref,
    start_ref,
    stencils_ref,
    wides,
    small,
    out,
    powers,
    vecs,
    weights,
    xmat,
    ymat,
    zmat,
    sends,
    gots,
    terms,
    send_sem,
    got_sem,
    term_send,
    term_got,
    in_sem,
    out_sem,
):
    here = tuple(lax.axis_index(a) for a in AXES)
    nx, ny, nz = sizes
    gx, gy, gz = here
    me = (gx * ny + gy) * nz + gz
    hops = lambda k, size: min(k, size - k)
    steps = sorted(
        ((i, j, k) for i in range(nx) for j in range(ny) for k in range(nz)),
        key=lambda d: -(hops(d[0], nx) + hops(d[1], ny) + hops(d[2], nz) / 2),
    )
    along = [[lax.rem(at + k, size) for k in range(size)] for at, size in zip(here, sizes)]
    everyone = [tuple(along[a][d[a]] for a in range(3)) for d in steps if any(d)]
    spans = [
        1 + jnp.where(at > 0, 1, 0) + jnp.where(at < size - 1, 1, 0)
        for at, size in zip(here, sizes)
    ]
    degree = spans[0] * spans[1] * spans[2] - 1
    degrees = sorted(
        {
            i * j * k - 1
            for i in span_set(nx)
            for j in span_set(ny)
            for k in span_set(nz)
        }
    )

    inputs = [
        pltpu.make_async_copy(start_hbm, start_ref, in_sem.at[0]),
        pltpu.make_async_copy(stencils_hbm, stencils_ref, in_sem.at[1]),
    ]
    for copy in inputs:
        copy.start()
    gots[...] = jnp.zeros_like(gots)
    barrier = pltpu.get_barrier_semaphore()
    for there in everyone:
        pl.semaphore_signal(barrier, inc=1, device_id=there, device_id_type=MESH)

    weights[...] = weight_field(sizes, here)
    for copy in inputs:
        copy.wait()
    kx, ky, kz, mx, my, mz = (stencils_ref[i] for i in range(6))
    xmat[...] = spread(jnp.concatenate([mx, kx], axis=0))
    top = jnp.concatenate([my, ky], axis=1)
    ymat[...] = spread(jnp.concatenate([top, jnp.concatenate([jnp.zeros((C, C), F32), my], axis=1)], axis=0))
    zmat[...] = jnp.concatenate(
        split(jnp.concatenate([block_diagonal(mz.T), block_diagonal(kz.T)], axis=0)), axis=1
    )

    def exchange_start(par):
        pack(out, sends.at[par])
        if True:
            for d in sorted(DIRS, key=lambda d: -sum(abs(i) for i in d)):
                fine, there = neighbour(sizes, here, d)

                @pl.when(fine)
                def _():
                    pltpu.make_async_remote_copy(
                        src_ref=sends.at[par, SLOT[d]],
                        dst_ref=gots.at[par, SLOT[d]],
                        send_sem=send_sem.at[par],
                        recv_sem=got_sem.at[par],
                        device_id=there,
                        device_id_type=MESH,
                    ).start()

    def exchange_end(par):
        for n in degrees:

            @pl.when(degree == n)
            def _():
                both = pltpu.make_async_remote_copy(
                    src_ref=sends.at[par, pl.ds(0, n)],
                    dst_ref=gots.at[par, pl.ds(0, n)],
                    send_sem=send_sem.at[par],
                    recv_sem=got_sem.at[par],
                    device_id=everyone[0],
                    device_id_type=MESH,
                )
                both.wait_recv()
                both.wait_send()

        unpack(out, gots.at[par])

    def gather_start(k, pairs):
        s, l = iota((8, 128), 0), iota((8, 128), 1)
        tile = jnp.zeros((8, 128), F32)
        for i, (left, right) in enumerate(pairs):
            lanes = jnp.sum(jnp.sum((left * right).reshape(32, 8, 128), axis=0), axis=0, keepdims=True)
            tile = jnp.where(s == i, lanes, tile)
        column = jnp.sum(tile, axis=1, keepdims=True)
        gather_row(k, jnp.sum(jnp.where(s == l, column, 0.0), axis=0, keepdims=True))

    def gather_row(k, row):
        mine = pl.ds(me, 1)
        terms[k, mine] = row
        for there in everyone:
            pltpu.make_async_remote_copy(
                src_ref=terms.at[k, mine],
                dst_ref=terms.at[k, mine],
                send_sem=term_send.at[k],
                recv_sem=term_got.at[k],
                device_id=there,
                device_id_type=MESH,
            ).start()

    def gather_end(k, count):
        others = pl.ds(0, len(everyone))
        both = pltpu.make_async_remote_copy(
            src_ref=terms.at[k, others],
            dst_ref=terms.at[k, others],
            send_sem=term_send.at[k],
            recv_sem=term_got.at[k],
            device_id=everyone[0],
            device_id_type=MESH,
        )
        both.wait_recv()
        both.wait_send()
        row = jnp.sum(terms[k], axis=0, keepdims=True)
        s, l = iota((8, 128), 0), iota((8, 128), 1)
        column = jnp.sum(jnp.where(s == l, row, 0.0), axis=1, keepdims=True)
        return [column[i : i + 1] for i in range(count)]

    def leaving(i):
        return pltpu.make_async_copy(wides.at[i - 1], basis_ref.at[i - 1], out_sem.at[i - 1])

    def settle(i, image, height):
        new = image
        for k in range(i):
            new = new - height[k] * vecs[k]
        new = new * (1.0 / height[i])
        if i < ITERS:
            vecs[i] = new
        if i > 0:
            wides[i - 1] = wide(new)
            leaving(i).start()

    def heights(products, known):
        *with_known, with_last, square = products
        i = len(known)
        found = list(with_known)
        last = with_last
        for k in range(i - 1):
            last = last - known[i - 1][k] * found[k]
        found.append(last / known[i - 1][i - 1])
        for value in found:
            square = square - value * value
        found.append(jnp.sqrt(square))
        return found

    out[...] = tall(start_ref[...]) * weights[...] * SHRINK
    pl.semaphore_wait(barrier, len(everyone))
    exchange_start(0)
    trace = [jnp.sum(jnp.where(iota((C, C), 0) == iota((C, C), 1), m, 0.0), keepdims=True) / C for m in (kx, ky, kz, mx, my, mz)]
    mean = trace[0] * trace[4] * trace[5] + trace[3] * trace[1] * trace[5] + trace[3] * trace[4] * trace[2]
    gather_row(0, jnp.broadcast_to(mean / (nx * ny * nz), (1, 128)))
    exchange_end(0)
    powers[0] = out[...]

    out[...] = matvec(powers[0], xmat, ymat, zmat)
    exchange_start(1)
    exchange_end(1)
    powers[1] = out[...]

    out[...] = matvec(powers[1], xmat, ymat, zmat)
    exchange_start(0)
    weighted = weights[...] * powers[1]
    gather_start(1, [(powers[0], weights[...] * powers[0]), (powers[0], weighted), (powers[1], weighted)])
    (size,) = gather_end(0, 1)
    exchange_end(0)
    powers[2] = out[...] * (1.0 / size)

    triangle, alphas, betas = [], [], []
    for j in range(2, ITERS + 1):
        if j < ITERS:
            out[...] = matvec(powers[j], xmat, ymat, zmat)
            exchange_start((j + 1) % 2)
        weighted = weights[...] * powers[j]
        earlier = [vecs[k] if j > 2 else powers[0] for k in range(j - 1)]
        gather_start(j, [(v, weighted) for v in earlier + [powers[j - 1], powers[j]]])
        rounds = [j - 1] if j < ITERS else [j - 1, j]
        for k in rounds:
            if k == 1:
                square, *rest = gather_end(1, 3)
                triangle.append([jnp.sqrt(square)])
                settle(0, powers[0], triangle[0])
                triangle.append(heights(rest, triangle))
                hess = {(1, 0): 1.0, (1, 1): 0.0, (2, 1): size}
            else:
                products = gather_end(k, k + 1)
                if k == 2:
                    products[0] = products[0] / triangle[0][0]
                triangle.append(heights(products, triangle))
            settle(k, powers[k], triangle[k])
            i = k - 1
            diagonal = triangle[k][i] * hess[(k, i)] / triangle[i][i]
            if i > 0:
                diagonal = diagonal + hess[(i, i)] - triangle[i][i - 1] * hess[(i, i - 1)] / triangle[i - 1][i - 1]
            alphas.append(diagonal)
            betas.append(triangle[k][k] * hess[(k, i)] / triangle[i][i])
        if j < ITERS:
            exchange_end((j + 1) % 2)
            new = out[...] - alphas[j - 2] * powers[j]
            lead = betas[j - 2]
            if j == 2:
                lead = lead * triangle[0][0]
            else:
                behind = betas[j - 3]
                if j == 3:
                    behind = behind / triangle[0][0]
                new = new - behind * powers[j - 1]
            powers[j + 1] = new * (1.0 / lead)
            hess[(j, j)], hess[(j + 1, j)] = alphas[j - 2], lead

    s, l = iota((8, 128), 0), iota((8, 128), 1)
    tile = jnp.zeros((8, 128), F32)
    for j in range(ITERS):
        tile = jnp.where((s == 0) & (l == j), alphas[j], jnp.where((s == 1) & (l == j), betas[j], tile))
    small[...] = tile[0:2, 0:ITERS]
    last = pltpu.make_async_copy(small, coefficients_ref, out_sem.at[ITERS])
    last.start()
    for i in range(1, ITERS + 1):
        leaving(i).wait()
    last.wait()


def span_set(size):
    return {1} if size == 1 else {2} if size == 2 else {2, 3}


def shards(sizes, start, stencils):
    nx, ny, nz = sizes
    hbm = pl.BlockSpec(memory_space=pltpu.HBM)
    anyw = pl.BlockSpec(memory_space=pl.ANY)
    basis, coefficients = pl.pallas_call(
        functools.partial(kernel, sizes),
        out_shape=(
            jax.ShapeDtypeStruct((ITERS, C, C * C), F32),
            jax.ShapeDtypeStruct((2, ITERS), F32),
        ),
        in_specs=[hbm, hbm],
        out_specs=(anyw, anyw),
        scratch_shapes=[
            pltpu.VMEM((C, C * C), F32),
            pltpu.VMEM((6, C, C), F32),
            pltpu.VMEM((ITERS, C, C * C), F32),
            pltpu.VMEM((2, ITERS), F32),
            pltpu.VMEM((256, 128), F32),
            pltpu.VMEM((ITERS + 1, 256, 128), F32),
            pltpu.VMEM((ITERS, 256, 128), F32),
            pltpu.VMEM((256, 128), F32),
            pltpu.VMEM((2 * C, 6 * C), BF16),
            pltpu.VMEM((2 * C, 12 * C), BF16),
            pltpu.VMEM((256, 384), BF16),
            pltpu.VMEM((2, len(DIRS), 8, 128), F32),
            pltpu.VMEM((2, len(DIRS), 8, 128), F32),
            pltpu.VMEM((ITERS + 1, nx * ny * nz, 128), F32),
        ]
        + [pltpu.SemaphoreType.DMA((2,))] * 2
        + [pltpu.SemaphoreType.DMA((ITERS + 1,))] * 2
        + [pltpu.SemaphoreType.DMA((2,)), pltpu.SemaphoreType.DMA((ITERS + 1,))],
        compiler_params=pltpu.CompilerParams(collective_id=0, has_side_effects=True),
    )(start.reshape(C, C * C), stencils.reshape(6, C, C))
    return (
        basis.reshape(1, 1, 1, 1, ITERS, C, C * C),
        coefficients.reshape(1, 2, ITERS),
    )


def solution(mesh):
    sizes = tuple(mesh.shape[a] for a in AXES)
    return jax.shard_map(
        functools.partial(shards, sizes),
        mesh=mesh,
        in_specs=(P("gx", "gy", "gz", None, None, None), P(None, "gx", "gy", "gz", None, None)),
        out_specs=(P("gx", "gy", "gz", None, None, None, None), P()),
        check_vma=False,
    )
```

```python
import functools
import itertools

import jax
import jax.numpy as jnp
from jax import lax
from jax.experimental import pallas as pl
from jax.experimental.pallas import tpu as pltpu
from jax.sharding import PartitionSpec as P

ITERS = 5
C = 32
MESH = pl.DeviceIdType.MESH
F32 = jnp.float32
BF16 = jnp.bfloat16
AXES = ("gx", "gy", "gz")
DIRS = [
    (dx, dy, dz)
    for dx in (-1, 0, 1)
    for dy in (-1, 0, 1)
    for dz in (-1, 0, 1)
    if (dx, dy, dz) != (0, 0, 0)
]
TILES = [d for d in DIRS if d[0] == 0 or d[1:] == (0, 0)]
ROWS = [d for d in DIRS if d not in TILES]
SLOT = {d: i for dirs in (TILES, ROWS) for i, d in enumerate(dirs)}
SHRINK = 2.0**-17


def iota(shape, dim):
    return lax.broadcasted_iota(jnp.int32, shape, dim)


def roll(x, shift, axis):
    size = x.shape[axis]
    shift = shift % size
    return x if shift == 0 else pltpu.roll(x, shift, axis)


def swap(field):
    x = field.reshape(32, 8, 128)
    s, l = iota((1, 8, 128), 1), iota((1, 8, 128), 2)
    s1, l1 = (s // 2) % 2, l // 64
    r = roll(x, 64, 2)
    x = jnp.where(s1 == l1, x, jnp.where(s1 == 0, roll(r, -2, 1), roll(r, 2, 1)))
    s0, l0 = s % 2, (l // 32) % 2
    up, down = roll(roll(x, 32, 2), -1, 1), roll(roll(x, -32, 2), 1, 1)
    x = jnp.where(s0 == l0, x, jnp.where(s0 == 0, up, down))
    even = jnp.concatenate([x[t * 4 : t * 4 + 4] for t in range(0, 8, 2)], axis=0)
    odd = jnp.concatenate([x[t * 4 : t * 4 + 4] for t in range(1, 8, 2)], axis=0)
    half = s < 4
    top = jnp.where(half, even, roll(odd, 4, 1))
    bottom = jnp.where(half, roll(even, 4, 1), odd)
    parts = []
    for ai in range(4):
        for part in (top, bottom):
            for k in range(4):
                parts.append(part[k * 4 + ai : k * 4 + ai + 1])
    return jnp.concatenate(parts, axis=0).reshape(256, 128)


def wide(field):
    return jnp.concatenate([field[t * 32 : t * 32 + 32] for t in range(8)], axis=1)


def tall(field):
    return jnp.concatenate([field[:, t * 128 : t * 128 + 128] for t in range(8)], axis=0)


def split(x):
    high = x.astype(BF16)
    rest = x - high.astype(F32)
    middle = rest.astype(BF16)
    return high, middle, (rest - middle.astype(F32)).astype(BF16)


PAIRS = ((0, 0), (0, 1), (1, 0), (1, 1), (0, 2), (2, 0))


def dot(left, right):
    return jnp.dot(left, right, preferred_element_type=F32)


def spread(matrix):
    parts = split(matrix)
    return jnp.concatenate([parts[i] for i, _ in PAIRS], axis=1)


def stack(field):
    parts = split(field)
    return jnp.concatenate([parts[i] for _, i in PAIRS], axis=0)


def matvec(field, first_ref, second_ref, zmat_ref):
    first = dot(first_ref[...], stack(wide(field)))
    mass, stiff = swap(tall(first[:C])), swap(tall(first[C:]))
    second = dot(second_ref[...], stack(jnp.concatenate([wide(stiff), wide(mass)], axis=0)))
    third = jnp.concatenate([tall(second[:C]), tall(second[C:])], axis=1)
    high, middle, low = split(third)
    pair = zmat_ref[:, 0:256]
    both = dot(high, pair) + dot(middle, pair)
    rest = dot(low, zmat_ref[:, 0:128]) + dot(high, zmat_ref[:, 256:384])
    return both[:, :128] + (both[:, 128:] + rest)


def block_diagonal(matrix):
    zero = jnp.zeros((C, C), F32)
    rows = []
    for i in range(4):
        rows.append(jnp.concatenate([matrix if k == i else zero for k in range(4)], axis=1))
    return jnp.concatenate(rows, axis=0)


def weight_field(sizes, here):
    row, lane = iota((256, 128), 0), iota((256, 128), 1)
    places = (row % C, (row // C) * 4 + lane // C, lane % C)
    weight = jnp.ones((256, 128), F32)
    for place, size, at in zip(places, sizes, here):
        low = jnp.where(at > 0, 0.5, 1.0).astype(F32)
        high = jnp.where(at < size - 1, 0.5, 1.0).astype(F32)
        weight = weight * jnp.where(place == 0, low, jnp.where(place == C - 1, high, 1.0))
    return weight


def neighbour(sizes, here, step):
    fine = None
    for size, at, d in zip(sizes, here, step):
        if d != 0:
            inside = at > 0 if d < 0 else at < size - 1
            fine = inside if fine is None else jnp.logical_and(fine, inside)
    return fine, tuple(at + d for at, d in zip(here, step))


def pack(out_ref, tile_ref, row_ref):
    s, l = iota((8, 128), 0), iota((8, 128), 1)
    line = iota((1, 128), 1)
    lower = lambda t, ai: out_ref[pl.ds(t * 32 + ai * 8, 8), :]
    zero = jnp.zeros((8, 128), F32)
    low, high = zero, zero
    for t in range(8):
        for ai in range(4):
            r = ai * 8 + t
            moved = roll(lower(t, ai), r, 1)
            low = jnp.where(l % C == r, moved, low)
            high = jnp.where(l % C == (r + C - 1) % C, moved, high)

    def send_row(d, plane, source, keep):
        row_ref[pl.ds(SLOT[d], 1), :] = jnp.where(keep, plane[source : source + 1], 0.0)

    for dx in (-1, 1):
        source = 0 if dx < 0 else 7
        for dz, plane, base in ((-1, low, 0), (1, high, -31)):
            for dy in (-1, 0, 1):
                keep = (line % C) // 8 == (3 if dx < 0 else 0)
                if dy != 0:
                    keep = keep & (line // C == (3 if dy < 0 else 0)) & (line % 8 == (7 if dy < 0 else 0))
                send_row((dx, dy, dz), roll(plane, base - dx * 24 - dy * 103, 1), source, keep)
        plane = out_ref[pl.ds(0 if dx < 0 else C - 1, 8, stride=C), :]
        tile_ref[SLOT[(dx, 0, 0)]] = plane
        for dy in (-1, 1):
            keep = line // C == (3 if dy < 0 else 0)
            send_row((dx, dy, 0), roll(plane, 96 if dy < 0 else 32, 1), 0 if dy < 0 else 7, keep)
    for dz, plane, base in ((-1, low, 0), (1, high, -31)):
        tile_ref[SLOT[(0, 0, dz)]] = roll(plane, base, 1)
        for dy in (-1, 1):
            keep = (l // C == (3 if dy < 0 else 0)) & (l % 8 == (7 if dy < 0 else 0))
            tile_ref[SLOT[(0, dy, dz)]] = jnp.where(keep, roll(plane, base - dy * 103, 1), 0.0)
    for dy in (-1, 1):
        plane = zero
        for ai in range(4):
            piece = roll(lower(0 if dy < 0 else 7, ai), C * (ai + (0 if dy < 0 else 1)), 1)
            plane = jnp.where(l // C == ai, piece, plane)
        tile_ref[SLOT[(0, dy, 0)]] = plane


def unpack(out_ref, tile_ref, row_ref):
    s, l = iota((8, 128), 0), iota((8, 128), 1)
    near = (-1, 0, 1)
    got = lambda *d: tile_ref[SLOT[d]]
    row = lambda *d: row_ref[pl.ds(SLOT[d], 1), :]
    ends = lambda last, first: jnp.where(s == 7, last, jnp.where(s == 0, first, 0.0))
    for dx in (-1, 1):
        plane = got(dx, 0, 0) + ends(row(dx, -1, 0), row(dx, 1, 0))
        rows = pl.ds(C - 1 if dx < 0 else 0, 8, stride=C)
        out_ref[rows, :] = out_ref[rows, :] + plane
    low, high = (
        sum(got(0, dy, dz) for dy in near)
        + ends(sum(row(-1, dy, dz) for dy in near), sum(row(1, dy, dz) for dy in near))
        for dz in (1, -1)
    )
    first, last = got(0, 1, 0), got(0, -1, 0)
    for t in range(8):
        for ai in range(4):
            r = ai * 8 + t
            rows = pl.ds(t * 32 + ai * 8, 8)
            add = jnp.where(l % C == 0, roll(low, -r, 1), 0.0)
            add = add + jnp.where(l % C == C - 1, roll(high, 31 - r, 1), 0.0)
            if t == 0:
                add = add + jnp.where(l < C, roll(first, -C * ai, 1), 0.0)
            if t == 7:
                add = add + jnp.where(l >= 96, roll(last, 96 - C * ai, 1), 0.0)
            out_ref[rows, :] = out_ref[rows, :] + add


def kernel(
    sizes,
    start_hbm,
    stencils_hbm,
    basis_ref,
    coefficients_ref,
    start_ref,
    stencils_ref,
    wides,
    small,
    out,
    powers,
    turned,
    vecs,
    weights,
    first,
    second,
    zmat,
    tiles,
    rows,
    got_tiles,
    got_rows,
    terms,
    send_sem,
    got_sem,
    term_send,
    term_got,
    in_sem,
    out_sem,
):
    here = tuple(lax.axis_index(a) for a in AXES)
    nx, ny, nz = sizes
    gx, gy, gz = here
    me = (gx * ny + gy) * nz + gz
    hops = lambda k, size: min(k, size - k)
    steps = sorted(
        ((i, j, k) for i in range(nx) for j in range(ny) for k in range(nz)),
        key=lambda d: -(hops(d[0], nx) + hops(d[1], ny) + hops(d[2], nz) / 2),
    )
    along = [[lax.rem(at + k, size) for k in range(size)] for at, size in zip(here, sizes)]
    everyone = [tuple(along[a][d[a]] for a in range(3)) for d in steps if any(d)]
    beside = [
        jnp.where(at > 0, 1, 0) + jnp.where(at < size - 1, 1, 0) for at, size in zip(here, sizes)
    ]

    inputs = [
        pltpu.make_async_copy(start_hbm, start_ref, in_sem.at[0]),
        pltpu.make_async_copy(stencils_hbm, stencils_ref, in_sem.at[1]),
    ]
    for copy in inputs:
        copy.start()
    got_tiles[...] = jnp.zeros_like(got_tiles)
    got_rows[...] = jnp.zeros_like(got_rows)
    barrier = pltpu.get_barrier_semaphore()
    for there in everyone:
        pl.semaphore_signal(barrier, inc=1, device_id=there, device_id_type=MESH)

    weights[...] = weight_field(sizes, here)
    for copy in inputs:
        copy.wait()
    kx, ky, kz, mx, my, mz = (stencils_ref[i] for i in range(6))
    empty = jnp.zeros((C, C), F32)
    for i, (mass, stiff) in enumerate(((mx, kx), (my, ky))):
        first[i] = spread(jnp.concatenate([mass, stiff], axis=0))
        upper, lower = (jnp.concatenate(p, axis=1) for p in ((mass, stiff), (empty, mass)))
        second[1 - i] = spread(jnp.concatenate([upper, lower], axis=0))
    zmat[...] = jnp.concatenate(
        split(jnp.concatenate([block_diagonal(mz.T), block_diagonal(kz.T)], axis=0)), axis=1
    )

    def exchange_start(par):
        pack(out, tiles.at[par], rows.at[par])
        for d in sorted(DIRS, key=lambda d: -sum(abs(i) for i in d)):
            fine, there = neighbour(sizes, here, (d[1], d[0], d[2]) if par else d)
            if d in TILES:
                source, target = tiles.at[par, SLOT[d]], got_tiles.at[par, SLOT[d]]
            else:
                source, target = rows.at[par, pl.ds(SLOT[d], 1)], got_rows.at[par, pl.ds(SLOT[d], 1)]

            @pl.when(fine)
            def _():
                pltpu.make_async_remote_copy(
                    src_ref=source,
                    dst_ref=target,
                    send_sem=send_sem.at[par, int(d in ROWS)],
                    recv_sem=got_sem.at[par, int(d in ROWS)],
                    device_id=there,
                    device_id_type=MESH,
                ).start()

    def exchange_end(par):
        order = (1, 0, 2) if par else (0, 1, 2)
        counts = message_counts(*(beside[i] for i in order))
        choices = [{0} if n == 1 else {1} if n == 2 else {1, 2} for n in (sizes[i] for i in order)]
        for n, m in sorted({message_counts(*c) for c in itertools.product(*choices)}):

            @pl.when((counts[0] == n) & (counts[1] == m))
            def _():
                for kind, (count, sent, got) in enumerate(((n, tiles, got_tiles), (m, rows, got_rows))):
                    if count:
                        both = pltpu.make_async_remote_copy(
                            src_ref=sent.at[par, pl.ds(0, count)],
                            dst_ref=got.at[par, pl.ds(0, count)],
                            send_sem=send_sem.at[par, kind],
                            recv_sem=got_sem.at[par, kind],
                            device_id=everyone[0],
                            device_id_type=MESH,
                        )
                        both.wait_recv()
                        both.wait_send()

        unpack(out, got_tiles.at[par], got_rows.at[par])

    def gather_start(k, pairs):
        s, l = iota((8, 128), 0), iota((8, 128), 1)
        tile = jnp.zeros((8, 128), F32)
        for i, (left, right) in enumerate(pairs):
            lanes = jnp.sum(jnp.sum((left * right).reshape(32, 8, 128), axis=0), axis=0, keepdims=True)
            tile = jnp.where(s == i, lanes, tile)
        column = jnp.sum(tile, axis=1, keepdims=True)
        gather_row(k, jnp.sum(jnp.where(s == l, column, 0.0), axis=0, keepdims=True))

    def gather_row(k, row):
        mine = pl.ds(me, 1)
        terms[k, mine] = row
        for there in everyone:
            pltpu.make_async_remote_copy(
                src_ref=terms.at[k, mine],
                dst_ref=terms.at[k, mine],
                send_sem=term_send.at[k],
                recv_sem=term_got.at[k],
                device_id=there,
                device_id_type=MESH,
            ).start()

    def gather_end(k, count):
        others = pl.ds(0, len(everyone))
        both = pltpu.make_async_remote_copy(
            src_ref=terms.at[k, others],
            dst_ref=terms.at[k, others],
            send_sem=term_send.at[k],
            recv_sem=term_got.at[k],
            device_id=everyone[0],
            device_id_type=MESH,
        )
        both.wait_recv()
        both.wait_send()
        row = jnp.sum(terms[k], axis=0, keepdims=True)
        s, l = iota((8, 128), 0), iota((8, 128), 1)
        column = jnp.sum(jnp.where(s == l, row, 0.0), axis=1, keepdims=True)
        return [column[i : i + 1] for i in range(count)]

    def leaving(i):
        return pltpu.make_async_copy(wides.at[i - 1], basis_ref.at[i - 1], out_sem.at[i - 1])

    def settle(i, image, height):
        new = image
        for k in range(i):
            new = new - height[k] * vecs[k]
        new = new * (1.0 / height[i])
        if i < ITERS:
            vecs[i] = new
        if i > 0:
            wides[i - 1] = wide(new)
            leaving(i).start()

    def heights(products, known):
        *with_known, with_last, square = products
        i = len(known)
        found = list(with_known)
        last = with_last
        for k in range(i - 1):
            last = last - known[i - 1][k] * found[k]
        found.append(last / known[i - 1][i - 1])
        for value in found:
            square = square - value * value
        found.append(jnp.sqrt(square))
        return found

    out[...] = tall(start_ref[...]) * weights[...] * SHRINK
    pl.semaphore_wait(barrier, len(everyone))
    exchange_start(0)
    trace = [jnp.sum(jnp.where(iota((C, C), 0) == iota((C, C), 1), m, 0.0), keepdims=True) / C for m in (kx, ky, kz, mx, my, mz)]
    mean = trace[0] * trace[4] * trace[5] + trace[3] * trace[1] * trace[5] + trace[3] * trace[4] * trace[2]
    gather_row(0, jnp.broadcast_to(mean / (nx * ny * nz), (1, 128)))
    exchange_end(0)
    powers[0] = out[...]

    def apply(j):
        here = (turned if j % 2 else powers)[j]
        out[...] = matvec(here, first.at[j % 2], second.at[j % 2], zmat)
        exchange_start((j + 1) % 2)

    def turn(j):
        if j % 2:
            powers[j] = swap(turned[j])
        else:
            turned[j] = swap(powers[j])

    apply(0)
    exchange_end(1)
    turned[1] = out[...]

    apply(1)
    turn(1)
    weighted = weights[...] * powers[1]
    gather_start(1, [(powers[0], weights[...] * powers[0]), (powers[0], weighted), (powers[1], weighted)])
    (size,) = gather_end(0, 1)
    exchange_end(0)
    powers[2] = out[...] * (1.0 / size)

    triangle, alphas, betas = [], [], []
    for j in range(2, ITERS + 1):
        if j < ITERS:
            apply(j)
            turn(j)
        weighted = weights[...] * powers[j]
        earlier = [vecs[k] if j > 2 else powers[0] for k in range(j - 1)]
        gather_start(j, [(v, weighted) for v in earlier + [powers[j - 1], powers[j]]])
        rounds = [j - 1] if j < ITERS else [j - 1, j]
        for k in rounds:
            if k == 1:
                square, *rest = gather_end(1, 3)
                triangle.append([jnp.sqrt(square)])
                settle(0, powers[0], triangle[0])
                triangle.append(heights(rest, triangle))
                hess = {(1, 0): 1.0, (1, 1): 0.0, (2, 1): size}
            else:
                products = gather_end(k, k + 1)
                if k == 2:
                    products[0] = products[0] / triangle[0][0]
                triangle.append(heights(products, triangle))
            settle(k, powers[k], triangle[k])
            i = k - 1
            diagonal = triangle[k][i] * hess[(k, i)] / triangle[i][i]
            if i > 0:
                diagonal = diagonal + hess[(i, i)] - triangle[i][i - 1] * hess[(i, i - 1)] / triangle[i - 1][i - 1]
            alphas.append(diagonal)
            betas.append(triangle[k][k] * hess[(k, i)] / triangle[i][i])
        if j < ITERS:
            exchange_end((j + 1) % 2)
            side = powers if j % 2 else turned
            new = out[...] - alphas[j - 2] * side[j]
            lead = betas[j - 2]
            if j == 2:
                lead = lead * triangle[0][0]
            else:
                behind = betas[j - 3]
                if j == 3:
                    behind = behind / triangle[0][0]
                new = new - behind * side[j - 1]
            new = new * (1.0 / lead)
            if j + 1 == ITERS:
                powers[ITERS] = swap(new) if j % 2 == 0 else new
            else:
                side[j + 1] = new
            hess[(j, j)], hess[(j + 1, j)] = alphas[j - 2], lead

    s, l = iota((8, 128), 0), iota((8, 128), 1)
    tile = jnp.zeros((8, 128), F32)
    for j in range(ITERS):
        tile = jnp.where((s == 0) & (l == j), alphas[j], jnp.where((s == 1) & (l == j), betas[j], tile))
    small[...] = tile[0:2, 0:ITERS]
    last = pltpu.make_async_copy(small, coefficients_ref, out_sem.at[ITERS])
    last.start()
    for i in range(1, ITERS + 1):
        leaving(i).wait()
    last.wait()


def message_counts(x, y, z):
    return x + y + z + y * z, x * (y + z + y * z)


def shards(sizes, start, stencils):
    nx, ny, nz = sizes
    hbm = pl.BlockSpec(memory_space=pltpu.HBM)
    anyw = pl.BlockSpec(memory_space=pl.ANY)
    basis, coefficients = pl.pallas_call(
        functools.partial(kernel, sizes),
        out_shape=(
            jax.ShapeDtypeStruct((ITERS, C, C * C), F32),
            jax.ShapeDtypeStruct((2, ITERS), F32),
        ),
        in_specs=[hbm, hbm],
        out_specs=(anyw, anyw),
        scratch_shapes=[
            pltpu.VMEM((C, C * C), F32),
            pltpu.VMEM((6, C, C), F32),
            pltpu.VMEM((ITERS, C, C * C), F32),
            pltpu.VMEM((2, ITERS), F32),
            pltpu.VMEM((256, 128), F32),
            pltpu.VMEM((ITERS + 1, 256, 128), F32),
            pltpu.VMEM((ITERS, 256, 128), F32),
            pltpu.VMEM((ITERS, 256, 128), F32),
            pltpu.VMEM((256, 128), F32),
            pltpu.VMEM((2, 2 * C, 6 * C), BF16),
            pltpu.VMEM((2, 2 * C, 12 * C), BF16),
            pltpu.VMEM((256, 384), BF16),
            pltpu.VMEM((2, len(TILES), 8, 128), F32),
            pltpu.VMEM((2, len(ROWS), 128), F32),
            pltpu.VMEM((2, len(TILES), 8, 128), F32),
            pltpu.VMEM((2, len(ROWS), 128), F32),
            pltpu.VMEM((ITERS + 1, nx * ny * nz, 128), F32),
        ]
        + [pltpu.SemaphoreType.DMA((2, 2))] * 2
        + [pltpu.SemaphoreType.DMA((ITERS + 1,))] * 2
        + [pltpu.SemaphoreType.DMA((2,)), pltpu.SemaphoreType.DMA((ITERS + 1,))],
        compiler_params=pltpu.CompilerParams(collective_id=0, has_side_effects=True),
    )(start.reshape(C, C * C), stencils.reshape(6, C, C))
    return (
        basis.reshape(1, 1, 1, 1, ITERS, C, C * C),
        coefficients.reshape(1, 2, ITERS),
    )


def solution(mesh):
    sizes = tuple(mesh.shape[a] for a in AXES)
    return jax.shard_map(
        functools.partial(shards, sizes),
        mesh=mesh,
        in_specs=(P("gx", "gy", "gz", None, None, None), P(None, "gx", "gy", "gz", None, None)),
        out_specs=(P("gx", "gy", "gz", None, None, None, None), P()),
        check_vma=False,
    )
```

```python
import functools
import itertools

import jax
import jax.numpy as jnp
from jax import lax
from jax.experimental import pallas as pl
from jax.experimental.pallas import tpu as pltpu
from jax.sharding import PartitionSpec as P

ITERS = 5
C = 32
MESH = pl.DeviceIdType.MESH
F32 = jnp.float32
BF16 = jnp.bfloat16
AXES = ("gx", "gy", "gz")
DIRS = [
    (dx, dy, dz)
    for dx in (-1, 0, 1)
    for dy in (-1, 0, 1)
    for dz in (-1, 0, 1)
    if (dx, dy, dz) != (0, 0, 0)
]
TILES = [d for d in DIRS if d[0] == 0 or d[1:] == (0, 0)]
ROWS = [d for d in DIRS if d not in TILES]
SLOT = {d: i for dirs in (TILES, ROWS) for i, d in enumerate(dirs)}
SHRINK = 2.0**-17


def iota(shape, dim):
    return lax.broadcasted_iota(jnp.int32, shape, dim)


def roll(x, shift, axis):
    size = x.shape[axis]
    shift = shift % size
    return x if shift == 0 else pltpu.roll(x, shift, axis)


def swap(field):
    x = field.reshape(32, 8, 128)
    s, l = iota((1, 8, 128), 1), iota((1, 8, 128), 2)
    s1, l1 = (s // 2) % 2, l // 64
    r = roll(x, 64, 2)
    x = jnp.where(s1 == l1, x, jnp.where(s1 == 0, roll(r, -2, 1), roll(r, 2, 1)))
    s0, l0 = s % 2, (l // 32) % 2
    up, down = roll(roll(x, 32, 2), -1, 1), roll(roll(x, -32, 2), 1, 1)
    x = jnp.where(s0 == l0, x, jnp.where(s0 == 0, up, down))
    even = jnp.concatenate([x[t * 4 : t * 4 + 4] for t in range(0, 8, 2)], axis=0)
    odd = jnp.concatenate([x[t * 4 : t * 4 + 4] for t in range(1, 8, 2)], axis=0)
    half = s < 4
    top = jnp.where(half, even, roll(odd, 4, 1))
    bottom = jnp.where(half, roll(even, 4, 1), odd)
    parts = []
    for ai in range(4):
        for part in (top, bottom):
            for k in range(4):
                parts.append(part[k * 4 + ai : k * 4 + ai + 1])
    return jnp.concatenate(parts, axis=0).reshape(256, 128)


def wide(field):
    return jnp.concatenate([field[t * 32 : t * 32 + 32] for t in range(8)], axis=1)


def tall(field):
    return jnp.concatenate([field[:, t * 128 : t * 128 + 128] for t in range(8)], axis=0)


def split(x):
    high = x.astype(BF16)
    rest = x - high.astype(F32)
    middle = rest.astype(BF16)
    return high, middle, (rest - middle.astype(F32)).astype(BF16)


PAIRS = ((0, 0), (0, 1), (1, 0), (1, 1), (0, 2), (2, 0))


def dot(left, right):
    return jnp.dot(left, right, preferred_element_type=F32)


def spread(matrix):
    parts = split(matrix)
    return jnp.concatenate([parts[i] for i, _ in PAIRS], axis=1)


def stack(field):
    parts = split(field)
    return jnp.concatenate([parts[i] for _, i in PAIRS], axis=0)


def matvec(field, first_ref, second_ref, zmat_ref):
    first = dot(first_ref[...], stack(wide(field)))
    mass, stiff = swap(tall(first[:C])), swap(tall(first[C:]))
    second = dot(second_ref[...], stack(jnp.concatenate([wide(stiff), wide(mass)], axis=0)))
    third = jnp.concatenate([tall(second[:C]), tall(second[C:])], axis=1)
    high, middle, low = split(third)
    pair = zmat_ref[:, 0:256]
    both = dot(high, pair) + dot(middle, pair)
    rest = dot(low, zmat_ref[:, 0:128]) + dot(high, zmat_ref[:, 256:384])
    return both[:, :128] + (both[:, 128:] + rest)


def block_diagonal(matrix):
    zero = jnp.zeros((C, C), F32)
    rows = []
    for i in range(4):
        rows.append(jnp.concatenate([matrix if k == i else zero for k in range(4)], axis=1))
    return jnp.concatenate(rows, axis=0)


def weight_field(sizes, here):
    row, lane = iota((256, 128), 0), iota((256, 128), 1)
    places = (row % C, (row // C) * 4 + lane // C, lane % C)
    weight = jnp.ones((256, 128), F32)
    for place, size, at in zip(places, sizes, here):
        low = jnp.where(at > 0, 0.5, 1.0).astype(F32)
        high = jnp.where(at < size - 1, 0.5, 1.0).astype(F32)
        weight = weight * jnp.where(place == 0, low, jnp.where(place == C - 1, high, 1.0))
    return weight


def neighbour(sizes, here, step):
    fine = None
    for size, at, d in zip(sizes, here, step):
        if d != 0:
            inside = at > 0 if d < 0 else at < size - 1
            fine = inside if fine is None else jnp.logical_and(fine, inside)
    return fine, tuple(at + d for at, d in zip(here, step))


def pack(out_ref, tile_ref, row_ref):
    s, l = iota((8, 128), 0), iota((8, 128), 1)
    line = iota((1, 128), 1)
    lower = lambda t, ai: out_ref[pl.ds(t * 32 + ai * 8, 8), :]
    zero = jnp.zeros((8, 128), F32)
    low, high = zero, zero
    for t in range(8):
        for ai in range(4):
            r = ai * 8 + t
            moved = roll(lower(t, ai), r, 1)
            low = jnp.where(l % C == r, moved, low)
            high = jnp.where(l % C == (r + C - 1) % C, moved, high)

    def send_row(d, plane, source, keep):
        row_ref[pl.ds(SLOT[d], 1), :] = jnp.where(keep, plane[source : source + 1], 0.0)

    for dx in (-1, 1):
        source = 0 if dx < 0 else 7
        for dz, plane, base in ((-1, low, 0), (1, high, -31)):
            for dy in (-1, 0, 1):
                keep = (line % C) // 8 == (3 if dx < 0 else 0)
                if dy != 0:
                    keep = keep & (line // C == (3 if dy < 0 else 0)) & (line % 8 == (7 if dy < 0 else 0))
                send_row((dx, dy, dz), roll(plane, base - dx * 24 - dy * 103, 1), source, keep)
        plane = out_ref[pl.ds(0 if dx < 0 else C - 1, 8, stride=C), :]
        tile_ref[SLOT[(dx, 0, 0)]] = plane
        for dy in (-1, 1):
            keep = line // C == (3 if dy < 0 else 0)
            send_row((dx, dy, 0), roll(plane, 96 if dy < 0 else 32, 1), 0 if dy < 0 else 7, keep)
    for dz, plane, base in ((-1, low, 0), (1, high, -31)):
        tile_ref[SLOT[(0, 0, dz)]] = roll(plane, base, 1)
        for dy in (-1, 1):
            keep = (l // C == (3 if dy < 0 else 0)) & (l % 8 == (7 if dy < 0 else 0))
            tile_ref[SLOT[(0, dy, dz)]] = jnp.where(keep, roll(plane, base - dy * 103, 1), 0.0)
    for dy in (-1, 1):
        plane = zero
        for ai in range(4):
            piece = roll(lower(0 if dy < 0 else 7, ai), C * (ai + (0 if dy < 0 else 1)), 1)
            plane = jnp.where(l // C == ai, piece, plane)
        tile_ref[SLOT[(0, dy, 0)]] = plane


def unpack(out_ref, tile_ref, row_ref):
    s, l = iota((8, 128), 0), iota((8, 128), 1)
    near = (-1, 0, 1)
    got = lambda *d: tile_ref[SLOT[d]]
    row = lambda *d: row_ref[pl.ds(SLOT[d], 1), :]
    ends = lambda last, first: jnp.where(s == 7, last, jnp.where(s == 0, first, 0.0))
    for dx in (-1, 1):
        plane = got(dx, 0, 0) + ends(row(dx, -1, 0), row(dx, 1, 0))
        rows = pl.ds(C - 1 if dx < 0 else 0, 8, stride=C)
        out_ref[rows, :] = out_ref[rows, :] + plane
    low, high = (
        sum(got(0, dy, dz) for dy in near)
        + ends(sum(row(-1, dy, dz) for dy in near), sum(row(1, dy, dz) for dy in near))
        for dz in (1, -1)
    )
    first, last = got(0, 1, 0), got(0, -1, 0)
    for t in range(8):
        for ai in range(4):
            r = ai * 8 + t
            rows = pl.ds(t * 32 + ai * 8, 8)
            add = jnp.where(l % C == 0, roll(low, -r, 1), 0.0)
            add = add + jnp.where(l % C == C - 1, roll(high, 31 - r, 1), 0.0)
            if t == 0:
                add = add + jnp.where(l < C, roll(first, -C * ai, 1), 0.0)
            if t == 7:
                add = add + jnp.where(l >= 96, roll(last, 96 - C * ai, 1), 0.0)
            out_ref[rows, :] = out_ref[rows, :] + add


def kernel(
    sizes,
    start_hbm,
    stencils_hbm,
    basis_ref,
    coefficients_ref,
    start_ref,
    stencils_ref,
    wides,
    small,
    out,
    powers,
    turned,
    vecs,
    turned_vecs,
    turned_weights,
    weights,
    first,
    second,
    zmat,
    tiles,
    rows,
    got_tiles,
    got_rows,
    terms,
    marks,
    send_sem,
    got_sem,
    term_send,
    term_got,
    mark_send,
    mark_got,
    in_sem,
    out_sem,
):
    here = tuple(lax.axis_index(a) for a in AXES)
    nx, ny, nz = sizes
    gx, gy, gz = here
    me = (gx * ny + gy) * nz + gz
    hops = lambda k, size: min(k, size - k)
    steps = sorted(
        ((i, j, k) for i in range(nx) for j in range(ny) for k in range(nz)),
        key=lambda d: -(hops(d[0], nx) + hops(d[1], ny) + hops(d[2], nz) / 2),
    )
    along = [[lax.rem(at + k, size) for k in range(size)] for at, size in zip(here, sizes)]
    everyone = [tuple(along[a][d[a]] for a in range(3)) for d in steps if any(d)]
    beside = [
        jnp.where(at > 0, 1, 0) + jnp.where(at < size - 1, 1, 0) for at, size in zip(here, sizes)
    ]

    inputs = [
        pltpu.make_async_copy(start_hbm, start_ref, in_sem.at[0]),
        pltpu.make_async_copy(stencils_hbm, stencils_ref, in_sem.at[1]),
    ]
    for copy in inputs:
        copy.start()
    got_tiles[...] = jnp.zeros_like(got_tiles)
    got_rows[...] = jnp.zeros_like(got_rows)
    barrier = pltpu.get_barrier_semaphore()
    line = [(gx, gy, lax.rem(gz + k, nz)) for k in range(1, nz)]
    plane = [
        (along[0][i], along[1][k], gz) for i in range(nx) for k in range(ny) if (i, k) != (0, 0)
    ]
    for there in plane + line:
        pl.semaphore_signal(barrier, inc=1, device_id=there, device_id_type=MESH)
    for d in DIRS:
        if d[2] != 0 and d[:2] != (0, 0):
            fine, there = neighbour(sizes, here, d)

            @pl.when(fine)
            def _():
                pl.semaphore_signal(barrier, inc=1, device_id=there, device_id_type=MESH)

    greetings = len(plane) + len(line) + beside[2] * ((1 + beside[0]) * (1 + beside[1]) - 1)

    weights[...] = weight_field(sizes, here)
    for copy in inputs:
        copy.wait()
    kx, ky, kz, mx, my, mz = (stencils_ref[i] for i in range(6))
    empty = jnp.zeros((C, C), F32)
    for i, (mass, stiff) in enumerate(((mx, kx), (my, ky))):
        first[i] = spread(jnp.concatenate([mass, stiff], axis=0))
        upper, lower = (jnp.concatenate(p, axis=1) for p in ((mass, stiff), (empty, mass)))
        second[1 - i] = spread(jnp.concatenate([upper, lower], axis=0))
    zmat[...] = jnp.concatenate(
        split(jnp.concatenate([block_diagonal(mz.T), block_diagonal(kz.T)], axis=0)), axis=1
    )

    def exchange_start(par):
        pack(out, tiles.at[par], rows.at[par])
        for d in sorted(DIRS, key=lambda d: -sum(abs(i) for i in d)):
            fine, there = neighbour(sizes, here, (d[1], d[0], d[2]) if par else d)
            if d in TILES:
                source, target = tiles.at[par, SLOT[d]], got_tiles.at[par, SLOT[d]]
            else:
                source, target = rows.at[par, pl.ds(SLOT[d], 1)], got_rows.at[par, pl.ds(SLOT[d], 1)]

            @pl.when(fine)
            def _():
                pltpu.make_async_remote_copy(
                    src_ref=source,
                    dst_ref=target,
                    send_sem=send_sem.at[par, int(d in ROWS)],
                    recv_sem=got_sem.at[par, int(d in ROWS)],
                    device_id=there,
                    device_id_type=MESH,
                ).start()

    def exchange_end(par):
        order = (1, 0, 2) if par else (0, 1, 2)
        counts = message_counts(*(beside[i] for i in order))
        choices = [{0} if n == 1 else {1} if n == 2 else {1, 2} for n in (sizes[i] for i in order)]
        for n, m in sorted({message_counts(*c) for c in itertools.product(*choices)}):

            @pl.when((counts[0] == n) & (counts[1] == m))
            def _():
                for kind, (count, sent, got) in enumerate(((n, tiles, got_tiles), (m, rows, got_rows))):
                    if count:
                        both = pltpu.make_async_remote_copy(
                            src_ref=sent.at[par, pl.ds(0, count)],
                            dst_ref=got.at[par, pl.ds(0, count)],
                            send_sem=send_sem.at[par, kind],
                            recv_sem=got_sem.at[par, kind],
                            device_id=everyone[0],
                            device_id_type=MESH,
                        )
                        both.wait_recv()
                        both.wait_send()

        unpack(out, got_tiles.at[par], got_rows.at[par])

    def gather_start(k, pairs):
        s, l = iota((8, 128), 0), iota((8, 128), 1)
        tile = jnp.zeros((8, 128), F32)
        for i, (left, right) in enumerate(pairs):
            lanes = jnp.sum(jnp.sum((left * right).reshape(32, 8, 128), axis=0), axis=0, keepdims=True)
            tile = jnp.where(s == i, lanes, tile)
        column = jnp.sum(tile, axis=1, keepdims=True)
        gather_row(k, jnp.sum(jnp.where(s == l, column, 0.0), axis=0, keepdims=True))

    def gather_row(k, row):
        mine = pl.ds(me, 1)
        terms[k, mine] = row
        for there in everyone:
            pltpu.make_async_remote_copy(
                src_ref=terms.at[k, mine],
                dst_ref=terms.at[k, mine],
                send_sem=term_send.at[k],
                recv_sem=term_got.at[k],
                device_id=there,
                device_id_type=MESH,
            ).start()

    def mark_start(k, at, peers, row):
        marks[k, pl.ds(at, 1)] = row
        for there in peers:
            pltpu.make_async_remote_copy(
                src_ref=marks.at[k, pl.ds(at, 1)],
                dst_ref=marks.at[k, pl.ds(at, 1)],
                send_sem=mark_send.at[k],
                recv_sem=mark_got.at[k],
                device_id=there,
                device_id_type=MESH,
            ).start()

    def mark_end(k, peers):
        if peers:
            both = pltpu.make_async_remote_copy(
                src_ref=marks.at[k, pl.ds(0, len(peers))],
                dst_ref=marks.at[k, pl.ds(0, len(peers))],
                send_sem=mark_send.at[k],
                recv_sem=mark_got.at[k],
                device_id=peers[0],
                device_id_type=MESH,
            )
            both.wait_recv()
            both.wait_send()
        return jnp.sum(marks[k, 0 : len(peers) + 1], axis=0, keepdims=True)

    def gather_end(k, count):
        others = pl.ds(0, len(everyone))
        both = pltpu.make_async_remote_copy(
            src_ref=terms.at[k, others],
            dst_ref=terms.at[k, others],
            send_sem=term_send.at[k],
            recv_sem=term_got.at[k],
            device_id=everyone[0],
            device_id_type=MESH,
        )
        both.wait_recv()
        both.wait_send()
        row = jnp.sum(terms[k], axis=0, keepdims=True)
        s, l = iota((8, 128), 0), iota((8, 128), 1)
        column = jnp.sum(jnp.where(s == l, row, 0.0), axis=1, keepdims=True)
        return [column[i : i + 1] for i in range(count)]

    def leaving(i):
        return pltpu.make_async_copy(wides.at[i - 1], basis_ref.at[i - 1], out_sem.at[i - 1])

    def settle(i, image, height):
        new = image
        for k in range(i):
            new = new - height[k] * vecs[k]
        new = new * (1.0 / height[i])
        if i < ITERS:
            vecs[i] = new
        if i < ITERS - 1:
            turned_vecs[i] = swap(new)
        if i > 0:
            wides[i - 1] = wide(new)
            leaving(i).start()

    def heights(products, known):
        *with_known, with_last, square = products
        i = len(known)
        found = list(with_known)
        last = with_last
        for k in range(i - 1):
            last = last - known[i - 1][k] * found[k]
        found.append(last / known[i - 1][i - 1])
        for value in found:
            square = square - value * value
        found.append(jnp.sqrt(square))
        return found

    out[...] = tall(start_ref[...]) * weights[...] * SHRINK
    pl.semaphore_wait(barrier, greetings)
    exchange_start(0)
    trace = [jnp.sum(jnp.where(iota((C, C), 0) == iota((C, C), 1), m, 0.0), keepdims=True) / C for m in (kx, ky, kz, mx, my, mz)]
    mean = trace[0] * trace[4] * trace[5] + trace[3] * trace[1] * trace[5] + trace[3] * trace[4] * trace[2]
    mark_start(0, gz, line, jnp.broadcast_to(mean / (nx * ny * nz), (1, 128)))
    exchange_end(0)
    powers[0] = out[...]
    mark_start(1, gx * ny + gy, plane, mark_end(0, line))

    def apply(j):
        here = (turned if j % 2 else powers)[j]
        out[...] = matvec(here, first.at[j % 2], second.at[j % 2], zmat)
        exchange_start((j + 1) % 2)

    def turn(j):
        if j % 2:
            powers[j] = swap(turned[j])
        else:
            turned[j] = swap(powers[j])

    apply(0)
    exchange_end(1)
    turned[1] = out[...]

    apply(1)
    turn(1)
    turned_weights[...] = swap(weights[...])
    size = mark_end(1, plane)
    weighted = weights[...] * powers[1]
    gather_start(1, [(powers[0], weights[...] * powers[0]), (powers[0], weighted), (powers[1], weighted)])
    exchange_end(0)
    powers[2] = out[...] * (1.0 / size)

    triangle, alphas, betas = [], [], []
    for j in range(2, ITERS + 1):
        if j < ITERS:
            apply(j)
            turn(j)
        if j < ITERS:
            weighted = weights[...] * powers[j]
            earlier = [vecs[k] if j > 2 else powers[0] for k in range(j - 1)] + [powers[j - 1]]
            image = powers[j]
        else:
            weighted = turned_weights[...] * turned[j]
            earlier = [turned_vecs[k] for k in range(j - 1)] + [turned[j - 1]]
            image = turned[j]
        if j == 2:
            earlier = [powers[0], powers[1]]
        gather_start(j, [(v, weighted) for v in earlier + [image]])
        if j == ITERS:
            powers[j] = swap(image)
        rounds = [j - 1] if j < ITERS else [j - 1, j]
        for k in rounds:
            if k == 1:
                square, *rest = gather_end(1, 3)
                triangle.append([jnp.sqrt(square)])
                settle(0, powers[0], triangle[0])
                triangle.append(heights(rest, triangle))
                hess = {(1, 0): 1.0, (1, 1): 0.0, (2, 1): size}
            else:
                products = gather_end(k, k + 1)
                if k == 2:
                    products[0] = products[0] / triangle[0][0]
                triangle.append(heights(products, triangle))
            settle(k, powers[k], triangle[k])
            i = k - 1
            diagonal = triangle[k][i] * hess[(k, i)] / triangle[i][i]
            if i > 0:
                diagonal = diagonal + hess[(i, i)] - triangle[i][i - 1] * hess[(i, i - 1)] / triangle[i - 1][i - 1]
            alphas.append(diagonal)
            betas.append(triangle[k][k] * hess[(k, i)] / triangle[i][i])
        if j < ITERS:
            exchange_end((j + 1) % 2)
            side = powers if j % 2 else turned
            new = out[...] - alphas[j - 2] * side[j]
            lead = betas[j - 2]
            if j == 2:
                lead = lead * triangle[0][0]
            else:
                behind = betas[j - 3]
                if j == 3:
                    behind = behind / triangle[0][0]
                new = new - behind * side[j - 1]
            new = new * (1.0 / lead)
            side[j + 1] = new
            hess[(j, j)], hess[(j + 1, j)] = alphas[j - 2], lead

    s, l = iota((8, 128), 0), iota((8, 128), 1)
    tile = jnp.zeros((8, 128), F32)
    for j in range(ITERS):
        tile = jnp.where((s == 0) & (l == j), alphas[j], jnp.where((s == 1) & (l == j), betas[j], tile))
    small[...] = tile[0:2, 0:ITERS]
    last = pltpu.make_async_copy(small, coefficients_ref, out_sem.at[ITERS])
    last.start()
    for i in range(1, ITERS + 1):
        leaving(i).wait()
    last.wait()


def message_counts(x, y, z):
    return x + y + z + y * z, x * (y + z + y * z)


def hand_over(basis_in, coefficients_in, basis_out, coefficients_out, wides, small, in_sem, out_sem):
    pairs = [(basis_in.at[i], wides.at[i], basis_out.at[i]) for i in range(ITERS)]
    pairs.append((coefficients_in, small, coefficients_out))
    come = [pltpu.make_async_copy(a, b, in_sem.at[i]) for i, (a, b, _) in enumerate(pairs)]
    go = [pltpu.make_async_copy(b, c, out_sem.at[i]) for i, (_, b, c) in enumerate(pairs)]
    for copy in come:
        copy.start()
    for first, then in zip(come, go):
        first.wait()
        then.start()
    for copy in go:
        copy.wait()


def shards(sizes, start, stencils):
    nx, ny, nz = sizes
    hbm = pl.BlockSpec(memory_space=pltpu.HBM)
    anyw = pl.BlockSpec(memory_space=pl.ANY)
    basis, coefficients = pl.pallas_call(
        functools.partial(kernel, sizes),
        out_shape=(
            jax.ShapeDtypeStruct((ITERS, C, C * C), F32),
            jax.ShapeDtypeStruct((2, ITERS), F32),
        ),
        in_specs=[hbm, hbm],
        out_specs=(anyw, anyw),
        scratch_shapes=[
            pltpu.VMEM((C, C * C), F32),
            pltpu.VMEM((6, C, C), F32),
            pltpu.VMEM((ITERS, C, C * C), F32),
            pltpu.VMEM((2, ITERS), F32),
            pltpu.VMEM((256, 128), F32),
            pltpu.VMEM((ITERS + 1, 256, 128), F32),
            pltpu.VMEM((ITERS + 1, 256, 128), F32),
            pltpu.VMEM((ITERS, 256, 128), F32),
            pltpu.VMEM((ITERS - 1, 256, 128), F32),
            pltpu.VMEM((256, 128), F32),
            pltpu.VMEM((256, 128), F32),
            pltpu.VMEM((2, 2 * C, 6 * C), BF16),
            pltpu.VMEM((2, 2 * C, 12 * C), BF16),
            pltpu.VMEM((256, 384), BF16),
            pltpu.VMEM((2, len(TILES), 8, 128), F32),
            pltpu.VMEM((2, len(ROWS), 128), F32),
            pltpu.VMEM((2, len(TILES), 8, 128), F32),
            pltpu.VMEM((2, len(ROWS), 128), F32),
            pltpu.VMEM((ITERS + 1, nx * ny * nz, 128), F32),
            pltpu.VMEM((2, max(nx * ny, nz), 128), F32),
        ]
        + [pltpu.SemaphoreType.DMA((2, 2))] * 2
        + [pltpu.SemaphoreType.DMA((ITERS + 1,))] * 2
        + [pltpu.SemaphoreType.DMA((2,))] * 2
        + [pltpu.SemaphoreType.DMA((2,)), pltpu.SemaphoreType.DMA((ITERS + 1,))],
        compiler_params=pltpu.CompilerParams(collective_id=0, has_side_effects=True),
    )(start.reshape(C, C * C), stencils.reshape(6, C, C))
    basis, coefficients = pl.pallas_call(
        hand_over,
        out_shape=(
            jax.ShapeDtypeStruct((ITERS, C, C * C), F32),
            jax.ShapeDtypeStruct((2, ITERS), F32),
        ),
        in_specs=[anyw, anyw],
        out_specs=(anyw, anyw),
        scratch_shapes=[
            pltpu.VMEM((ITERS, C, C * C), F32),
            pltpu.VMEM((2, ITERS), F32),
            pltpu.SemaphoreType.DMA((ITERS + 1,)),
            pltpu.SemaphoreType.DMA((ITERS + 1,)),
        ],
    )(basis, coefficients)
    return (
        basis.reshape(1, 1, 1, 1, ITERS, C, C * C),
        coefficients.reshape(1, 2, ITERS),
    )


def solution(mesh):
    sizes = tuple(mesh.shape[a] for a in AXES)
    return jax.shard_map(
        functools.partial(shards, sizes),
        mesh=mesh,
        in_specs=(P("gx", "gy", "gz", None, None, None), P(None, "gx", "gy", "gz", None, None)),
        out_specs=(P("gx", "gy", "gz", None, None, None, None), P()),
        check_vma=False,
    )
```

```python
import functools
import itertools

import jax
import jax.numpy as jnp
from jax import lax
from jax.experimental import pallas as pl
from jax.experimental.pallas import tpu as pltpu
from jax.sharding import PartitionSpec as P

ITERS = 5
C = 32
MESH = pl.DeviceIdType.MESH
F32 = jnp.float32
BF16 = jnp.bfloat16
AXES = ("gx", "gy", "gz")
DIRS = [
    (dx, dy, dz)
    for dx in (-1, 0, 1)
    for dy in (-1, 0, 1)
    for dz in (-1, 0, 1)
    if (dx, dy, dz) != (0, 0, 0)
]
TILES = [d for d in DIRS if d[0] == 0 or d[1:] == (0, 0)]
ROWS = [d for d in DIRS if d not in TILES]
SLOT = {d: i for dirs in (TILES, ROWS) for i, d in enumerate(dirs)}
SHRINK = 2.0**-17


def iota(shape, dim):
    return lax.broadcasted_iota(jnp.int32, shape, dim)


def roll(x, shift, axis):
    size = x.shape[axis]
    shift = shift % size
    return x if shift == 0 else pltpu.roll(x, shift, axis)


def swap(field):
    x = field.reshape(32, 8, 128)
    s, l = iota((1, 8, 128), 1), iota((1, 8, 128), 2)
    s1, l1 = (s // 2) % 2, l // 64
    r = roll(x, 64, 2)
    x = jnp.where(s1 == l1, x, jnp.where(s1 == 0, roll(r, -2, 1), roll(r, 2, 1)))
    s0, l0 = s % 2, (l // 32) % 2
    up, down = roll(roll(x, 32, 2), -1, 1), roll(roll(x, -32, 2), 1, 1)
    x = jnp.where(s0 == l0, x, jnp.where(s0 == 0, up, down))
    even = jnp.concatenate([x[t * 4 : t * 4 + 4] for t in range(0, 8, 2)], axis=0)
    odd = jnp.concatenate([x[t * 4 : t * 4 + 4] for t in range(1, 8, 2)], axis=0)
    half = s < 4
    top = jnp.where(half, even, roll(odd, 4, 1))
    bottom = jnp.where(half, roll(even, 4, 1), odd)
    parts = []
    for ai in range(4):
        for part in (top, bottom):
            for k in range(4):
                parts.append(part[k * 4 + ai : k * 4 + ai + 1])
    return jnp.concatenate(parts, axis=0).reshape(256, 128)


def wide(field):
    return jnp.concatenate([field[t * 32 : t * 32 + 32] for t in range(8)], axis=1)


def tall(field):
    return jnp.concatenate([field[:, t * 128 : t * 128 + 128] for t in range(8)], axis=0)


def split(x):
    high = x.astype(BF16)
    rest = x - high.astype(F32)
    middle = rest.astype(BF16)
    return high, middle, (rest - middle.astype(F32)).astype(BF16)


PAIRS = ((0, 0), (0, 1), (1, 0), (1, 1), (0, 2), (2, 0))


def dot(left, right):
    return jnp.dot(left, right, preferred_element_type=F32)


def spread(matrix):
    parts = split(matrix)
    return jnp.concatenate([parts[i] for i, _ in PAIRS], axis=1)


def stack(field):
    parts = split(field)
    return jnp.concatenate([parts[i] for _, i in PAIRS], axis=0)


def matvec(field, first_ref, second_ref, zmat_ref):
    first = dot(first_ref[...], stack(wide(field)))
    mass, stiff = swap(tall(first[:C])), swap(tall(first[C:]))
    second = dot(second_ref[...], stack(jnp.concatenate([wide(stiff), wide(mass)], axis=0)))
    third = jnp.concatenate([tall(second[:C]), tall(second[C:])], axis=1)
    high, middle, low = split(third)
    pair = zmat_ref[:, 0:256]
    both = dot(high, pair) + dot(middle, pair)
    rest = dot(low, zmat_ref[:, 0:128]) + dot(high, zmat_ref[:, 256:384])
    return both[:, :128] + (both[:, 128:] + rest)


def block_diagonal(matrix):
    zero = jnp.zeros((C, C), F32)
    rows = []
    for i in range(4):
        rows.append(jnp.concatenate([matrix if k == i else zero for k in range(4)], axis=1))
    return jnp.concatenate(rows, axis=0)


def weight_field(sizes, here):
    row, lane = iota((256, 128), 0), iota((256, 128), 1)
    places = (row % C, (row // C) * 4 + lane // C, lane % C)
    weight = jnp.ones((256, 128), F32)
    for place, size, at in zip(places, sizes, here):
        low = jnp.where(at > 0, 0.5, 1.0).astype(F32)
        high = jnp.where(at < size - 1, 0.5, 1.0).astype(F32)
        weight = weight * jnp.where(place == 0, low, jnp.where(place == C - 1, high, 1.0))
    return weight


def neighbour(sizes, here, step):
    fine = None
    for size, at, d in zip(sizes, here, step):
        if d != 0:
            inside = at > 0 if d < 0 else at < size - 1
            fine = inside if fine is None else jnp.logical_and(fine, inside)
    return fine, tuple(at + d for at, d in zip(here, step))


def pack(out_ref, tile_ref, row_ref):
    s, l = iota((8, 128), 0), iota((8, 128), 1)
    line = iota((1, 128), 1)
    lower = lambda t, ai: out_ref[pl.ds(t * 32 + ai * 8, 8), :]
    zero = jnp.zeros((8, 128), F32)
    low, high = zero, zero
    for t in range(8):
        for ai in range(4):
            r = ai * 8 + t
            moved = roll(lower(t, ai), r, 1)
            low = jnp.where(l % C == r, moved, low)
            high = jnp.where(l % C == (r + C - 1) % C, moved, high)

    def send_row(d, plane, source, keep):
        row_ref[pl.ds(SLOT[d], 1), :] = jnp.where(keep, plane[source : source + 1], 0.0)

    for dx in (-1, 1):
        source = 0 if dx < 0 else 7
        for dz, plane, base in ((-1, low, 0), (1, high, -31)):
            for dy in (-1, 0, 1):
                keep = (line % C) // 8 == (3 if dx < 0 else 0)
                if dy != 0:
                    keep = keep & (line // C == (3 if dy < 0 else 0)) & (line % 8 == (7 if dy < 0 else 0))
                send_row((dx, dy, dz), roll(plane, base - dx * 24 - dy * 103, 1), source, keep)
        plane = out_ref[pl.ds(0 if dx < 0 else C - 1, 8, stride=C), :]
        tile_ref[SLOT[(dx, 0, 0)]] = plane
        for dy in (-1, 1):
            keep = line // C == (3 if dy < 0 else 0)
            send_row((dx, dy, 0), roll(plane, 96 if dy < 0 else 32, 1), 0 if dy < 0 else 7, keep)
    for dz, plane, base in ((-1, low, 0), (1, high, -31)):
        tile_ref[SLOT[(0, 0, dz)]] = roll(plane, base, 1)
        for dy in (-1, 1):
            keep = (l // C == (3 if dy < 0 else 0)) & (l % 8 == (7 if dy < 0 else 0))
            tile_ref[SLOT[(0, dy, dz)]] = jnp.where(keep, roll(plane, base - dy * 103, 1), 0.0)
    for dy in (-1, 1):
        plane = zero
        for ai in range(4):
            piece = roll(lower(0 if dy < 0 else 7, ai), C * (ai + (0 if dy < 0 else 1)), 1)
            plane = jnp.where(l // C == ai, piece, plane)
        tile_ref[SLOT[(0, dy, 0)]] = plane


def unpack(out_ref, tile_ref, row_ref):
    s, l = iota((8, 128), 0), iota((8, 128), 1)
    near = (-1, 0, 1)
    got = lambda *d: tile_ref[SLOT[d]]
    row = lambda *d: row_ref[pl.ds(SLOT[d], 1), :]
    ends = lambda last, first: jnp.where(s == 7, last, jnp.where(s == 0, first, 0.0))
    for dx in (-1, 1):
        plane = got(dx, 0, 0) + ends(row(dx, -1, 0), row(dx, 1, 0))
        rows = pl.ds(C - 1 if dx < 0 else 0, 8, stride=C)
        out_ref[rows, :] = out_ref[rows, :] + plane
    low, high = (
        sum(got(0, dy, dz) for dy in near)
        + ends(sum(row(-1, dy, dz) for dy in near), sum(row(1, dy, dz) for dy in near))
        for dz in (1, -1)
    )
    first, last = got(0, 1, 0), got(0, -1, 0)
    for t in range(8):
        for ai in range(4):
            r = ai * 8 + t
            rows = pl.ds(t * 32 + ai * 8, 8)
            add = jnp.where(l % C == 0, roll(low, -r, 1), 0.0)
            add = add + jnp.where(l % C == C - 1, roll(high, 31 - r, 1), 0.0)
            if t == 0:
                add = add + jnp.where(l < C, roll(first, -C * ai, 1), 0.0)
            if t == 7:
                add = add + jnp.where(l >= 96, roll(last, 96 - C * ai, 1), 0.0)
            out_ref[rows, :] = out_ref[rows, :] + add


def kernel(
    sizes,
    start_hbm,
    stencils_hbm,
    basis_ref,
    coefficients_ref,
    start_ref,
    stencils_ref,
    wides,
    small,
    out,
    powers,
    turned,
    vecs,
    turned_vecs,
    turned_weights,
    lifted,
    turned_lifted,
    images,
    shifting,
    weights,
    first,
    second,
    zmat,
    tiles,
    rows,
    got_tiles,
    got_rows,
    terms,
    marks,
    send_sem,
    got_sem,
    term_send,
    term_got,
    mark_send,
    mark_got,
    in_sem,
    out_sem,
):
    here = tuple(lax.axis_index(a) for a in AXES)
    nx, ny, nz = sizes
    gx, gy, gz = here
    me = (gx * ny + gy) * nz + gz
    hops = lambda k, size: min(k, size - k)
    steps = sorted(
        ((i, j, k) for i in range(nx) for j in range(ny) for k in range(nz)),
        key=lambda d: -(hops(d[0], nx) + hops(d[1], ny) + hops(d[2], nz) / 2),
    )
    along = [[lax.rem(at + k, size) for k in range(size)] for at, size in zip(here, sizes)]
    everyone = [tuple(along[a][d[a]] for a in range(3)) for d in steps if any(d)]
    beside = [
        jnp.where(at > 0, 1, 0) + jnp.where(at < size - 1, 1, 0) for at, size in zip(here, sizes)
    ]

    inputs = [
        pltpu.make_async_copy(start_hbm, start_ref, in_sem.at[0]),
        pltpu.make_async_copy(stencils_hbm, stencils_ref, in_sem.at[1]),
    ]
    for copy in inputs:
        copy.start()
    got_tiles[...] = jnp.zeros_like(got_tiles)
    got_rows[...] = jnp.zeros_like(got_rows)
    barrier = pltpu.get_barrier_semaphore()
    line = [(gx, gy, lax.rem(gz + k, nz)) for k in range(1, nz)]
    plane = [
        (along[0][i], along[1][k], gz) for i in range(nx) for k in range(ny) if (i, k) != (0, 0)
    ]
    for there in plane + line:
        pl.semaphore_signal(barrier, inc=1, device_id=there, device_id_type=MESH)
    for d in DIRS:
        if d[2] != 0 and d[:2] != (0, 0):
            fine, there = neighbour(sizes, here, d)

            @pl.when(fine)
            def _():
                pl.semaphore_signal(barrier, inc=1, device_id=there, device_id_type=MESH)

    greetings = len(plane) + len(line) + beside[2] * ((1 + beside[0]) * (1 + beside[1]) - 1)

    weights[...] = weight_field(sizes, here)
    for copy in inputs:
        copy.wait()
    kx, ky, kz, mx, my, mz = (stencils_ref[i] for i in range(6))
    empty = jnp.zeros((C, C), F32)
    for i, (mass, stiff) in enumerate(((mx, kx), (my, ky))):
        first[i] = spread(jnp.concatenate([mass, stiff], axis=0))
        upper, lower = (jnp.concatenate(p, axis=1) for p in ((mass, stiff), (empty, mass)))
        second[1 - i] = spread(jnp.concatenate([upper, lower], axis=0))
    zmat[...] = jnp.concatenate(
        split(jnp.concatenate([block_diagonal(mz.T), block_diagonal(kz.T)], axis=0)), axis=1
    )

    def exchange_start(par):
        pack(out, tiles.at[par], rows.at[par])
        for d in sorted(DIRS, key=lambda d: -sum(abs(i) for i in d)):
            fine, there = neighbour(sizes, here, (d[1], d[0], d[2]) if par else d)
            if d in TILES:
                source, target = tiles.at[par, SLOT[d]], got_tiles.at[par, SLOT[d]]
            else:
                source, target = rows.at[par, pl.ds(SLOT[d], 1)], got_rows.at[par, pl.ds(SLOT[d], 1)]

            @pl.when(fine)
            def _():
                pltpu.make_async_remote_copy(
                    src_ref=source,
                    dst_ref=target,
                    send_sem=send_sem.at[par, int(d in ROWS)],
                    recv_sem=got_sem.at[par, int(d in ROWS)],
                    device_id=there,
                    device_id_type=MESH,
                ).start()

    def exchange_end(par):
        order = (1, 0, 2) if par else (0, 1, 2)
        counts = message_counts(*(beside[i] for i in order))
        choices = [{0} if n == 1 else {1} if n == 2 else {1, 2} for n in (sizes[i] for i in order)]
        for n, m in sorted({message_counts(*c) for c in itertools.product(*choices)}):

            @pl.when((counts[0] == n) & (counts[1] == m))
            def _():
                for kind, (count, sent, got) in enumerate(((n, tiles, got_tiles), (m, rows, got_rows))):
                    if count:
                        both = pltpu.make_async_remote_copy(
                            src_ref=sent.at[par, pl.ds(0, count)],
                            dst_ref=got.at[par, pl.ds(0, count)],
                            send_sem=send_sem.at[par, kind],
                            recv_sem=got_sem.at[par, kind],
                            device_id=everyone[0],
                            device_id_type=MESH,
                        )
                        both.wait_recv()
                        both.wait_send()

        unpack(out, got_tiles.at[par], got_rows.at[par])

    def gather_start(k, pairs):
        s, l = iota((8, 128), 0), iota((8, 128), 1)
        tile = jnp.zeros((8, 128), F32)
        for i, (left, right) in enumerate(pairs):
            lanes = jnp.sum(jnp.sum((left * right).reshape(32, 8, 128), axis=0), axis=0, keepdims=True)
            tile = jnp.where(s == i, lanes, tile)
        column = jnp.sum(tile, axis=1, keepdims=True)
        gather_row(k, jnp.sum(jnp.where(s == l, column, 0.0), axis=0, keepdims=True))

    def gather_row(k, row):
        mine = pl.ds(me, 1)
        terms[k, mine] = row
        for there in everyone:
            pltpu.make_async_remote_copy(
                src_ref=terms.at[k, mine],
                dst_ref=terms.at[k, mine],
                send_sem=term_send.at[k],
                recv_sem=term_got.at[k],
                device_id=there,
                device_id_type=MESH,
            ).start()

    def mark_start(k, at, peers, row):
        marks[k, pl.ds(at, 1)] = row
        for there in peers:
            pltpu.make_async_remote_copy(
                src_ref=marks.at[k, pl.ds(at, 1)],
                dst_ref=marks.at[k, pl.ds(at, 1)],
                send_sem=mark_send.at[k],
                recv_sem=mark_got.at[k],
                device_id=there,
                device_id_type=MESH,
            ).start()

    def mark_end(k, peers):
        if peers:
            both = pltpu.make_async_remote_copy(
                src_ref=marks.at[k, pl.ds(0, len(peers))],
                dst_ref=marks.at[k, pl.ds(0, len(peers))],
                send_sem=mark_send.at[k],
                recv_sem=mark_got.at[k],
                device_id=peers[0],
                device_id_type=MESH,
            )
            both.wait_recv()
            both.wait_send()
        return jnp.sum(marks[k, 0 : len(peers) + 1], axis=0, keepdims=True)

    def gather_end(k, count):
        others = pl.ds(0, len(everyone))
        both = pltpu.make_async_remote_copy(
            src_ref=terms.at[k, others],
            dst_ref=terms.at[k, others],
            send_sem=term_send.at[k],
            recv_sem=term_got.at[k],
            device_id=everyone[0],
            device_id_type=MESH,
        )
        both.wait_recv()
        both.wait_send()
        row = jnp.sum(terms[k], axis=0, keepdims=True)
        s, l = iota((8, 128), 0), iota((8, 128), 1)
        column = jnp.sum(jnp.where(s == l, row, 0.0), axis=1, keepdims=True)
        return [column[i : i + 1] for i in range(count)]

    def leaving(i):
        return pltpu.make_async_copy(wides.at[i - 1], basis_ref.at[i - 1], out_sem.at[i - 1])

    def settle(i, image, height):
        new = image
        for k in range(i):
            new = new - height[k] * vecs[k]
        new = new * (1.0 / height[i])
        if i < ITERS:
            vecs[i] = new
        if i < ITERS - 1:
            turned_vecs[i] = swap(new)
        if i > 0:
            wides[i - 1] = wide(new)
            leaving(i).start()

    def heights(products, known):
        *with_known, with_last, square = products
        i = len(known)
        found = list(with_known)
        last = with_last
        for k in range(i - 1):
            last = last - known[i - 1][k] * found[k]
        found.append(last / known[i - 1][i - 1])
        for value in found:
            square = square - value * value
        found.append(jnp.sqrt(square))
        return found

    out[...] = tall(start_ref[...]) * weights[...] * SHRINK
    pl.semaphore_wait(barrier, greetings)
    exchange_start(0)
    trace = [jnp.sum(jnp.where(iota((C, C), 0) == iota((C, C), 1), m, 0.0), keepdims=True) / C for m in (kx, ky, kz, mx, my, mz)]
    mean = trace[0] * trace[4] * trace[5] + trace[3] * trace[1] * trace[5] + trace[3] * trace[4] * trace[2]
    mark_start(0, gz, line, jnp.broadcast_to(mean / (nx * ny * nz), (1, 128)))
    exchange_end(0)
    powers[0] = out[...]
    mark_start(1, gx * ny + gy, plane, mark_end(0, line))

    def apply(j):
        here = (turned if j % 2 else powers)[j]
        out[...] = matvec(here, first.at[j % 2], second.at[j % 2], zmat)
        exchange_start((j + 1) % 2)

    def turn(j):
        if j % 2:
            powers[j] = swap(turned[j])
        else:
            turned[j] = swap(powers[j])

    apply(0)
    exchange_end(1)
    turned[1] = out[...]

    apply(1)
    turn(1)
    turned_weights[...] = swap(weights[...])
    size = mark_end(1, plane)
    weighted = weights[...] * powers[1]
    gather_start(1, [(powers[0], weights[...] * powers[0]), (powers[0], weighted), (powers[1], weighted)])
    exchange_end(0)
    powers[2] = out[...] * (1.0 / size)

    triangle, alphas, betas = [], [], []
    shifts = {2: size}
    for j in range(2, ITERS + 1):
        if j < ITERS:
            apply(j)
            turn(j)
            if j == 2:
                lifted[j] = powers[2] - 2.0 * powers[1] + size * powers[0]
            else:
                lifted[j] = powers[j] + shifting[...]
            weighted = weights[...] * lifted[j]
            earlier = [powers[0], powers[1]] if j == 2 else [vecs[k] for k in range(j - 1)] + [lifted[j - 1]]
            image = lifted[j]
        else:
            image = turned[j]
            weighted = turned_weights[...] * image
            earlier = [turned_vecs[k] for k in range(j - 1)] + [turned_lifted[...]]
        gather_start(j, [(v, weighted) for v in earlier + [image]])
        if j == ITERS:
            lifted[j] = swap(image)
        for k in [j - 1] if j < ITERS else [j - 1, j]:
            if k == 1:
                square, *rest = gather_end(1, 3)
                triangle.append([jnp.sqrt(square)])
                start_size = triangle[0][0]
                settle(0, powers[0], triangle[0])
                triangle.append(heights(rest, triangle))
                settle(1, powers[1], triangle[1])
                alphas.append(triangle[1][0] / start_size)
                betas.append(triangle[1][1] / start_size)
                images[0] = powers[1] * (1.0 / (start_size * size))
            else:
                products = gather_end(k, k + 1)
                scale = size
                if k == 2:
                    products[0] = products[0] / start_size
                    scale = size / start_size
                triangle.append(heights(products, triangle))
                settle(k, lifted[k], triangle[k])
                scale = scale / betas[k - 2]
                alphas.append(2.0 * shifts[k] - alphas[k - 2] + triangle[k][k - 1] * scale)
                betas.append(triangle[k][k] * scale)
        if j == ITERS:
            break
        image = powers[j] * (1.0 / start_size) if j == 2 else powers[j] - betas[j - 3] * images[j - 3]
        image = (image - alphas[j - 2] * images[j - 2]) * (1.0 / betas[j - 2])
        images[j - 1] = image
        shift = shifts[j + 1] = alphas[j - 2]
        change = (shift * shift / size) * vecs[j - 1] - (2.0 * shift) * image
        if j + 1 < ITERS:
            shifting[...] = change
        else:
            shifting[...] = swap(change)
            turned_lifted[...] = swap(lifted[j])
        exchange_end((j + 1) % 2)
        side = powers if j % 2 else turned
        new = out[...] - alphas[j - 2] * side[j]
        lead = betas[j - 2]
        if j == 2:
            lead = lead * start_size
        else:
            behind = betas[j - 3]
            if j == 3:
                behind = behind / start_size
            new = new - behind * side[j - 1]
        new = new * (1.0 / lead)
        if j + 1 == ITERS:
            new = new + shifting[...]
        side[j + 1] = new

    s, l = iota((8, 128), 0), iota((8, 128), 1)
    tile = jnp.zeros((8, 128), F32)
    for j in range(ITERS):
        tile = jnp.where((s == 0) & (l == j), alphas[j], jnp.where((s == 1) & (l == j), betas[j], tile))
    small[...] = tile[0:2, 0:ITERS]
    last = pltpu.make_async_copy(small, coefficients_ref, out_sem.at[ITERS])
    last.start()
    for i in range(1, ITERS + 1):
        leaving(i).wait()
    last.wait()


def message_counts(x, y, z):
    return x + y + z + y * z, x * (y + z + y * z)


def hand_over(basis_in, coefficients_in, basis_out, coefficients_out, wides, small, in_sem, out_sem):
    pairs = [(basis_in.at[i], wides.at[i], basis_out.at[i]) for i in range(ITERS)]
    pairs.append((coefficients_in, small, coefficients_out))
    come = [pltpu.make_async_copy(a, b, in_sem.at[i]) for i, (a, b, _) in enumerate(pairs)]
    go = [pltpu.make_async_copy(b, c, out_sem.at[i]) for i, (_, b, c) in enumerate(pairs)]
    for copy in come:
        copy.start()
    for first, then in zip(come, go):
        first.wait()
        then.start()
    for copy in go:
        copy.wait()


def shards(sizes, start, stencils):
    nx, ny, nz = sizes
    hbm = pl.BlockSpec(memory_space=pltpu.HBM)
    anyw = pl.BlockSpec(memory_space=pl.ANY)
    basis, coefficients = pl.pallas_call(
        functools.partial(kernel, sizes),
        out_shape=(
            jax.ShapeDtypeStruct((ITERS, C, C * C), F32),
            jax.ShapeDtypeStruct((2, ITERS), F32),
        ),
        in_specs=[hbm, hbm],
        out_specs=(anyw, anyw),
        scratch_shapes=[
            pltpu.VMEM((C, C * C), F32),
            pltpu.VMEM((6, C, C), F32),
            pltpu.VMEM((ITERS, C, C * C), F32),
            pltpu.VMEM((2, ITERS), F32),
            pltpu.VMEM((256, 128), F32),
            pltpu.VMEM((ITERS + 1, 256, 128), F32),
            pltpu.VMEM((ITERS + 1, 256, 128), F32),
            pltpu.VMEM((ITERS, 256, 128), F32),
            pltpu.VMEM((ITERS - 1, 256, 128), F32),
            pltpu.VMEM((256, 128), F32),
            pltpu.VMEM((ITERS + 1, 256, 128), F32),
            pltpu.VMEM((256, 128), F32),
            pltpu.VMEM((ITERS - 1, 256, 128), F32),
            pltpu.VMEM((256, 128), F32),
            pltpu.VMEM((256, 128), F32),
            pltpu.VMEM((2, 2 * C, 6 * C), BF16),
            pltpu.VMEM((2, 2 * C, 12 * C), BF16),
            pltpu.VMEM((256, 384), BF16),
            pltpu.VMEM((2, len(TILES), 8, 128), F32),
            pltpu.VMEM((2, len(ROWS), 128), F32),
            pltpu.VMEM((2, len(TILES), 8, 128), F32),
            pltpu.VMEM((2, len(ROWS), 128), F32),
            pltpu.VMEM((ITERS + 1, nx * ny * nz, 128), F32),
            pltpu.VMEM((2, max(nx * ny, nz), 128), F32),
        ]
        + [pltpu.SemaphoreType.DMA((2, 2))] * 2
        + [pltpu.SemaphoreType.DMA((ITERS + 1,))] * 2
        + [pltpu.SemaphoreType.DMA((2,))] * 2
        + [pltpu.SemaphoreType.DMA((2,)), pltpu.SemaphoreType.DMA((ITERS + 1,))],
        compiler_params=pltpu.CompilerParams(collective_id=0, has_side_effects=True),
    )(start.reshape(C, C * C), stencils.reshape(6, C, C))
    basis, coefficients = pl.pallas_call(
        hand_over,
        out_shape=(
            jax.ShapeDtypeStruct((ITERS, C, C * C), F32),
            jax.ShapeDtypeStruct((2, ITERS), F32),
        ),
        in_specs=[anyw, anyw],
        out_specs=(anyw, anyw),
        scratch_shapes=[
            pltpu.VMEM((ITERS, C, C * C), F32),
            pltpu.VMEM((2, ITERS), F32),
            pltpu.SemaphoreType.DMA((ITERS + 1,)),
            pltpu.SemaphoreType.DMA((ITERS + 1,)),
        ],
    )(basis, coefficients)
    return (
        basis.reshape(1, 1, 1, 1, ITERS, C, C * C),
        coefficients.reshape(1, 2, ITERS),
    )


def solution(mesh):
    sizes = tuple(mesh.shape[a] for a in AXES)
    return jax.shard_map(
        functools.partial(shards, sizes),
        mesh=mesh,
        in_specs=(P("gx", "gy", "gz", None, None, None), P(None, "gx", "gy", "gz", None, None)),
        out_specs=(P("gx", "gy", "gz", None, None, None, None), P()),
        check_vma=False,
    )
```

```python
import functools
import itertools

import jax
import jax.numpy as jnp
from jax import lax
from jax.experimental import pallas as pl
from jax.experimental.pallas import tpu as pltpu
from jax.sharding import PartitionSpec as P

ITERS = 5
C = 32
MESH = pl.DeviceIdType.MESH
F32 = jnp.float32
BF16 = jnp.bfloat16
AXES = ("gx", "gy", "gz")
DIRS = [
    (dx, dy, dz)
    for dx in (-1, 0, 1)
    for dy in (-1, 0, 1)
    for dz in (-1, 0, 1)
    if (dx, dy, dz) != (0, 0, 0)
]
TILES = [d for d in DIRS if d[0] == 0 or d[1:] == (0, 0)]
ROWS = [d for d in DIRS if d not in TILES]
SLOT = {d: i for dirs in (TILES, ROWS) for i, d in enumerate(dirs)}
SHRINK = 2.0**-17


def iota(shape, dim):
    return lax.broadcasted_iota(jnp.int32, shape, dim)


def roll(x, shift, axis):
    size = x.shape[axis]
    shift = shift % size
    return x if shift == 0 else pltpu.roll(x, shift, axis)


def swap(field):
    x = field.reshape(32, 8, 128)
    s, l = iota((1, 8, 128), 1), iota((1, 8, 128), 2)
    s1, l1 = (s // 2) % 2, l // 64
    r = roll(x, 64, 2)
    x = jnp.where(s1 == l1, x, jnp.where(s1 == 0, roll(r, -2, 1), roll(r, 2, 1)))
    s0, l0 = s % 2, (l // 32) % 2
    up, down = roll(roll(x, 32, 2), -1, 1), roll(roll(x, -32, 2), 1, 1)
    x = jnp.where(s0 == l0, x, jnp.where(s0 == 0, up, down))
    even = jnp.concatenate([x[t * 4 : t * 4 + 4] for t in range(0, 8, 2)], axis=0)
    odd = jnp.concatenate([x[t * 4 : t * 4 + 4] for t in range(1, 8, 2)], axis=0)
    half = s < 4
    top = jnp.where(half, even, roll(odd, 4, 1))
    bottom = jnp.where(half, roll(even, 4, 1), odd)
    parts = []
    for ai in range(4):
        for part in (top, bottom):
            for k in range(4):
                parts.append(part[k * 4 + ai : k * 4 + ai + 1])
    return jnp.concatenate(parts, axis=0).reshape(256, 128)


def wide(field):
    return jnp.concatenate([field[t * 32 : t * 32 + 32] for t in range(8)], axis=1)


def tall(field):
    return jnp.concatenate([field[:, t * 128 : t * 128 + 128] for t in range(8)], axis=0)


def split(x):
    high = x.astype(BF16)
    rest = x - high.astype(F32)
    middle = rest.astype(BF16)
    return high, middle, (rest - middle.astype(F32)).astype(BF16)


PAIRS = ((0, 0), (0, 1), (1, 0), (1, 1), (0, 2), (2, 0))


def dot(left, right):
    return jnp.dot(left, right, preferred_element_type=F32)


def spread(matrix):
    parts = split(matrix)
    return jnp.concatenate([parts[i] for i, _ in PAIRS], axis=1)


def stack(field):
    parts = split(field)
    return jnp.concatenate([parts[i] for _, i in PAIRS], axis=0)


def matvec(field, first_ref, second_ref, zmat_ref):
    first = dot(first_ref[...], stack(wide(field)))
    mass, stiff = swap(tall(first[:C])), swap(tall(first[C:]))
    second = dot(second_ref[...], stack(jnp.concatenate([wide(stiff), wide(mass)], axis=0)))
    third = jnp.concatenate([tall(second[:C]), tall(second[C:])], axis=1)
    high, middle, low = split(third)
    pair = zmat_ref[:, 0:256]
    both = dot(high, pair) + dot(middle, pair)
    rest = dot(low, zmat_ref[:, 0:128]) + dot(high, zmat_ref[:, 256:384])
    return both[:, :128] + (both[:, 128:] + rest)


def block_diagonal(matrix):
    zero = jnp.zeros((C, C), F32)
    rows = []
    for i in range(4):
        rows.append(jnp.concatenate([matrix if k == i else zero for k in range(4)], axis=1))
    return jnp.concatenate(rows, axis=0)


def weight_field(sizes, here):
    row, lane = iota((256, 128), 0), iota((256, 128), 1)
    places = (row % C, (row // C) * 4 + lane // C, lane % C)
    weight = jnp.ones((256, 128), F32)
    for place, size, at in zip(places, sizes, here):
        low = jnp.where(at > 0, 0.5, 1.0).astype(F32)
        high = jnp.where(at < size - 1, 0.5, 1.0).astype(F32)
        weight = weight * jnp.where(place == 0, low, jnp.where(place == C - 1, high, 1.0))
    return weight


def neighbour(sizes, here, step):
    fine = None
    for size, at, d in zip(sizes, here, step):
        if d != 0:
            inside = at > 0 if d < 0 else at < size - 1
            fine = inside if fine is None else jnp.logical_and(fine, inside)
    return fine, tuple(at + d for at, d in zip(here, step))


def pack(out_ref, tile_ref, row_ref):
    s, l = iota((8, 128), 0), iota((8, 128), 1)
    line = iota((1, 128), 1)
    lower = lambda t, ai: out_ref[pl.ds(t * 32 + ai * 8, 8), :]
    zero = jnp.zeros((8, 128), F32)
    low, high = zero, zero
    for t in range(8):
        for ai in range(4):
            r = ai * 8 + t
            moved = roll(lower(t, ai), r, 1)
            low = jnp.where(l % C == r, moved, low)
            high = jnp.where(l % C == (r + C - 1) % C, moved, high)

    def send_row(d, plane, source, keep):
        row_ref[pl.ds(SLOT[d], 1), :] = jnp.where(keep, plane[source : source + 1], 0.0)

    for dx in (-1, 1):
        source = 0 if dx < 0 else 7
        for dz, plane, base in ((-1, low, 0), (1, high, -31)):
            for dy in (-1, 0, 1):
                keep = (line % C) // 8 == (3 if dx < 0 else 0)
                if dy != 0:
                    keep = keep & (line // C == (3 if dy < 0 else 0)) & (line % 8 == (7 if dy < 0 else 0))
                send_row((dx, dy, dz), roll(plane, base - dx * 24 - dy * 103, 1), source, keep)
        plane = out_ref[pl.ds(0 if dx < 0 else C - 1, 8, stride=C), :]
        tile_ref[SLOT[(dx, 0, 0)]] = plane
        for dy in (-1, 1):
            keep = line // C == (3 if dy < 0 else 0)
            send_row((dx, dy, 0), roll(plane, 96 if dy < 0 else 32, 1), 0 if dy < 0 else 7, keep)
    for dz, plane, base in ((-1, low, 0), (1, high, -31)):
        tile_ref[SLOT[(0, 0, dz)]] = roll(plane, base, 1)
        for dy in (-1, 1):
            keep = (l // C == (3 if dy < 0 else 0)) & (l % 8 == (7 if dy < 0 else 0))
            tile_ref[SLOT[(0, dy, dz)]] = jnp.where(keep, roll(plane, base - dy * 103, 1), 0.0)
    for dy in (-1, 1):
        plane = zero
        for ai in range(4):
            piece = roll(lower(0 if dy < 0 else 7, ai), C * (ai + (0 if dy < 0 else 1)), 1)
            plane = jnp.where(l // C == ai, piece, plane)
        tile_ref[SLOT[(0, dy, 0)]] = plane


def unpack(out_ref, tile_ref, row_ref):
    s, l = iota((8, 128), 0), iota((8, 128), 1)
    near = (-1, 0, 1)
    got = lambda *d: tile_ref[SLOT[d]]
    row = lambda *d: row_ref[pl.ds(SLOT[d], 1), :]
    ends = lambda last, first: jnp.where(s == 7, last, jnp.where(s == 0, first, 0.0))
    for dx in (-1, 1):
        plane = got(dx, 0, 0) + ends(row(dx, -1, 0), row(dx, 1, 0))
        rows = pl.ds(C - 1 if dx < 0 else 0, 8, stride=C)
        out_ref[rows, :] = out_ref[rows, :] + plane
    low, high = (
        sum(got(0, dy, dz) for dy in near)
        + ends(sum(row(-1, dy, dz) for dy in near), sum(row(1, dy, dz) for dy in near))
        for dz in (1, -1)
    )
    first, last = got(0, 1, 0), got(0, -1, 0)
    for t in range(8):
        for ai in range(4):
            r = ai * 8 + t
            rows = pl.ds(t * 32 + ai * 8, 8)
            add = jnp.where(l % C == 0, roll(low, -r, 1), 0.0)
            add = add + jnp.where(l % C == C - 1, roll(high, 31 - r, 1), 0.0)
            if t == 0:
                add = add + jnp.where(l < C, roll(first, -C * ai, 1), 0.0)
            if t == 7:
                add = add + jnp.where(l >= 96, roll(last, 96 - C * ai, 1), 0.0)
            out_ref[rows, :] = out_ref[rows, :] + add


def kernel(
    sizes,
    start_hbm,
    stencils_hbm,
    basis_ref,
    coefficients_ref,
    start_ref,
    stencils_ref,
    wides,
    small,
    out,
    powers,
    turned,
    vecs,
    turned_vecs,
    turned_weights,
    lifted,
    turned_lifted,
    images,
    shifting,
    weights,
    first,
    second,
    zmat,
    tiles,
    rows,
    got_tiles,
    got_rows,
    terms,
    marks,
    send_sem,
    got_sem,
    term_send,
    term_got,
    mark_send,
    mark_got,
    in_sem,
    out_sem,
):
    here = tuple(lax.axis_index(a) for a in AXES)
    nx, ny, nz = sizes
    gx, gy, gz = here
    me = (gx * ny + gy) * nz + gz
    hops = lambda k, size: min(k, size - k)
    steps = sorted(
        ((i, j, k) for i in range(nx) for j in range(ny) for k in range(nz)),
        key=lambda d: -(hops(d[0], nx) + hops(d[1], ny) + hops(d[2], nz) / 2),
    )
    along = [[lax.rem(at + k, size) for k in range(size)] for at, size in zip(here, sizes)]
    everyone = [tuple(along[a][d[a]] for a in range(3)) for d in steps if any(d)]
    beside = [
        jnp.where(at > 0, 1, 0) + jnp.where(at < size - 1, 1, 0) for at, size in zip(here, sizes)
    ]

    inputs = [
        pltpu.make_async_copy(start_hbm, start_ref, in_sem.at[0]),
        pltpu.make_async_copy(stencils_hbm, stencils_ref, in_sem.at[1]),
    ]
    for copy in inputs:
        copy.start()
    got_tiles[...] = jnp.zeros_like(got_tiles)
    got_rows[...] = jnp.zeros_like(got_rows)
    barrier = pltpu.get_barrier_semaphore()
    line = [(gx, gy, lax.rem(gz + k, nz)) for k in range(1, nz)]
    plane = [
        (along[0][i], along[1][k], gz) for i in range(nx) for k in range(ny) if (i, k) != (0, 0)
    ]
    for there in plane + line:
        pl.semaphore_signal(barrier, inc=1, device_id=there, device_id_type=MESH)
    for d in DIRS:
        if d[2] != 0 and d[:2] != (0, 0):
            fine, there = neighbour(sizes, here, d)

            @pl.when(fine)
            def _():
                pl.semaphore_signal(barrier, inc=1, device_id=there, device_id_type=MESH)

    greetings = len(plane) + len(line) + beside[2] * ((1 + beside[0]) * (1 + beside[1]) - 1)

    weights[...] = weight_field(sizes, here)
    for copy in inputs:
        copy.wait()
    kx, ky, kz, mx, my, mz = (stencils_ref[i] for i in range(6))
    empty = jnp.zeros((C, C), F32)
    for i, (mass, stiff) in enumerate(((mx, kx), (my, ky))):
        first[i] = spread(jnp.concatenate([mass, stiff], axis=0))
        upper, lower = (jnp.concatenate(p, axis=1) for p in ((mass, stiff), (empty, mass)))
        second[1 - i] = spread(jnp.concatenate([upper, lower], axis=0))
    zmat[...] = jnp.concatenate(
        split(jnp.concatenate([block_diagonal(mz.T), block_diagonal(kz.T)], axis=0)), axis=1
    )

    def exchange_start(par):
        pack(out, tiles.at[par], rows.at[par])
        for d in sorted(DIRS, key=lambda d: -(2 * abs(d[0]) + 2 * abs(d[1]) + abs(d[2]))):
            fine, there = neighbour(sizes, here, (d[1], d[0], d[2]) if par else d)
            if d in TILES:
                source, target = tiles.at[par, SLOT[d]], got_tiles.at[par, SLOT[d]]
            else:
                source, target = rows.at[par, pl.ds(SLOT[d], 1)], got_rows.at[par, pl.ds(SLOT[d], 1)]

            @pl.when(fine)
            def _():
                pltpu.make_async_remote_copy(
                    src_ref=source,
                    dst_ref=target,
                    send_sem=send_sem.at[par, int(d in ROWS)],
                    recv_sem=got_sem.at[par, int(d in ROWS)],
                    device_id=there,
                    device_id_type=MESH,
                ).start()

    def exchange_end(par):
        order = (1, 0, 2) if par else (0, 1, 2)
        counts = message_counts(*(beside[i] for i in order))
        choices = [{0} if n == 1 else {1} if n == 2 else {1, 2} for n in (sizes[i] for i in order)]
        for n, m in sorted({message_counts(*c) for c in itertools.product(*choices)}):

            @pl.when((counts[0] == n) & (counts[1] == m))
            def _():
                for kind, (count, sent, got) in enumerate(((n, tiles, got_tiles), (m, rows, got_rows))):
                    if count:
                        both = pltpu.make_async_remote_copy(
                            src_ref=sent.at[par, pl.ds(0, count)],
                            dst_ref=got.at[par, pl.ds(0, count)],
                            send_sem=send_sem.at[par, kind],
                            recv_sem=got_sem.at[par, kind],
                            device_id=everyone[0],
                            device_id_type=MESH,
                        )
                        both.wait_recv()
                        both.wait_send()

        unpack(out, got_tiles.at[par], got_rows.at[par])

    def gather_start(k, pairs):
        s, l = iota((8, 128), 0), iota((8, 128), 1)
        tile = jnp.zeros((8, 128), F32)
        for i, (left, right) in enumerate(pairs):
            lanes = jnp.sum(jnp.sum((left * right).reshape(32, 8, 128), axis=0), axis=0, keepdims=True)
            tile = jnp.where(s == i, lanes, tile)
        column = jnp.sum(tile, axis=1, keepdims=True)
        gather_row(k, jnp.sum(jnp.where(s == l, column, 0.0), axis=0, keepdims=True))

    def gather_row(k, row):
        mine = pl.ds(me, 1)
        terms[k, mine] = row
        for there in everyone:
            pltpu.make_async_remote_copy(
                src_ref=terms.at[k, mine],
                dst_ref=terms.at[k, mine],
                send_sem=term_send.at[k],
                recv_sem=term_got.at[k],
                device_id=there,
                device_id_type=MESH,
            ).start()

    def mark_start(k, at, peers, row):
        marks[k, pl.ds(at, 1)] = row
        for there in peers:
            pltpu.make_async_remote_copy(
                src_ref=marks.at[k, pl.ds(at, 1)],
                dst_ref=marks.at[k, pl.ds(at, 1)],
                send_sem=mark_send.at[k],
                recv_sem=mark_got.at[k],
                device_id=there,
                device_id_type=MESH,
            ).start()

    def mark_end(k, peers):
        if peers:
            both = pltpu.make_async_remote_copy(
                src_ref=marks.at[k, pl.ds(0, len(peers))],
                dst_ref=marks.at[k, pl.ds(0, len(peers))],
                send_sem=mark_send.at[k],
                recv_sem=mark_got.at[k],
                device_id=peers[0],
                device_id_type=MESH,
            )
            both.wait_recv()
            both.wait_send()
        return jnp.sum(marks[k, 0 : len(peers) + 1], axis=0, keepdims=True)

    def gather_end(k, count):
        others = pl.ds(0, len(everyone))
        both = pltpu.make_async_remote_copy(
            src_ref=terms.at[k, others],
            dst_ref=terms.at[k, others],
            send_sem=term_send.at[k],
            recv_sem=term_got.at[k],
            device_id=everyone[0],
            device_id_type=MESH,
        )
        both.wait_recv()
        both.wait_send()
        row = jnp.sum(terms[k], axis=0, keepdims=True)
        s, l = iota((8, 128), 0), iota((8, 128), 1)
        column = jnp.sum(jnp.where(s == l, row, 0.0), axis=1, keepdims=True)
        return [column[i : i + 1] for i in range(count)]

    def leaving(i):
        return pltpu.make_async_copy(wides.at[i - 1], basis_ref.at[i - 1], out_sem.at[i - 1])

    def settle(i, image, height):
        new = image
        for k in range(i):
            new = new - height[k] * vecs[k]
        new = new * height[i + 1]
        if i < ITERS:
            vecs[i] = new
        if i < ITERS - 1:
            turned_vecs[i] = swap(new)
        if i > 0:
            wides[i - 1] = wide(new)
            leaving(i).start()

    def heights(products, known):
        *with_known, with_last, square = products
        i = len(known)
        found = list(with_known)
        last = with_last
        for k in range(i - 1):
            last = last - known[i - 1][k] * found[k]
        found.append(last * known[i - 1][i])
        for value in found:
            square = square - value * value
        over = lax.rsqrt(square)
        found += [square * over, over]
        return found

    out[...] = tall(start_ref[...]) * weights[...] * SHRINK
    pl.semaphore_wait(barrier, greetings)
    exchange_start(0)
    trace = [jnp.sum(jnp.where(iota((C, C), 0) == iota((C, C), 1), m, 0.0), keepdims=True) / C for m in (kx, ky, kz, mx, my, mz)]
    mean = trace[0] * trace[4] * trace[5] + trace[3] * trace[1] * trace[5] + trace[3] * trace[4] * trace[2]
    mark_start(0, gz, line, jnp.broadcast_to(mean / (nx * ny * nz), (1, 128)))
    exchange_end(0)
    powers[0] = out[...]
    mark_start(1, gx * ny + gy, plane, mark_end(0, line))

    def apply(j):
        here = (turned if j % 2 else powers)[j]
        out[...] = matvec(here, first.at[j % 2], second.at[j % 2], zmat)
        exchange_start((j + 1) % 2)

    def turn(j):
        if j % 2:
            powers[j] = swap(turned[j])
        else:
            turned[j] = swap(powers[j])

    apply(0)
    exchange_end(1)
    turned[1] = out[...]

    apply(1)
    turn(1)
    size = mark_end(1, plane)
    over_size = 1.0 / size
    weighted = weights[...] * powers[1]
    gather_start(1, [(powers[0], weights[...] * powers[0]), (powers[0], weighted), (powers[1], weighted)])
    turned_weights[...] = swap(weights[...])
    exchange_end(0)
    powers[2] = out[...] * over_size

    triangle, alphas, betas, over_betas = [], [], [], []
    shifts = {2: size}
    for j in range(2, ITERS + 1):
        if j < ITERS:
            apply(j)
            if j % 2:
                turn(j)
            if j == 2:
                lifted[j] = powers[2] - 2.0 * powers[1] + size * powers[0]
            else:
                lifted[j] = powers[j] + shifting[...]
            weighted = weights[...] * lifted[j]
            earlier = [powers[0], powers[1]] if j == 2 else [vecs[k] for k in range(j - 1)] + [lifted[j - 1]]
            image = lifted[j]
        else:
            image = turned[j]
            weighted = turned_weights[...] * image
            earlier = [turned_vecs[k] for k in range(j - 1)] + [turned_lifted[...]]
        gather_start(j, [(v, weighted) for v in earlier + [image]])
        if j == ITERS:
            lifted[j] = swap(image)
        elif j % 2 == 0:
            turn(j)
        for k in [j - 1] if j < ITERS else [j - 1, j]:
            if k == 1:
                square, *rest = gather_end(1, 3)
                triangle.append([jnp.sqrt(square), lax.rsqrt(square)])
                start_size, over_start = triangle[0]
                settle(0, powers[0], triangle[0])
                triangle.append(heights(rest, triangle))
                settle(1, powers[1], triangle[1])
                alphas.append(triangle[1][0] * over_start)
                betas.append(triangle[1][1] * over_start)
                over_betas.append(triangle[1][2] * start_size)
                images[0] = powers[1] * (over_start * over_size)
            else:
                products = gather_end(k, k + 1)
                scale, over_scale = size, over_size
                if k == 2:
                    products[0] = products[0] * over_start
                    scale, over_scale = size * over_start, over_size * start_size
                triangle.append(heights(products, triangle))
                settle(k, lifted[k], triangle[k])
                scale = scale * over_betas[k - 2]
                alphas.append(2.0 * shifts[k] - alphas[k - 2] + triangle[k][k - 1] * scale)
                betas.append(triangle[k][k] * scale)
                over_betas.append(triangle[k][k + 1] * (over_scale * betas[k - 2]))
        if j == ITERS:
            break
        image = powers[j] * over_start if j == 2 else powers[j] - betas[j - 3] * images[j - 3]
        image = (image - alphas[j - 2] * images[j - 2]) * over_betas[j - 2]
        images[j - 1] = image
        shift = shifts[j + 1] = alphas[j - 2]
        change = (shift * shift * over_size) * vecs[j - 1] - (2.0 * shift) * image
        if j + 1 < ITERS:
            shifting[...] = change
        else:
            shifting[...] = swap(change)
            turned_lifted[...] = swap(lifted[j])
        exchange_end((j + 1) % 2)
        side = powers if j % 2 else turned
        new = out[...] - alphas[j - 2] * side[j]
        over_lead = over_betas[j - 2]
        if j == 2:
            over_lead = over_lead * over_start
        else:
            behind = betas[j - 3]
            if j == 3:
                behind = behind * over_start
            new = new - behind * side[j - 1]
        new = new * over_lead
        if j + 1 == ITERS:
            new = new + shifting[...]
        side[j + 1] = new

    s, l = iota((8, 128), 0), iota((8, 128), 1)
    tile = jnp.zeros((8, 128), F32)
    for j in range(ITERS):
        tile = jnp.where((s == 0) & (l == j), alphas[j], jnp.where((s == 1) & (l == j), betas[j], tile))
    small[...] = tile[0:2, 0:ITERS]
    last = pltpu.make_async_copy(small, coefficients_ref, out_sem.at[ITERS])
    last.start()
    for i in range(1, ITERS + 1):
        leaving(i).wait()
    last.wait()


def message_counts(x, y, z):
    return x + y + z + y * z, x * (y + z + y * z)


def hand_over(basis_in, coefficients_in, basis_out, coefficients_out, wides, small, in_sem, out_sem):
    pairs = [(basis_in.at[i], wides.at[i], basis_out.at[i]) for i in range(ITERS)]
    pairs.append((coefficients_in, small, coefficients_out))
    come = [pltpu.make_async_copy(a, b, in_sem.at[i]) for i, (a, b, _) in enumerate(pairs)]
    go = [pltpu.make_async_copy(b, c, out_sem.at[i]) for i, (_, b, c) in enumerate(pairs)]
    for copy in come:
        copy.start()
    for first, then in zip(come, go):
        first.wait()
        then.start()
    for copy in go:
        copy.wait()


def shards(sizes, start, stencils):
    nx, ny, nz = sizes
    hbm = pl.BlockSpec(memory_space=pltpu.HBM)
    anyw = pl.BlockSpec(memory_space=pl.ANY)
    basis, coefficients = pl.pallas_call(
        functools.partial(kernel, sizes),
        out_shape=(
            jax.ShapeDtypeStruct((ITERS, C, C * C), F32),
            jax.ShapeDtypeStruct((2, ITERS), F32),
        ),
        in_specs=[hbm, hbm],
        out_specs=(anyw, anyw),
        scratch_shapes=[
            pltpu.VMEM((C, C * C), F32),
            pltpu.VMEM((6, C, C), F32),
            pltpu.VMEM((ITERS, C, C * C), F32),
            pltpu.VMEM((2, ITERS), F32),
            pltpu.VMEM((256, 128), F32),
            pltpu.VMEM((ITERS + 1, 256, 128), F32),
            pltpu.VMEM((ITERS + 1, 256, 128), F32),
            pltpu.VMEM((ITERS, 256, 128), F32),
            pltpu.VMEM((ITERS - 1, 256, 128), F32),
            pltpu.VMEM((256, 128), F32),
            pltpu.VMEM((ITERS + 1, 256, 128), F32),
            pltpu.VMEM((256, 128), F32),
            pltpu.VMEM((ITERS - 1, 256, 128), F32),
            pltpu.VMEM((256, 128), F32),
            pltpu.VMEM((256, 128), F32),
            pltpu.VMEM((2, 2 * C, 6 * C), BF16),
            pltpu.VMEM((2, 2 * C, 12 * C), BF16),
            pltpu.VMEM((256, 384), BF16),
            pltpu.VMEM((2, len(TILES), 8, 128), F32),
            pltpu.VMEM((2, len(ROWS), 128), F32),
            pltpu.VMEM((2, len(TILES), 8, 128), F32),
            pltpu.VMEM((2, len(ROWS), 128), F32),
            pltpu.VMEM((ITERS + 1, nx * ny * nz, 128), F32),
            pltpu.VMEM((2, max(nx * ny, nz), 128), F32),
        ]
        + [pltpu.SemaphoreType.DMA((2, 2))] * 2
        + [pltpu.SemaphoreType.DMA((ITERS + 1,))] * 2
        + [pltpu.SemaphoreType.DMA((2,))] * 2
        + [pltpu.SemaphoreType.DMA((2,)), pltpu.SemaphoreType.DMA((ITERS + 1,))],
        compiler_params=pltpu.CompilerParams(collective_id=0, has_side_effects=True),
    )(start.reshape(C, C * C), stencils.reshape(6, C, C))
    basis, coefficients = pl.pallas_call(
        hand_over,
        out_shape=(
            jax.ShapeDtypeStruct((ITERS, C, C * C), F32),
            jax.ShapeDtypeStruct((2, ITERS), F32),
        ),
        in_specs=[anyw, anyw],
        out_specs=(anyw, anyw),
        scratch_shapes=[
            pltpu.VMEM((ITERS, C, C * C), F32),
            pltpu.VMEM((2, ITERS), F32),
            pltpu.SemaphoreType.DMA((ITERS + 1,)),
            pltpu.SemaphoreType.DMA((ITERS + 1,)),
        ],
    )(basis, coefficients)
    return (
        basis.reshape(1, 1, 1, 1, ITERS, C, C * C),
        coefficients.reshape(1, 2, ITERS),
    )


def solution(mesh):
    sizes = tuple(mesh.shape[a] for a in AXES)
    return jax.shard_map(
        functools.partial(shards, sizes),
        mesh=mesh,
        in_specs=(P("gx", "gy", "gz", None, None, None), P(None, "gx", "gy", "gz", None, None)),
        out_specs=(P("gx", "gy", "gz", None, None, None, None), P()),
        check_vma=False,
    )
```

```python
import functools
import itertools

import jax
import jax.numpy as jnp
from jax import lax
from jax.experimental import pallas as pl
from jax.experimental.pallas import tpu as pltpu
from jax.sharding import PartitionSpec as P

ITERS = 5
C = 32
MESH = pl.DeviceIdType.MESH
F32 = jnp.float32
BF16 = jnp.bfloat16
AXES = ("gx", "gy", "gz")
DIRS = [
    (dx, dy, dz)
    for dx in (-1, 0, 1)
    for dy in (-1, 0, 1)
    for dz in (-1, 0, 1)
    if (dx, dy, dz) != (0, 0, 0)
]
TILES = [d for d in DIRS if d[0] == 0 or d[1:] == (0, 0)]
ROWS = [d for d in DIRS if d not in TILES]
SLOT = {d: i for dirs in (TILES, ROWS) for i, d in enumerate(dirs)}
SHRINK = 2.0**-17


def iota(shape, dim):
    return lax.broadcasted_iota(jnp.int32, shape, dim)


def roll(x, shift, axis):
    size = x.shape[axis]
    shift = shift % size
    return x if shift == 0 else pltpu.roll(x, shift, axis)


def swap(field):
    x = field.reshape(32, 8, 128)
    s, l = iota((1, 8, 128), 1), iota((1, 8, 128), 2)
    s1, l1 = (s // 2) % 2, l // 64
    r = roll(x, 64, 2)
    x = jnp.where(s1 == l1, x, jnp.where(s1 == 0, roll(r, -2, 1), roll(r, 2, 1)))
    s0, l0 = s % 2, (l // 32) % 2
    up, down = roll(roll(x, 32, 2), -1, 1), roll(roll(x, -32, 2), 1, 1)
    x = jnp.where(s0 == l0, x, jnp.where(s0 == 0, up, down))
    even = jnp.concatenate([x[t * 4 : t * 4 + 4] for t in range(0, 8, 2)], axis=0)
    odd = jnp.concatenate([x[t * 4 : t * 4 + 4] for t in range(1, 8, 2)], axis=0)
    half = s < 4
    top = jnp.where(half, even, roll(odd, 4, 1))
    bottom = jnp.where(half, roll(even, 4, 1), odd)
    parts = []
    for ai in range(4):
        for part in (top, bottom):
            for k in range(4):
                parts.append(part[k * 4 + ai : k * 4 + ai + 1])
    return jnp.concatenate(parts, axis=0).reshape(256, 128)


def wide(field):
    return jnp.concatenate([field[t * 32 : t * 32 + 32] for t in range(8)], axis=1)


def tall(field):
    return jnp.concatenate([field[:, t * 128 : t * 128 + 128] for t in range(8)], axis=0)


def split(x):
    high = x.astype(BF16)
    rest = x - high.astype(F32)
    middle = rest.astype(BF16)
    return high, middle, (rest - middle.astype(F32)).astype(BF16)


PAIRS = ((0, 0), (0, 1), (1, 0), (1, 1), (0, 2), (2, 0))


def dot(left, right):
    return jnp.dot(left, right, preferred_element_type=F32)


def spread(matrix):
    parts = split(matrix)
    return jnp.concatenate([parts[i] for i, _ in PAIRS], axis=1)


def stack(field):
    parts = split(field)
    return jnp.concatenate([parts[i] for _, i in PAIRS], axis=0)


def matvec(field, first_ref, second_ref, zmat_ref):
    first = dot(first_ref[...], stack(wide(field)))
    mass, stiff = swap(tall(first[:C])), swap(tall(first[C:]))
    second = dot(second_ref[...], stack(jnp.concatenate([wide(stiff), wide(mass)], axis=0)))
    third = jnp.concatenate([tall(second[:C]), tall(second[C:])], axis=1)
    high, middle, low = split(third)
    pair = zmat_ref[:, 0:256]
    both = dot(high, pair) + dot(middle, pair)
    rest = dot(low, zmat_ref[:, 0:128]) + dot(high, zmat_ref[:, 256:384])
    return both[:, :128] + (both[:, 128:] + rest)


def block_diagonal(matrix):
    zero = jnp.zeros((C, C), F32)
    rows = []
    for i in range(4):
        rows.append(jnp.concatenate([matrix if k == i else zero for k in range(4)], axis=1))
    return jnp.concatenate(rows, axis=0)


def weight_field(sizes, here):
    row, lane = iota((256, 128), 0), iota((256, 128), 1)
    places = (row % C, (row // C) * 4 + lane // C, lane % C)
    weight = jnp.ones((256, 128), F32)
    for place, size, at in zip(places, sizes, here):
        low = jnp.where(at > 0, 0.5, 1.0).astype(F32)
        high = jnp.where(at < size - 1, 0.5, 1.0).astype(F32)
        weight = weight * jnp.where(place == 0, low, jnp.where(place == C - 1, high, 1.0))
    return weight


def neighbour(sizes, here, step):
    fine = None
    for size, at, d in zip(sizes, here, step):
        if d != 0:
            inside = at > 0 if d < 0 else at < size - 1
            fine = inside if fine is None else jnp.logical_and(fine, inside)
    return fine, tuple(lax.rem(at + d + size, size) if d else at for size, at, d in zip(sizes, here, step))


def pack(out_ref, tile_ref, row_ref):
    s, l = iota((8, 128), 0), iota((8, 128), 1)
    line = iota((1, 128), 1)
    lower = lambda t, ai: out_ref[pl.ds(t * 32 + ai * 8, 8), :]
    zero = jnp.zeros((8, 128), F32)
    low, high = zero, zero
    for t in range(8):
        for ai in range(4):
            r = ai * 8 + t
            moved = roll(lower(t, ai), r, 1)
            low = jnp.where(l % C == r, moved, low)
            high = jnp.where(l % C == (r + C - 1) % C, moved, high)

    def send_row(d, plane, source, keep):
        row_ref[pl.ds(SLOT[d], 1), :] = jnp.where(keep, plane[source : source + 1], 0.0)

    for dx in (-1, 1):
        source = 0 if dx < 0 else 7
        for dz, plane, base in ((-1, low, 0), (1, high, -31)):
            for dy in (-1, 0, 1):
                keep = (line % C) // 8 == (3 if dx < 0 else 0)
                if dy != 0:
                    keep = keep & (line // C == (3 if dy < 0 else 0)) & (line % 8 == (7 if dy < 0 else 0))
                send_row((dx, dy, dz), roll(plane, base - dx * 24 - dy * 103, 1), source, keep)
        plane = out_ref[pl.ds(0 if dx < 0 else C - 1, 8, stride=C), :]
        tile_ref[SLOT[(dx, 0, 0)]] = plane
        for dy in (-1, 1):
            keep = line // C == (3 if dy < 0 else 0)
            send_row((dx, dy, 0), roll(plane, 96 if dy < 0 else 32, 1), 0 if dy < 0 else 7, keep)
    for dz, plane, base in ((-1, low, 0), (1, high, -31)):
        tile_ref[SLOT[(0, 0, dz)]] = roll(plane, base, 1)
        for dy in (-1, 1):
            keep = (l // C == (3 if dy < 0 else 0)) & (l % 8 == (7 if dy < 0 else 0))
            tile_ref[SLOT[(0, dy, dz)]] = jnp.where(keep, roll(plane, base - dy * 103, 1), 0.0)
    for dy in (-1, 1):
        plane = zero
        for ai in range(4):
            piece = roll(lower(0 if dy < 0 else 7, ai), C * (ai + (0 if dy < 0 else 1)), 1)
            plane = jnp.where(l // C == ai, piece, plane)
        tile_ref[SLOT[(0, dy, 0)]] = plane


def unpack(out_ref, tile_ref, row_ref):
    s, l = iota((8, 128), 0), iota((8, 128), 1)
    near = (-1, 0, 1)
    got = lambda *d: tile_ref[SLOT[d]]
    row = lambda *d: row_ref[pl.ds(SLOT[d], 1), :]
    ends = lambda last, first: jnp.where(s == 7, last, jnp.where(s == 0, first, 0.0))
    for dx in (-1, 1):
        plane = got(dx, 0, 0) + ends(row(dx, -1, 0), row(dx, 1, 0))
        rows = pl.ds(C - 1 if dx < 0 else 0, 8, stride=C)
        out_ref[rows, :] = out_ref[rows, :] + plane
    low, high = (
        sum(got(0, dy, dz) for dy in near)
        + ends(sum(row(-1, dy, dz) for dy in near), sum(row(1, dy, dz) for dy in near))
        for dz in (1, -1)
    )
    first, last = got(0, 1, 0), got(0, -1, 0)
    for t in range(8):
        for ai in range(4):
            r = ai * 8 + t
            rows = pl.ds(t * 32 + ai * 8, 8)
            add = jnp.where(l % C == 0, roll(low, -r, 1), 0.0)
            add = add + jnp.where(l % C == C - 1, roll(high, 31 - r, 1), 0.0)
            if t == 0:
                add = add + jnp.where(l < C, roll(first, -C * ai, 1), 0.0)
            if t == 7:
                add = add + jnp.where(l >= 96, roll(last, 96 - C * ai, 1), 0.0)
            out_ref[rows, :] = out_ref[rows, :] + add


def kernel(
    sizes,
    start_hbm,
    stencils_hbm,
    basis_ref,
    coefficients_ref,
    start_ref,
    stencils_ref,
    wides,
    small,
    out,
    powers,
    turned,
    vecs,
    turned_vecs,
    turned_weights,
    lifted,
    turned_lifted,
    images,
    shifting,
    weights,
    first,
    second,
    zmat,
    tiles,
    rows,
    got_tiles,
    got_rows,
    terms,
    marks,
    send_sem,
    got_sem,
    term_send,
    term_got,
    mark_send,
    mark_got,
    in_sem,
    out_sem,
):
    here = tuple(lax.axis_index(a) for a in AXES)
    nx, ny, nz = sizes
    gx, gy, gz = here
    me = (gx * ny + gy) * nz + gz
    hops = lambda k, size: min(k, size - k)
    steps = sorted(
        ((i, j, k) for i in range(nx) for j in range(ny) for k in range(nz)),
        key=lambda d: -(hops(d[0], nx) + hops(d[1], ny) + hops(d[2], nz) / 2),
    )
    along = [[lax.rem(at + k, size) for k in range(size)] for at, size in zip(here, sizes)]
    everyone = [tuple(along[a][d[a]] for a in range(3)) for d in steps if any(d)]
    beside = [
        jnp.where(at > 0, 1, 0) + jnp.where(at < size - 1, 1, 0) for at, size in zip(here, sizes)
    ]

    inputs = [
        pltpu.make_async_copy(start_hbm, start_ref, in_sem.at[0]),
        pltpu.make_async_copy(stencils_hbm, stencils_ref, in_sem.at[1]),
    ]
    for copy in inputs:
        copy.start()
    got_tiles[...] = jnp.zeros_like(got_tiles)
    got_rows[...] = jnp.zeros_like(got_rows)
    barrier = pltpu.get_barrier_semaphore()
    line = [(gx, gy, lax.rem(gz + k, nz)) for k in range(1, nz)]
    plane = [
        (along[0][i], along[1][k], gz) for i in range(nx) for k in range(ny) if (i, k) != (0, 0)
    ]
    for there in plane + line:
        pl.semaphore_signal(barrier, inc=1, device_id=there, device_id_type=MESH)
    for d in DIRS:
        if d[2] != 0 and d[:2] != (0, 0):
            fine, there = neighbour(sizes, here, d)

            @pl.when(fine)
            def _():
                pl.semaphore_signal(barrier, inc=1, device_id=there, device_id_type=MESH)

    greetings = len(plane) + len(line) + beside[2] * ((1 + beside[0]) * (1 + beside[1]) - 1)

    weights[...] = weight_field(sizes, here)
    for copy in inputs:
        copy.wait()
    kx, ky, kz, mx, my, mz = (stencils_ref[i] for i in range(6))
    empty = jnp.zeros((C, C), F32)
    for i, (mass, stiff) in enumerate(((mx, kx), (my, ky))):
        first[i] = spread(jnp.concatenate([mass, stiff], axis=0))
        upper, lower = (jnp.concatenate(p, axis=1) for p in ((mass, stiff), (empty, mass)))
        second[1 - i] = spread(jnp.concatenate([upper, lower], axis=0))
    zmat[...] = jnp.concatenate(
        split(jnp.concatenate([block_diagonal(mz.T), block_diagonal(kz.T)], axis=0)), axis=1
    )

    def exchange_start(par):
        pack(out, tiles.at[par], rows.at[par])
        for d in sorted(DIRS, key=lambda d: -(2 * abs(d[0]) + 2 * abs(d[1]) + abs(d[2]))):
            fine, there = neighbour(sizes, here, (d[1], d[0], d[2]) if par else d)
            if d in TILES:
                source, target = tiles.at[par, SLOT[d]], got_tiles.at[par, SLOT[d]]
            else:
                source, target = rows.at[par, pl.ds(SLOT[d], 1)], got_rows.at[par, pl.ds(SLOT[d], 1)]

            @pl.when(fine)
            def _():
                pltpu.make_async_remote_copy(
                    src_ref=source,
                    dst_ref=target,
                    send_sem=send_sem.at[par, int(d in ROWS)],
                    recv_sem=got_sem.at[par, int(d in ROWS)],
                    device_id=there,
                    device_id_type=MESH,
                ).start()

    def exchange_end(par):
        order = (1, 0, 2) if par else (0, 1, 2)
        counts = message_counts(*(beside[i] for i in order))
        choices = [{0} if n == 1 else {1} if n == 2 else {1, 2} for n in (sizes[i] for i in order)]
        for n, m in sorted({message_counts(*c) for c in itertools.product(*choices)}):

            @pl.when((counts[0] == n) & (counts[1] == m))
            def _():
                for kind, (count, sent, got) in enumerate(((n, tiles, got_tiles), (m, rows, got_rows))):
                    if count:
                        both = pltpu.make_async_remote_copy(
                            src_ref=sent.at[par, pl.ds(0, count)],
                            dst_ref=got.at[par, pl.ds(0, count)],
                            send_sem=send_sem.at[par, kind],
                            recv_sem=got_sem.at[par, kind],
                            device_id=everyone[0],
                            device_id_type=MESH,
                        )
                        both.wait_recv()
                        both.wait_send()

        unpack(out, got_tiles.at[par], got_rows.at[par])

    def gather_start(k, pairs):
        s, l = iota((8, 128), 0), iota((8, 128), 1)
        tile = jnp.zeros((8, 128), F32)
        for i, (left, right) in enumerate(pairs):
            lanes = jnp.sum(jnp.sum((left * right).reshape(32, 8, 128), axis=0), axis=0, keepdims=True)
            tile = jnp.where(s == i, lanes, tile)
        column = jnp.sum(tile, axis=1, keepdims=True)
        gather_row(k, jnp.sum(jnp.where(s == l, column, 0.0), axis=0, keepdims=True))

    def gather_row(k, row):
        mine = pl.ds(me, 1)
        terms[k, mine] = row
        for there in everyone:
            pltpu.make_async_remote_copy(
                src_ref=terms.at[k, mine],
                dst_ref=terms.at[k, mine],
                send_sem=term_send.at[k],
                recv_sem=term_got.at[k],
                device_id=there,
                device_id_type=MESH,
            ).start()

    def mark_start(k, at, peers, row):
        marks[k, pl.ds(at, 1)] = row
        for there in peers:
            pltpu.make_async_remote_copy(
                src_ref=marks.at[k, pl.ds(at, 1)],
                dst_ref=marks.at[k, pl.ds(at, 1)],
                send_sem=mark_send.at[k],
                recv_sem=mark_got.at[k],
                device_id=there,
                device_id_type=MESH,
            ).start()

    def mark_end(k, peers):
        if peers:
            both = pltpu.make_async_remote_copy(
                src_ref=marks.at[k, pl.ds(0, len(peers))],
                dst_ref=marks.at[k, pl.ds(0, len(peers))],
                send_sem=mark_send.at[k],
                recv_sem=mark_got.at[k],
                device_id=peers[0],
                device_id_type=MESH,
            )
            both.wait_recv()
            both.wait_send()
        return jnp.sum(marks[k, 0 : len(peers) + 1], axis=0, keepdims=True)

    def gather_end(k, count):
        others = pl.ds(0, len(everyone))
        both = pltpu.make_async_remote_copy(
            src_ref=terms.at[k, others],
            dst_ref=terms.at[k, others],
            send_sem=term_send.at[k],
            recv_sem=term_got.at[k],
            device_id=everyone[0],
            device_id_type=MESH,
        )
        both.wait_recv()
        both.wait_send()
        row = jnp.sum(terms[k], axis=0, keepdims=True)
        s, l = iota((8, 128), 0), iota((8, 128), 1)
        column = jnp.sum(jnp.where(s == l, row, 0.0), axis=1, keepdims=True)
        return [column[i : i + 1] for i in range(count)]

    def leaving(i):
        return pltpu.make_async_copy(wides.at[i - 1], basis_ref.at[i - 1], out_sem.at[i - 1])

    def settle(i, image, height):
        new = image
        for k in range(i):
            new = new - height[k] * vecs[k]
        new = new * height[i + 1]
        if i < ITERS:
            vecs[i] = new
        if i < ITERS - 1:
            turned_vecs[i] = swap(new)
        if i > 0:
            wides[i - 1] = wide(new)
            leaving(i).start()

    def heights(products, known):
        *with_known, with_last, square = products
        i = len(known)
        found = list(with_known)
        last = with_last
        for k in range(i - 1):
            last = last - known[i - 1][k] * found[k]
        found.append(last * known[i - 1][i])
        for value in found:
            square = square - value * value
        over = lax.rsqrt(square)
        found += [square * over, over]
        return found

    out[...] = tall(start_ref[...]) * weights[...] * SHRINK
    pl.semaphore_wait(barrier, greetings)
    exchange_start(0)
    trace = [jnp.sum(jnp.where(iota((C, C), 0) == iota((C, C), 1), m, 0.0), keepdims=True) / C for m in (kx, ky, kz, mx, my, mz)]
    mean = trace[0] * trace[4] * trace[5] + trace[3] * trace[1] * trace[5] + trace[3] * trace[4] * trace[2]
    mark_start(0, gz, line, jnp.broadcast_to(mean / (nx * ny * nz), (1, 128)))
    exchange_end(0)
    powers[0] = out[...]
    mark_start(1, gx * ny + gy, plane, mark_end(0, line))

    def apply(j):
        here = (turned if j % 2 else powers)[j]
        out[...] = matvec(here, first.at[j % 2], second.at[j % 2], zmat)
        exchange_start((j + 1) % 2)

    def turn(j):
        if j % 2:
            powers[j] = swap(turned[j])
        else:
            turned[j] = swap(powers[j])

    apply(0)
    exchange_end(1)
    turned[1] = out[...]

    apply(1)
    turn(1)
    size = mark_end(1, plane)
    over_size = 1.0 / size
    weighted = weights[...] * powers[1]
    gather_start(1, [(powers[0], weights[...] * powers[0]), (powers[0], weighted), (powers[1], weighted)])
    turned_weights[...] = swap(weights[...])
    exchange_end(0)
    powers[2] = out[...] * over_size

    triangle, alphas, betas, over_betas = [], [], [], []
    shifts = {2: size}
    for j in range(2, ITERS + 1):
        if j < ITERS:
            apply(j)
            if j % 2:
                turn(j)
            if j == 2:
                lifted[j] = powers[2] - 2.0 * powers[1] + size * powers[0]
            else:
                lifted[j] = powers[j] + shifting[...]
            weighted = weights[...] * lifted[j]
            earlier = [powers[0], powers[1]] if j == 2 else [vecs[k] for k in range(j - 1)] + [lifted[j - 1]]
            image = lifted[j]
        else:
            image = turned[j]
            weighted = turned_weights[...] * image
            earlier = [turned_vecs[k] for k in range(j - 1)] + [turned_lifted[...]]
        gather_start(j, [(v, weighted) for v in earlier + [image]])
        if j == ITERS:
            lifted[j] = swap(image)
        elif j % 2 == 0:
            turn(j)
        for k in [j - 1] if j < ITERS else [j - 1, j]:
            if k == 1:
                square, *rest = gather_end(1, 3)
                triangle.append([jnp.sqrt(square), lax.rsqrt(square)])
                start_size, over_start = triangle[0]
                settle(0, powers[0], triangle[0])
                triangle.append(heights(rest, triangle))
                settle(1, powers[1], triangle[1])
                alphas.append(triangle[1][0] * over_start)
                betas.append(triangle[1][1] * over_start)
                over_betas.append(triangle[1][2] * start_size)
                images[0] = powers[1] * (over_start * over_size)
            else:
                products = gather_end(k, k + 1)
                scale, over_scale = size, over_size
                if k == 2:
                    products[0] = products[0] * over_start
                    scale, over_scale = size * over_start, over_size * start_size
                triangle.append(heights(products, triangle))
                settle(k, lifted[k], triangle[k])
                scale = scale * over_betas[k - 2]
                alphas.append(2.0 * shifts[k] - alphas[k - 2] + triangle[k][k - 1] * scale)
                betas.append(triangle[k][k] * scale)
                over_betas.append(triangle[k][k + 1] * (over_scale * betas[k - 2]))
        if j == ITERS:
            break
        image = powers[j] * over_start if j == 2 else powers[j] - betas[j - 3] * images[j - 3]
        image = (image - alphas[j - 2] * images[j - 2]) * over_betas[j - 2]
        images[j - 1] = image
        shift = shifts[j + 1] = alphas[j - 2]
        change = (shift * shift * over_size) * vecs[j - 1] - (2.0 * shift) * image
        if j + 1 < ITERS:
            shifting[...] = change
        else:
            shifting[...] = swap(change)
            turned_lifted[...] = swap(lifted[j])
        exchange_end((j + 1) % 2)
        side = powers if j % 2 else turned
        new = out[...] - alphas[j - 2] * side[j]
        over_lead = over_betas[j - 2]
        if j == 2:
            over_lead = over_lead * over_start
        else:
            behind = betas[j - 3]
            if j == 3:
                behind = behind * over_start
            new = new - behind * side[j - 1]
        new = new * over_lead
        if j + 1 == ITERS:
            new = new + shifting[...]
        side[j + 1] = new

    s, l = iota((8, 128), 0), iota((8, 128), 1)
    tile = jnp.zeros((8, 128), F32)
    for j in range(ITERS):
        tile = jnp.where((s == 0) & (l == j), alphas[j], jnp.where((s == 1) & (l == j), betas[j], tile))
    small[...] = tile[0:2, 0:ITERS]
    last = pltpu.make_async_copy(small, coefficients_ref, out_sem.at[ITERS])
    last.start()
    for i in range(1, ITERS + 1):
        leaving(i).wait()
    last.wait()


def message_counts(x, y, z):
    return x + y + z + y * z, x * (y + z + y * z)


def hand_over(basis_in, coefficients_in, basis_out, coefficients_out, wides, small, in_sem, out_sem):
    pairs = [(basis_in.at[i], wides.at[i], basis_out.at[i]) for i in range(ITERS)]
    pairs.append((coefficients_in, small, coefficients_out))
    come = [pltpu.make_async_copy(a, b, in_sem.at[i]) for i, (a, b, _) in enumerate(pairs)]
    go = [pltpu.make_async_copy(b, c, out_sem.at[i]) for i, (_, b, c) in enumerate(pairs)]
    for copy in come:
        copy.start()
    for first, then in zip(come, go):
        first.wait()
        then.start()
    for copy in go:
        copy.wait()


def shards(sizes, start, stencils):
    nx, ny, nz = sizes
    hbm = pl.BlockSpec(memory_space=pltpu.HBM)
    anyw = pl.BlockSpec(memory_space=pl.ANY)
    basis, coefficients = pl.pallas_call(
        functools.partial(kernel, sizes),
        out_shape=(
            jax.ShapeDtypeStruct((ITERS, C, C * C), F32),
            jax.ShapeDtypeStruct((2, ITERS), F32),
        ),
        in_specs=[hbm, hbm],
        out_specs=(anyw, anyw),
        scratch_shapes=[
            pltpu.VMEM((C, C * C), F32),
            pltpu.VMEM((6, C, C), F32),
            pltpu.VMEM((ITERS, C, C * C), F32),
            pltpu.VMEM((2, ITERS), F32),
            pltpu.VMEM((256, 128), F32),
            pltpu.VMEM((ITERS + 1, 256, 128), F32),
            pltpu.VMEM((ITERS + 1, 256, 128), F32),
            pltpu.VMEM((ITERS, 256, 128), F32),
            pltpu.VMEM((ITERS - 1, 256, 128), F32),
            pltpu.VMEM((256, 128), F32),
            pltpu.VMEM((ITERS + 1, 256, 128), F32),
            pltpu.VMEM((256, 128), F32),
            pltpu.VMEM((ITERS - 1, 256, 128), F32),
            pltpu.VMEM((256, 128), F32),
            pltpu.VMEM((256, 128), F32),
            pltpu.VMEM((2, 2 * C, 6 * C), BF16),
            pltpu.VMEM((2, 2 * C, 12 * C), BF16),
            pltpu.VMEM((256, 384), BF16),
            pltpu.VMEM((2, len(TILES), 8, 128), F32),
            pltpu.VMEM((2, len(ROWS), 128), F32),
            pltpu.VMEM((2, len(TILES), 8, 128), F32),
            pltpu.VMEM((2, len(ROWS), 128), F32),
            pltpu.VMEM((ITERS + 1, nx * ny * nz, 128), F32),
            pltpu.VMEM((2, max(nx * ny, nz), 128), F32),
        ]
        + [pltpu.SemaphoreType.DMA((2, 2))] * 2
        + [pltpu.SemaphoreType.DMA((ITERS + 1,))] * 2
        + [pltpu.SemaphoreType.DMA((2,))] * 2
        + [pltpu.SemaphoreType.DMA((2,)), pltpu.SemaphoreType.DMA((ITERS + 1,))],
        compiler_params=pltpu.CompilerParams(collective_id=0, has_side_effects=True),
    )(start.reshape(C, C * C), stencils.reshape(6, C, C))
    basis, coefficients = pl.pallas_call(
        hand_over,
        out_shape=(
            jax.ShapeDtypeStruct((ITERS, C, C * C), F32),
            jax.ShapeDtypeStruct((2, ITERS), F32),
        ),
        in_specs=[anyw, anyw],
        out_specs=(anyw, anyw),
        scratch_shapes=[
            pltpu.VMEM((ITERS, C, C * C), F32),
            pltpu.VMEM((2, ITERS), F32),
            pltpu.SemaphoreType.DMA((ITERS + 1,)),
            pltpu.SemaphoreType.DMA((ITERS + 1,)),
        ],
    )(basis, coefficients)
    return (
        basis.reshape(1, 1, 1, 1, ITERS, C, C * C),
        coefficients.reshape(1, 2, ITERS),
    )


def solution(mesh):
    sizes = tuple(mesh.shape[a] for a in AXES)
    return jax.shard_map(
        functools.partial(shards, sizes),
        mesh=mesh,
        in_specs=(P("gx", "gy", "gz", None, None, None), P(None, "gx", "gy", "gz", None, None)),
        out_specs=(P("gx", "gy", "gz", None, None, None, None), P()),
        check_vma=False,
    )
```

```python
import functools
import itertools

import jax
import jax.numpy as jnp
from jax import lax
from jax.experimental import pallas as pl
from jax.experimental.pallas import tpu as pltpu
from jax.sharding import PartitionSpec as P

ITERS = 5
C = 32
MESH = pl.DeviceIdType.MESH
F32 = jnp.float32
BF16 = jnp.bfloat16
AXES = ("gx", "gy", "gz")
DIRS = [
    (dx, dy, dz)
    for dx in (-1, 0, 1)
    for dy in (-1, 0, 1)
    for dz in (-1, 0, 1)
    if (dx, dy, dz) != (0, 0, 0)
]
TILES = [d for d in DIRS if d[0] == 0 or d[1:] == (0, 0)]
ROWS = [d for d in DIRS if d not in TILES]
SLOT = {d: i for dirs in (TILES, ROWS) for i, d in enumerate(dirs)}
SHRINK = 2.0**-17


def iota(shape, dim):
    return lax.broadcasted_iota(jnp.int32, shape, dim)


def roll(x, shift, axis):
    size = x.shape[axis]
    shift = shift % size
    return x if shift == 0 else pltpu.roll(x, shift, axis)


def swap(field):
    x = field.reshape(32, 8, 128)
    s, l = iota((1, 8, 128), 1), iota((1, 8, 128), 2)
    s1, l1 = (s // 2) % 2, l // 64
    r = roll(x, 64, 2)
    x = jnp.where(s1 == l1, x, jnp.where(s1 == 0, roll(r, -2, 1), roll(r, 2, 1)))
    s0, l0 = s % 2, (l // 32) % 2
    up, down = roll(roll(x, 32, 2), -1, 1), roll(roll(x, -32, 2), 1, 1)
    x = jnp.where(s0 == l0, x, jnp.where(s0 == 0, up, down))
    even = jnp.concatenate([x[t * 4 : t * 4 + 4] for t in range(0, 8, 2)], axis=0)
    odd = jnp.concatenate([x[t * 4 : t * 4 + 4] for t in range(1, 8, 2)], axis=0)
    half = s < 4
    top = jnp.where(half, even, roll(odd, 4, 1))
    bottom = jnp.where(half, roll(even, 4, 1), odd)
    parts = []
    for ai in range(4):
        for part in (top, bottom):
            for k in range(4):
                parts.append(part[k * 4 + ai : k * 4 + ai + 1])
    return jnp.concatenate(parts, axis=0).reshape(256, 128)


def wide(field):
    return jnp.concatenate([field[t * 32 : t * 32 + 32] for t in range(8)], axis=1)


def tall(field):
    return jnp.concatenate([field[:, t * 128 : t * 128 + 128] for t in range(8)], axis=0)


def split(x):
    high = x.astype(BF16)
    rest = x - high.astype(F32)
    middle = rest.astype(BF16)
    return high, middle, (rest - middle.astype(F32)).astype(BF16)


PAIRS = ((0, 0), (0, 1), (1, 0), (1, 1), (0, 2), (2, 0))


def dot(left, right):
    return jnp.dot(left, right, preferred_element_type=F32)


def spread(matrix):
    parts = split(matrix)
    return jnp.concatenate([parts[i] for i, _ in PAIRS], axis=1)


def stack(field):
    parts = split(field)
    return jnp.concatenate([parts[i] for _, i in PAIRS], axis=0)


def matvec(field, first_ref, second_ref, zmat_ref):
    first = dot(first_ref[...], stack(wide(field)))
    mass, stiff = swap(tall(first[:C])), swap(tall(first[C:]))
    second = dot(second_ref[...], stack(jnp.concatenate([wide(stiff), wide(mass)], axis=0)))
    third = jnp.concatenate([tall(second[:C]), tall(second[C:])], axis=1)
    high, middle, low = split(third)
    pair = zmat_ref[:, 0:256]
    both = dot(high, pair) + dot(middle, pair)
    rest = dot(low, zmat_ref[:, 0:128]) + dot(high, zmat_ref[:, 256:384])
    return both[:, :128] + (both[:, 128:] + rest)


def block_diagonal(matrix):
    zero = jnp.zeros((C, C), F32)
    rows = []
    for i in range(4):
        rows.append(jnp.concatenate([matrix if k == i else zero for k in range(4)], axis=1))
    return jnp.concatenate(rows, axis=0)


def weight_field(sizes, here):
    row, lane = iota((256, 128), 0), iota((256, 128), 1)
    places = (row % C, (row // C) * 4 + lane // C, lane % C)
    weight = jnp.ones((256, 128), F32)
    for place, size, at in zip(places, sizes, here):
        low = jnp.where(at > 0, 0.5, 1.0).astype(F32)
        high = jnp.where(at < size - 1, 0.5, 1.0).astype(F32)
        weight = weight * jnp.where(place == 0, low, jnp.where(place == C - 1, high, 1.0))
    return weight


def neighbour(sizes, here, step):
    fine = None
    for size, at, d in zip(sizes, here, step):
        if d != 0:
            inside = at > 0 if d < 0 else at < size - 1
            fine = inside if fine is None else jnp.logical_and(fine, inside)
    return fine, tuple(at + d for at, d in zip(here, step))


def pack(out_ref, tile_ref, row_ref):
    s, l = iota((8, 128), 0), iota((8, 128), 1)
    line = iota((1, 128), 1)
    lower = lambda t, ai: out_ref[pl.ds(t * 32 + ai * 8, 8), :]
    zero = jnp.zeros((8, 128), F32)
    low, high = zero, zero
    for t in range(8):
        for ai in range(4):
            r = ai * 8 + t
            moved = roll(lower(t, ai), r, 1)
            low = jnp.where(l % C == r, moved, low)
            high = jnp.where(l % C == (r + C - 1) % C, moved, high)

    def send_row(d, plane, source, keep):
        row_ref[pl.ds(SLOT[d], 1), :] = jnp.where(keep, plane[source : source + 1], 0.0)

    for dx in (-1, 1):
        source = 0 if dx < 0 else 7
        for dz, plane, base in ((-1, low, 0), (1, high, -31)):
            for dy in (-1, 0, 1):
                keep = (line % C) // 8 == (3 if dx < 0 else 0)
                if dy != 0:
                    keep = keep & (line // C == (3 if dy < 0 else 0)) & (line % 8 == (7 if dy < 0 else 0))
                send_row((dx, dy, dz), roll(plane, base - dx * 24 - dy * 103, 1), source, keep)
        plane = out_ref[pl.ds(0 if dx < 0 else C - 1, 8, stride=C), :]
        tile_ref[SLOT[(dx, 0, 0)]] = plane
        for dy in (-1, 1):
            keep = line // C == (3 if dy < 0 else 0)
            send_row((dx, dy, 0), roll(plane, 96 if dy < 0 else 32, 1), 0 if dy < 0 else 7, keep)
    for dz, plane, base in ((-1, low, 0), (1, high, -31)):
        tile_ref[SLOT[(0, 0, dz)]] = roll(plane, base, 1)
        for dy in (-1, 1):
            keep = (l // C == (3 if dy < 0 else 0)) & (l % 8 == (7 if dy < 0 else 0))
            tile_ref[SLOT[(0, dy, dz)]] = jnp.where(keep, roll(plane, base - dy * 103, 1), 0.0)
    for dy in (-1, 1):
        plane = zero
        for ai in range(4):
            piece = roll(lower(0 if dy < 0 else 7, ai), C * (ai + (0 if dy < 0 else 1)), 1)
            plane = jnp.where(l // C == ai, piece, plane)
        tile_ref[SLOT[(0, dy, 0)]] = plane


def unpack(out_ref, tile_ref, row_ref):
    s, l = iota((8, 128), 0), iota((8, 128), 1)
    near = (-1, 0, 1)
    got = lambda *d: tile_ref[SLOT[d]]
    row = lambda *d: row_ref[pl.ds(SLOT[d], 1), :]
    ends = lambda last, first: jnp.where(s == 7, last, jnp.where(s == 0, first, 0.0))
    for dx in (-1, 1):
        plane = got(dx, 0, 0) + ends(row(dx, -1, 0), row(dx, 1, 0))
        rows = pl.ds(C - 1 if dx < 0 else 0, 8, stride=C)
        out_ref[rows, :] = out_ref[rows, :] + plane
    low, high = (
        sum(got(0, dy, dz) for dy in near)
        + ends(sum(row(-1, dy, dz) for dy in near), sum(row(1, dy, dz) for dy in near))
        for dz in (1, -1)
    )
    first, last = got(0, 1, 0), got(0, -1, 0)
    for t in range(8):
        for ai in range(4):
            r = ai * 8 + t
            rows = pl.ds(t * 32 + ai * 8, 8)
            add = jnp.where(l % C == 0, roll(low, -r, 1), 0.0)
            add = add + jnp.where(l % C == C - 1, roll(high, 31 - r, 1), 0.0)
            if t == 0:
                add = add + jnp.where(l < C, roll(first, -C * ai, 1), 0.0)
            if t == 7:
                add = add + jnp.where(l >= 96, roll(last, 96 - C * ai, 1), 0.0)
            out_ref[rows, :] = out_ref[rows, :] + add


def kernel(
    sizes,
    start_hbm,
    stencils_hbm,
    basis_ref,
    coefficients_ref,
    start_ref,
    stencils_ref,
    wides,
    small,
    out,
    powers,
    turned,
    vecs,
    turned_vecs,
    turned_weights,
    lifted,
    turned_lifted,
    images,
    shifting,
    weights,
    first,
    second,
    zmat,
    tiles,
    rows,
    got_tiles,
    got_rows,
    terms,
    marks,
    send_sem,
    got_sem,
    term_send,
    term_got,
    mark_send,
    mark_got,
    in_sem,
    out_sem,
):
    here = tuple(lax.axis_index(a) for a in AXES)
    nx, ny, nz = sizes
    gx, gy, gz = here
    me = (gx * ny + gy) * nz + gz
    hops = lambda k, size: min(k, size - k)
    steps = sorted(
        ((i, j, k) for i in range(nx) for j in range(ny) for k in range(nz)),
        key=lambda d: -(hops(d[0], nx) + hops(d[1], ny) + hops(d[2], nz) / 2),
    )
    along = [[lax.rem(at + k, size) for k in range(size)] for at, size in zip(here, sizes)]
    everyone = [tuple(along[a][d[a]] for a in range(3)) for d in steps if any(d)]
    beside = [
        jnp.where(at > 0, 1, 0) + jnp.where(at < size - 1, 1, 0) for at, size in zip(here, sizes)
    ]

    inputs = [
        pltpu.make_async_copy(start_hbm, start_ref, in_sem.at[0]),
        pltpu.make_async_copy(stencils_hbm, stencils_ref, in_sem.at[1]),
    ]
    for copy in inputs:
        copy.start()
    got_tiles[...] = jnp.zeros_like(got_tiles)
    got_rows[...] = jnp.zeros_like(got_rows)
    barrier = pltpu.get_barrier_semaphore()
    line = [(gx, gy, lax.rem(gz + k, nz)) for k in range(1, nz)]
    plane = [
        (along[0][i], along[1][k], gz) for i in range(nx) for k in range(ny) if (i, k) != (0, 0)
    ]
    for there in plane + line:
        pl.semaphore_signal(barrier, inc=1, device_id=there, device_id_type=MESH)
    for d in DIRS:
        if d[2] != 0 and d[:2] != (0, 0):
            fine, there = neighbour(sizes, here, d)

            @pl.when(fine)
            def _():
                pl.semaphore_signal(barrier, inc=1, device_id=there, device_id_type=MESH)

    greetings = len(plane) + len(line) + beside[2] * ((1 + beside[0]) * (1 + beside[1]) - 1)

    weights[...] = weight_field(sizes, here)
    for copy in inputs:
        copy.wait()
    kx, ky, kz, mx, my, mz = (stencils_ref[i] for i in range(6))
    empty = jnp.zeros((C, C), F32)
    for i, (mass, stiff) in enumerate(((mx, kx), (my, ky))):
        first[i] = spread(jnp.concatenate([mass, stiff], axis=0))
        upper, lower = (jnp.concatenate(p, axis=1) for p in ((mass, stiff), (empty, mass)))
        second[1 - i] = spread(jnp.concatenate([upper, lower], axis=0))
    zmat[...] = jnp.concatenate(
        split(jnp.concatenate([block_diagonal(mz.T), block_diagonal(kz.T)], axis=0)), axis=1
    )

    def exchange_start(par):
        pack(out, tiles.at[par], rows.at[par])
        for d in sorted(DIRS, key=lambda d: -(2 * abs(d[0]) + 2 * abs(d[1]) + abs(d[2]))):
            fine, there = neighbour(sizes, here, (d[1], d[0], d[2]) if par else d)
            if d in TILES:
                source, target = tiles.at[par, SLOT[d]], got_tiles.at[par, SLOT[d]]
            else:
                source, target = rows.at[par, pl.ds(SLOT[d], 1)], got_rows.at[par, pl.ds(SLOT[d], 1)]

            @pl.when(fine)
            def _():
                pltpu.make_async_remote_copy(
                    src_ref=source,
                    dst_ref=target,
                    send_sem=send_sem.at[par, int(d in ROWS)],
                    recv_sem=got_sem.at[par, int(d in ROWS)],
                    device_id=there,
                    device_id_type=MESH,
                ).start()

    def exchange_end(par):
        order = (1, 0, 2) if par else (0, 1, 2)
        counts = message_counts(*(beside[i] for i in order))
        choices = [{0} if n == 1 else {1} if n == 2 else {1, 2} for n in (sizes[i] for i in order)]
        for n, m in sorted({message_counts(*c) for c in itertools.product(*choices)}):

            @pl.when((counts[0] == n) & (counts[1] == m))
            def _():
                for kind, (count, sent, got) in enumerate(((n, tiles, got_tiles), (m, rows, got_rows))):
                    if count:
                        both = pltpu.make_async_remote_copy(
                            src_ref=sent.at[par, pl.ds(0, count)],
                            dst_ref=got.at[par, pl.ds(0, count)],
                            send_sem=send_sem.at[par, kind],
                            recv_sem=got_sem.at[par, kind],
                            device_id=everyone[0],
                            device_id_type=MESH,
                        )
                        both.wait_recv()
                        both.wait_send()

        unpack(out, got_tiles.at[par], got_rows.at[par])

    def gather_start(k, pairs):
        s, l = iota((8, 128), 0), iota((8, 128), 1)
        tile = jnp.zeros((8, 128), F32)
        for i, (left, right) in enumerate(pairs):
            lanes = jnp.sum(jnp.sum((left * right).reshape(32, 8, 128), axis=0), axis=0, keepdims=True)
            tile = jnp.where(s == i, lanes, tile)
        column = jnp.sum(tile, axis=1, keepdims=True)
        gather_row(k, jnp.sum(jnp.where(s == l, column, 0.0), axis=0, keepdims=True))

    def gather_row(k, row):
        mine = pl.ds(me, 1)
        terms[k, mine] = row
        for there in everyone:
            pltpu.make_async_remote_copy(
                src_ref=terms.at[k, mine],
                dst_ref=terms.at[k, mine],
                send_sem=term_send.at[k],
                recv_sem=term_got.at[k],
                device_id=there,
                device_id_type=MESH,
            ).start()

    def mark_start(k, at, peers, row):
        marks[k, pl.ds(at, 1)] = row
        for there in peers:
            pltpu.make_async_remote_copy(
                src_ref=marks.at[k, pl.ds(at, 1)],
                dst_ref=marks.at[k, pl.ds(at, 1)],
                send_sem=mark_send.at[k],
                recv_sem=mark_got.at[k],
                device_id=there,
                device_id_type=MESH,
            ).start()

    def mark_end(k, peers):
        if peers:
            both = pltpu.make_async_remote_copy(
                src_ref=marks.at[k, pl.ds(0, len(peers))],
                dst_ref=marks.at[k, pl.ds(0, len(peers))],
                send_sem=mark_send.at[k],
                recv_sem=mark_got.at[k],
                device_id=peers[0],
                device_id_type=MESH,
            )
            both.wait_recv()
            both.wait_send()
        return jnp.sum(marks[k, 0 : len(peers) + 1], axis=0, keepdims=True)

    def gather_end(k, count):
        others = pl.ds(0, len(everyone))
        both = pltpu.make_async_remote_copy(
            src_ref=terms.at[k, others],
            dst_ref=terms.at[k, others],
            send_sem=term_send.at[k],
            recv_sem=term_got.at[k],
            device_id=everyone[0],
            device_id_type=MESH,
        )
        both.wait_recv()
        both.wait_send()
        row = jnp.sum(terms[k], axis=0, keepdims=True)
        s, l = iota((8, 128), 0), iota((8, 128), 1)
        column = jnp.sum(jnp.where(s == l, row, 0.0), axis=1, keepdims=True)
        return [column[i : i + 1] for i in range(count)]

    def leaving(i):
        return pltpu.make_async_copy(wides.at[i - 1], basis_ref.at[i - 1], out_sem.at[i - 1])

    def settle(i, image, height):
        new = image
        for k in range(i):
            new = new - height[k] * vecs[k]
        new = new * height[i + 1]
        if i < ITERS:
            vecs[i] = new
        if i == ITERS - 2:
            turned_vecs[i] = swap(new)
        if i > 0:
            wides[i - 1] = wide(new)
            leaving(i).start()

    def heights(products, known):
        *with_known, with_last, square = products
        i = len(known)
        found = list(with_known)
        last = with_last
        for k in range(i - 1):
            last = last - known[i - 1][k] * found[k]
        found.append(last * known[i - 1][i])
        for value in found:
            square = square - value * value
        over = lax.rsqrt(square)
        found += [square * over, over]
        return found

    out[...] = tall(start_ref[...]) * weights[...] * SHRINK
    pl.semaphore_wait(barrier, greetings)
    exchange_start(0)
    trace = [jnp.sum(jnp.where(iota((C, C), 0) == iota((C, C), 1), m, 0.0), keepdims=True) / C for m in (kx, ky, kz, mx, my, mz)]
    mean = trace[0] * trace[4] * trace[5] + trace[3] * trace[1] * trace[5] + trace[3] * trace[4] * trace[2]
    mark_start(0, gz, line, jnp.broadcast_to(mean / (nx * ny * nz), (1, 128)))
    exchange_end(0)
    powers[0] = out[...]
    mark_start(1, gx * ny + gy, plane, mark_end(0, line))

    def apply(j):
        here = (turned if j % 2 else powers)[j]
        out[...] = matvec(here, first.at[j % 2], second.at[j % 2], zmat)
        exchange_start((j + 1) % 2)

    def turn(j):
        if j % 2:
            powers[j] = swap(turned[j])
        else:
            turned[j] = swap(powers[j])

    apply(0)
    exchange_end(1)
    turned[1] = out[...]

    apply(1)
    turn(1)
    size = mark_end(1, plane)
    over_size = 1.0 / size
    weighted = weights[...] * powers[1]
    gather_start(1, [(powers[0], weights[...] * powers[0]), (powers[0], weighted), (powers[1], weighted)])
    turned_weights[...] = swap(weights[...])
    exchange_end(0)
    powers[2] = out[...] * over_size

    triangle, alphas, betas, over_betas = [], [], [], []
    shifts = {2: size}
    for j in range(2, ITERS + 1):
        if j < ITERS:
            apply(j)
            if j % 2:
                turn(j)
            if j == 2:
                lifted[j] = powers[2] - 2.0 * powers[1] + size * powers[0]
            else:
                lifted[j] = powers[j] + shifting[...]
            weighted = weights[...] * lifted[j]
            earlier = [powers[0], powers[1]] if j == 2 else [vecs[k] for k in range(j - 1)] + [lifted[j - 1]]
            image = lifted[j]
        else:
            image = turned[j]
            weighted = turned_weights[...] * image
            earlier = [turned_vecs[k] for k in range(j - 1)] + [turned_lifted[...]]
        gather_start(j, [(v, weighted) for v in earlier + [image]])
        if j == ITERS:
            lifted[j] = swap(image)
        elif j % 2 == 0:
            turn(j)
        if j == ITERS - 2:
            turned_vecs[0] = swap(vecs[0])
            turned_vecs[1] = swap(vecs[1])
        if j == ITERS - 1:
            turned_vecs[2] = swap(vecs[2])
            turned_lifted[...] = swap(lifted[j])
        for k in [j - 1] if j < ITERS else [j - 1, j]:
            if k == 1:
                square, *rest = gather_end(1, 3)
                triangle.append([jnp.sqrt(square), lax.rsqrt(square)])
                start_size, over_start = triangle[0]
                settle(0, powers[0], triangle[0])
                triangle.append(heights(rest, triangle))
                settle(1, powers[1], triangle[1])
                alphas.append(triangle[1][0] * over_start)
                betas.append(triangle[1][1] * over_start)
                over_betas.append(triangle[1][2] * start_size)
                images[0] = powers[1] * (over_start * over_size)
            else:
                products = gather_end(k, k + 1)
                scale, over_scale = size, over_size
                if k == 2:
                    products[0] = products[0] * over_start
                    scale, over_scale = size * over_start, over_size * start_size
                triangle.append(heights(products, triangle))
                settle(k, lifted[k], triangle[k])
                scale = scale * over_betas[k - 2]
                alphas.append(2.0 * shifts[k] - alphas[k - 2] + triangle[k][k - 1] * scale)
                betas.append(triangle[k][k] * scale)
                over_betas.append(triangle[k][k + 1] * (over_scale * betas[k - 2]))
        if j == ITERS:
            break
        image = powers[j] * over_start if j == 2 else powers[j] - betas[j - 3] * images[j - 3]
        image = (image - alphas[j - 2] * images[j - 2]) * over_betas[j - 2]
        images[j - 1] = image
        shift = shifts[j + 1] = alphas[j - 2]
        change = (shift * shift * over_size) * vecs[j - 1] - (2.0 * shift) * image
        if j + 1 < ITERS:
            shifting[...] = change
        else:
            shifting[...] = swap(change)
        exchange_end((j + 1) % 2)
        side = powers if j % 2 else turned
        new = out[...] - alphas[j - 2] * side[j]
        over_lead = over_betas[j - 2]
        if j == 2:
            over_lead = over_lead * over_start
        else:
            behind = betas[j - 3]
            if j == 3:
                behind = behind * over_start
            new = new - behind * side[j - 1]
        new = new * over_lead
        if j + 1 == ITERS:
            new = new + shifting[...]
        side[j + 1] = new

    s, l = iota((8, 128), 0), iota((8, 128), 1)
    tile = jnp.zeros((8, 128), F32)
    for j in range(ITERS):
        tile = jnp.where((s == 0) & (l == j), alphas[j], jnp.where((s == 1) & (l == j), betas[j], tile))
    small[...] = tile[0:2, 0:ITERS]
    last = pltpu.make_async_copy(small, coefficients_ref, out_sem.at[ITERS])
    last.start()
    for i in range(1, ITERS + 1):
        leaving(i).wait()
    last.wait()


def message_counts(x, y, z):
    return x + y + z + y * z, x * (y + z + y * z)


def hand_over(basis_in, coefficients_in, basis_out, coefficients_out, wides, small, in_sem, out_sem):
    pairs = [(basis_in.at[i], wides.at[i], basis_out.at[i]) for i in range(ITERS)]
    pairs.append((coefficients_in, small, coefficients_out))
    come = [pltpu.make_async_copy(a, b, in_sem.at[i]) for i, (a, b, _) in enumerate(pairs)]
    go = [pltpu.make_async_copy(b, c, out_sem.at[i]) for i, (_, b, c) in enumerate(pairs)]
    for copy in come:
        copy.start()
    for first, then in zip(come, go):
        first.wait()
        then.start()
    for copy in go:
        copy.wait()


def shards(sizes, start, stencils):
    nx, ny, nz = sizes
    hbm = pl.BlockSpec(memory_space=pltpu.HBM)
    anyw = pl.BlockSpec(memory_space=pl.ANY)
    basis, coefficients = pl.pallas_call(
        functools.partial(kernel, sizes),
        out_shape=(
            jax.ShapeDtypeStruct((ITERS, C, C * C), F32),
            jax.ShapeDtypeStruct((2, ITERS), F32),
        ),
        in_specs=[hbm, hbm],
        out_specs=(anyw, anyw),
        scratch_shapes=[
            pltpu.VMEM((C, C * C), F32),
            pltpu.VMEM((6, C, C), F32),
            pltpu.VMEM((ITERS, C, C * C), F32),
            pltpu.VMEM((2, ITERS), F32),
            pltpu.VMEM((256, 128), F32),
            pltpu.VMEM((ITERS + 1, 256, 128), F32),
            pltpu.VMEM((ITERS + 1, 256, 128), F32),
            pltpu.VMEM((ITERS, 256, 128), F32),
            pltpu.VMEM((ITERS - 1, 256, 128), F32),
            pltpu.VMEM((256, 128), F32),
            pltpu.VMEM((ITERS + 1, 256, 128), F32),
            pltpu.VMEM((256, 128), F32),
            pltpu.VMEM((ITERS - 1, 256, 128), F32),
            pltpu.VMEM((256, 128), F32),
            pltpu.VMEM((256, 128), F32),
            pltpu.VMEM((2, 2 * C, 6 * C), BF16),
            pltpu.VMEM((2, 2 * C, 12 * C), BF16),
            pltpu.VMEM((256, 384), BF16),
            pltpu.VMEM((2, len(TILES), 8, 128), F32),
            pltpu.VMEM((2, len(ROWS), 128), F32),
            pltpu.VMEM((2, len(TILES), 8, 128), F32),
            pltpu.VMEM((2, len(ROWS), 128), F32),
            pltpu.VMEM((ITERS + 1, nx * ny * nz, 128), F32),
            pltpu.VMEM((2, max(nx * ny, nz), 128), F32),
        ]
        + [pltpu.SemaphoreType.DMA((2, 2))] * 2
        + [pltpu.SemaphoreType.DMA((ITERS + 1,))] * 2
        + [pltpu.SemaphoreType.DMA((2,))] * 2
        + [pltpu.SemaphoreType.DMA((2,)), pltpu.SemaphoreType.DMA((ITERS + 1,))],
        compiler_params=pltpu.CompilerParams(collective_id=0, has_side_effects=True),
    )(start.reshape(C, C * C), stencils.reshape(6, C, C))
    basis, coefficients = pl.pallas_call(
        hand_over,
        out_shape=(
            jax.ShapeDtypeStruct((ITERS, C, C * C), F32),
            jax.ShapeDtypeStruct((2, ITERS), F32),
        ),
        in_specs=[anyw, anyw],
        out_specs=(anyw, anyw),
        scratch_shapes=[
            pltpu.VMEM((ITERS, C, C * C), F32),
            pltpu.VMEM((2, ITERS), F32),
            pltpu.SemaphoreType.DMA((ITERS + 1,)),
            pltpu.SemaphoreType.DMA((ITERS + 1,)),
        ],
    )(basis, coefficients)
    return (
        basis.reshape(1, 1, 1, 1, ITERS, C, C * C),
        coefficients.reshape(1, 2, ITERS),
    )


def solution(mesh):
    sizes = tuple(mesh.shape[a] for a in AXES)
    return jax.shard_map(
        functools.partial(shards, sizes),
        mesh=mesh,
        in_specs=(P("gx", "gy", "gz", None, None, None), P(None, "gx", "gy", "gz", None, None)),
        out_specs=(P("gx", "gy", "gz", None, None, None, None), P()),
        check_vma=False,
    )
```
